32 devices in a mesh: rep: 4 (over z), fsdp: 2 (over x), tp: 4 (over y, core).
Axes of the slice: x: 2, y: 2, z: 4, core: 2. Of those that a mesh axis runs over, the one named last changes fastest.
Arguments:
- gate_pre: bfloat16 [1024, 14848], P(('rep', 'fsdp'), 'tp'), may hold values from -6 to 6
- up_pre: bfloat16 [1024, 14848], P(('rep', 'fsdp'), 'tp'), may hold values from -30 to 30
- out_grad: bfloat16 [1024, 4096], P(('rep', 'fsdp')), may hold values from -30 to 30
Outputs:
- down_grad: bfloat16 [4096, 14848], P('fsdp', 'tp')
The draws below stay inside these ranges and needn't reach their ends.
All inputs are finite; a program needn't handle non-finite values.
Results may differ from the reference program's by a relative error of at most 0.02.
Values may be sent and summed in bfloat16 or wider, within the bound.
A program may use at most 128 MiB of HBM per device.

```python
import jax
import jax.numpy as jnp
from jax import lax

D = 4096
FF = 14848
TOK_DEV = 128
TOKENS = 1024
N_REP = 4
N_FSDP = 2


def draw_up_pre(key, part):
    subkeys = jax.random.split(jax.random.fold_in(key, 11), 2)
    position = jnp.arange(FF, dtype=jnp.float32) / FF
    roughness = jax.random.uniform(subkeys[1], (FF,), jnp.float32, 1.0, 2.0)
    entries = jnp.clip(jax.random.normal(subkeys[0], (TOKENS, FF), jnp.float32), -5.0, 5.0)
    column_scale = 3.0 ** position * roughness / 3.0
    return (entries * column_scale[None, :]).astype(jnp.bfloat16)


def draw_out_grad(key, part):
    subkeys = jax.random.split(jax.random.fold_in(key, 23), 2)
    position = jnp.arange(D, dtype=jnp.float32) / D
    roughness = jax.random.uniform(subkeys[1], (D,), jnp.float32, 1.0, 2.0)
    entries = jnp.clip(jax.random.normal(subkeys[0], (TOKENS, D), jnp.float32), -5.0, 5.0)
    column_scale = 3.0 ** position * roughness / 3.0
    return (entries * column_scale[None, :]).astype(jnp.bfloat16)


def levels(stream_key, shape, cuts, least, top_value):
    def one(axis_at, parts):
        steps = jax.random.uniform(jax.random.fold_in(jax.random.fold_in(stream_key, 6), axis_at), (parts,), jnp.float32, least / len(cuts), top_value / len(cuts))
        return jnp.repeat(jnp.exp(steps), shape[axis_at] // parts).reshape((-1,) + (1,) * (len(shape) - axis_at - 1))

    gain = one(*cuts[0])
    for cut in cuts[1:]:
        gain = gain * one(*cut)
    return gain


def centred(rng, shape, deviation, limit, pieces=(), held_as=jnp.bfloat16):
    loudness = levels(rng, shape, pieces, -0.22, 0.18) if pieces else 1.0
    result = jax.random.normal(rng, shape, jnp.float32) * deviation * loudness
    return jnp.minimum(jnp.maximum(result, -limit), limit).astype(held_as)


def setup_inputs(seed: int = 0) -> dict:
    arg_keys = jax.random.split(jax.random.key(seed), 4)
    gate_pre = centred(arg_keys[0], (TOKENS, FF), 1.0, 6.0, ((0, 8), (1, 4)))
    up_pre = draw_up_pre(jax.random.fold_in(arg_keys[3], 71), 0)
    out_grad = draw_out_grad(jax.random.fold_in(arg_keys[3], 71), 0)
    return {"gate_pre": gate_pre, "up_pre": up_pre, "out_grad": out_grad}


def reference(gate_pre, up_pre, out_grad):
    hidden = (jax.nn.silu(gate_pre.astype(jnp.float32)) * up_pre.astype(jnp.float32)).astype(jnp.bfloat16)
    hidden_blocks = hidden.reshape(N_REP, N_FSDP, TOK_DEV, FF)
    grad_blocks = out_grad.reshape(N_REP, N_FSDP, TOK_DEV, D)

    def inner_add(running, paired):
        grad_rows, hidden_rows = paired
        partial_term = jnp.dot(grad_rows.T, hidden_rows, preferred_element_type=jnp.float32)
        return (running + partial_term.astype(jnp.bfloat16).astype(jnp.float32), None)

    def outer_add(running, paired):
        starting = jnp.zeros((D, FF), jnp.float32)
        replica_part, unused = lax.scan(inner_add, starting, paired)
        return (running + replica_part.astype(jnp.bfloat16).astype(jnp.float32), None)
    summed, unused = lax.scan(outer_add, jnp.zeros((D, FF), jnp.float32), (grad_blocks, hidden_blocks))
    square_total = jnp.sum(summed * summed)
    factor = 1.0 / jnp.sqrt(square_total / (D * FF) + 1e-06)
    return (summed * factor).astype(jnp.bfloat16)
```

```python
import functools

import jax
import jax.numpy as jnp
from jax import lax
from jax.experimental import pallas as pl
from jax.experimental.pallas import tpu as pltpu
from jax.sharding import PartitionSpec as P

MESH = pl.DeviceIdType.MESH
LANES = 128
VMEM_LIMIT = 60 * 1024 * 1024
WIDTH = 512
TILE = 512
LAG = 2
AHEAD = 2


class Chunk:
    def __init__(self, index, start, size):
        self.index, self.start, self.size = index, start, size

    @property
    def cols(self):
        start = self.start
        return pl.ds(start if isinstance(start, int) else pl.multiple_of(start, LANES), self.size)


def chunking(columns):
    head = columns % WIDTH
    first = 1 if head else 0
    count = first + columns // WIDTH

    def chunk(index):
        if isinstance(index, int) and index < first:
            return Chunk(index, 0, head)
        return Chunk(index, head + (index - first) * WIDTH, WIDTH)

    return first, count, chunk


def gather_multiply(
    entry_count, gate_ref, up_ref, grad_ref, out_ref, factor_ref,
    held, grads, turned, gate_in, up_in, sums, total_out,
    local_sem, gx_send, gx_recv, gz_recv, gz_out, gz_in, gy_send, gy_recv,
    gs_send, gs_recv, gf_send, gf_recv,
    z_recv, z_out, z_in, zo_recv, zo_send, x_send, x_recv,
    sq_send, sq_recv, fa_send, fa_recv,
):
    rep = lax.axis_index("rep")
    fsdp = lax.axis_index("fsdp")
    tp = lax.axis_index("tp")
    rows, columns = gate_ref.shape
    half = grads.shape[1]
    n_tp = 4
    quarter = half // n_tp
    first, count, chunk = chunking(columns)
    other = 1 - fsdp
    side = rep // 2
    edge, near, far, far_edge = 3 * side, 1 + side, 2 - side, 3 - 3 * side
    is_edge = rep == edge
    inner = jnp.where(is_edge, near, far)
    sibling = tp + 1 - 2 * lax.rem(tp, 2)
    opposite = lax.rem(tp + 2, n_tp)
    past = lax.rem(sibling + 2, n_tp)

    def rows_of(r, s):
        return pl.ds(pl.multiple_of((r * 2 + s) * rows, rows), rows)

    def quarter_of(t):
        return pl.ds(pl.multiple_of(t * quarter, LANES), quarter)

    def remote(src, dst, send, recv, device):
        return pltpu.make_async_remote_copy(
            src_ref=src, dst_ref=dst, send_sem=send, recv_sem=recv,
            device_id=device, device_id_type=MESH,
        )

    loads = [
        pltpu.make_async_copy(gate_ref, gate_in, local_sem.at[0]),
        pltpu.make_async_copy(up_ref, up_in, local_sem.at[1]),
        pltpu.make_async_copy(
            grad_ref.at[:, pl.ds(pl.multiple_of(fsdp * half, LANES), half)],
            grads.at[rows_of(rep, fsdp), :], local_sem.at[2],
        ),
    ]
    for load in loads:
        load.start()

    barrier = pltpu.get_barrier_semaphore()
    for k in range(n_tp):
        if k:
            pl.semaphore_signal(
                barrier, inc=1, device_id={"tp": lax.rem(tp + k, n_tp)}, device_id_type=MESH
            )
        pl.semaphore_signal(
            barrier, inc=1, device_id={"fsdp": other, "tp": lax.rem(tp + k, n_tp)},
            device_id_type=MESH,
        )
    pl.semaphore_signal(barrier, inc=1, device_id={"rep": inner}, device_id_type=MESH)

    @pl.when(jnp.logical_not(is_edge))
    def _():
        pl.semaphore_signal(barrier, inc=1, device_id={"rep": edge}, device_id_type=MESH)

    pl.semaphore_wait(barrier, 2 * n_tp + jnp.where(is_edge, 0, 1))

    def grad_across():
        src = grad_ref.at[:, pl.ds(pl.multiple_of(other * half + tp * quarter, LANES), quarter)]
        return remote(src, grads.at[rows_of(rep, fsdp), quarter_of(tp)], gx_send, gx_recv, {"fsdp": other})

    def grad_spot(r, s, t):
        return grads.at[rows_of(r, s), quarter_of(t)]

    def grad_hop(r, s, own, inward):
        spot = grad_spot(r, s, tp)
        src = spot
        if own:
            src = grad_ref.at[:, pl.ds(pl.multiple_of(fsdp * half + tp * quarter, LANES), quarter)]
        to = inner if inward else edge
        return remote(src, spot, (gz_in if inward else gz_out).at[r, s], gz_recv.at[r, s], {"rep": to})

    def grad_got(r, s):
        spot = grad_spot(r, s, tp)
        return remote(spot, spot, gz_in.at[r, s], gz_recv.at[r, s], {"rep": inner})

    def over_y(r, s, t):
        spot = grad_spot(r, s, t)
        return remote(spot, spot, gy_send.at[r, s], gy_recv.at[r, s], {"tp": opposite})

    def to_sibling(r, s, t):
        spot = grad_spot(r, s, t)
        return remote(spot, spot, gs_send.at[r, s], gs_recv.at[r, s], {"tp": sibling})

    def pass_sibling(r, s, t):
        spot = grad_spot(r, s, t)
        return remote(spot, spot, gf_send.at[r, s], gf_recv.at[r, s], {"tp": sibling})

    def hop(r, ch, inward):
        spot = held.at[rows_of(r, fsdp), ch.cols]
        to = inner if inward else edge
        return remote(spot, spot, (z_in if inward else z_out).at[r, ch.index], z_recv.at[r, ch.index], {"rep": to})

    def hop_got(r, ch):
        spot = held.at[rows_of(r, fsdp), ch.cols]
        return remote(spot, spot, z_in.at[r, ch.index], z_recv.at[r, ch.index], {"rep": inner})

    def hop_other(ch):
        spot = held.at[rows_of(edge, other), ch.cols]
        return remote(spot, spot, zo_send.at[ch.index], zo_recv.at[ch.index], {"rep": inner})

    def cross(r, ch):
        spot = held.at[rows_of(r, fsdp), ch.cols]
        return remote(spot, spot, x_send.at[r, ch.index], x_recv.at[r, ch.index], {"fsdp": other})

    def crossed(r, ch):
        spot = held.at[rows_of(r, other), ch.cols]
        return remote(spot, spot, x_send.at[r, ch.index], x_recv.at[r, ch.index], {"fsdp": other})

    def on_edge(act):
        pl.when(is_edge)(act)

    def on_middle(act):
        pl.when(jnp.logical_not(is_edge))(act)

    def chunks_from(low, high, act):
        while low < high and low < first:
            act(chunk(low))
            low += 1
        if low < high:
            @pl.loop(low, high)
            def _(index):
                act(chunk(index))

    grad_across().start()
    grad_hop(rep, fsdp, True, True).start()
    on_middle(lambda: grad_hop(rep, fsdp, True, False).start())

    loads[0].wait()
    loads[1].wait()

    @pl.loop(0, columns // LANES)
    def _(at):
        cols = pl.ds(pl.multiple_of(at * LANES, LANES), LANES)
        gate = gate_in[:, cols].astype(jnp.float32)
        held[rows_of(rep, fsdp), cols] = (
            jax.nn.silu(gate) * up_in[:, cols].astype(jnp.float32)
        ).astype(held.dtype)

    chunks_from(0, count, lambda ch: cross(rep, ch).start())
    hop(rep, chunk(0), True).start()
    on_middle(lambda: hop(rep, chunk(0), False).start())

    def share(r, s):
        over_y(r, s, tp).start()
        to_sibling(r, s, tp).start()

    def pass_on(r, s):
        over_y(r, s, opposite).wait_recv()
        pass_sibling(r, s, opposite).start()

    def settle(r, s):
        to_sibling(r, s, sibling).wait_recv()
        pass_sibling(r, s, past).wait_recv()

    tile = 256

    def turn(r):
        spot = pl.ds(pl.multiple_of(r * 2 * rows, 2 * rows), 2 * rows)

        @pl.loop(0, half // tile)
        def _(m):
            part = pl.ds(pl.multiple_of(m * tile, tile), tile)
            turned[part, spot] = grads[spot, part].T

    def take_own():
        grad_across().wait_recv()
        grad_hop(rep, other, False, True).start()
        on_middle(lambda: grad_hop(rep, other, False, False).start())
        share(rep, other)

    def spread(items, take, after):
        waiting = {}

        def land(name, r, s):
            pass_on(r, s)
            waiting.setdefault(name, []).append((r, s))
            if len(waiting[name]) == (1 if name == "own" else 2):
                for pair in waiting[name]:
                    settle(*pair)
                turn(r)

        for at, item in enumerate(items):
            take(*item)
            after(at)
            if at:
                land(*items[at - 1])
        land(*items[-1])

    loads[2].wait()

    @on_edge
    def _():
        share_of = [(at * count // 7, (at + 1) * count // 7) for at in range(7)]

        def take(name, r, s):
            if name == "own":
                take_own()
                chunks_from(1, count, lambda ch: hop(rep, ch, True).start())
            else:
                grad_got(r, s).wait_recv()
                share(r, s)

        def after(at):
            def act(ch):
                crossed(edge, ch).wait_recv()
                hop_other(ch).start()
            chunks_from(*share_of[at], act)

        spread(
            [("own", rep, other), ("near", near, fsdp), ("near", near, other),
             ("far", far, fsdp), ("far", far, other),
             ("last", far_edge, fsdp), ("last", far_edge, other)],
            take, after,
        )

    @on_middle
    def _():
        def take(name, r, s):
            if name == "own":
                take_own()
                return
            grad_got(r, s).wait_recv()
            grad_hop(r, s, False, name == "edge").start()
            share(r, s)

        spread(
            [("own", rep, other), ("edge", edge, fsdp), ("far", far, fsdp),
             ("edge", edge, other), ("far", far, other),
             ("last", far_edge, fsdp), ("last", far_edge, other)],
            take, lambda at: None,
        )

    def clear():
        sums[fsdp * n_tp + tp] = jnp.zeros(sums.shape[1:], sums.dtype)

    def multiply_tile(ch, m, squared):
        spot = pl.ds(pl.multiple_of(m * TILE, TILE), TILE)
        product = jnp.dot(turned[spot, :], held[:, ch.cols], preferred_element_type=jnp.float32)
        out_ref[spot, ch.cols] = product.astype(out_ref.dtype)
        if squared:
            squares = jnp.sum((product * product).reshape(TILE // 8, 8, ch.size), axis=0)
            total = squares[:, :LANES]
            for at in range(LANES, ch.size, LANES):
                total = total + squares[:, at:at + LANES]
            sums[fsdp * n_tp + tp] += total

    tiles = half // TILE

    def sweep(events, arrived, squared):
        places = [at * tiles // len(events) for at in range(len(events))]

        def step(index, lagging):
            def at_tile(m):
                for place, event in zip(places, events):
                    pl.when(m == place)(lambda: event(chunk(index)))
                if lagging is not None:
                    multiply_tile(lagging, m, squared)
            if lagging is not None:
                arrived(lagging)
                pl.loop(0, tiles)(at_tile)
            else:
                for event in events:
                    event(chunk(index))

        start = min(count, first + LAG)
        for index in range(start):
            step(index, chunk(index - LAG) if index >= LAG else None)

        @pl.loop(start, count)
        def _(index):
            step(index, chunk(index - LAG))

        def finish(ch):
            arrived(ch)
            pl.loop(0, tiles)(lambda m: multiply_tile(ch, m, squared))
        chunks_from(max(count - LAG, 0), count, finish)

    @on_edge
    def _():
        def pull(r):
            def event(ch):
                hop_got(r, ch).wait_recv()
                cross(r, ch).start()
            return event

        def arrived(ch):
            for r in (near, far, far_edge):
                crossed(r, ch).wait_recv()

        sweep([pull(near), pull(far), pull(far_edge)], arrived, False)

    @on_middle
    def _():
        def inward(ch):
            hop(rep, ch, True).start()
            hop_got(edge, ch).wait_recv()
            hop(edge, ch, True).start()

        hop_got(edge, chunk(0)).wait_recv()
        hop(edge, chunk(0), True).start()
        chunks_from(1, min(1 + AHEAD, count), inward)

        def outer(ch):
            index = ch.index
            if isinstance(index, int):
                if index:
                    hop(rep, ch, False).start()
                    if index + AHEAD < count:
                        inward(chunk(index + AHEAD))
            else:
                hop(rep, ch, False).start()
                pl.when(index + AHEAD < count)(lambda: inward(chunk(index + AHEAD)))

        def pull(r):
            def event(ch):
                hop_got(r, ch).wait_recv()
                hop(r, ch, False).start()
                cross(r, ch).start()
            return event

        def arrived(ch):
            hop_other(ch).wait_recv()
            for r in (rep, far, far_edge):
                crossed(r, ch).wait_recv()

        clear()
        sweep([outer, pull(far), pull(far_edge)], arrived, True)

        mine = fsdp * n_tp + tp
        peers = [(a, k) for a in range(2) for k in range(n_tp) if a or k]

        def exchange(at, towards):
            a, k = peers[at]
            to_side = other if a else fsdp
            to_tp = lax.rem(tp + (k if towards else n_tp - k), n_tp)
            spot = sums.at[mine if towards else to_side * n_tp + to_tp]
            return remote(spot, spot, sq_send.at[at], sq_recv.at[at], {"fsdp": to_side, "tp": to_tp})

        for at in range(len(peers)):
            exchange(at, True).start()
        for at in range(len(peers)):
            exchange(at, False).wait_recv()
        square_total = jnp.sum(jnp.sum(sums[...], axis=0), keepdims=True)
        factor = 1.0 / jnp.sqrt(square_total / entry_count + 1e-06)
        total_out[...] = jnp.broadcast_to(factor, total_out.shape)
        for at in range(len(peers)):
            exchange(at, True).wait_send()

    def tell():
        return remote(total_out, total_out, fa_send, fa_recv, {"rep": jnp.where(is_edge, near, edge)})

    on_middle(lambda: tell().start())
    on_edge(lambda: tell().wait_recv())
    factor_ref[...] = total_out[...]

    grad_across().wait_send()

    def sent_shares(r, s):
        over_y(r, s, tp).wait_send()
        to_sibling(r, s, tp).wait_send()
        pass_sibling(r, s, opposite).wait_send()

    sent_shares(rep, other)
    grad_hop(rep, fsdp, True, True).wait_send()
    grad_hop(rep, other, False, True).wait_send()
    chunks_from(0, count, lambda ch: cross(rep, ch).wait_send())

    @on_edge
    def _():
        for r in (near, far, far_edge):
            for s in (fsdp, other):
                sent_shares(r, s)

        def sent(ch):
            hop(rep, ch, True).wait_send()
            hop_other(ch).wait_send()
            for r in (near, far, far_edge):
                cross(r, ch).wait_send()
        chunks_from(0, count, sent)

    @on_middle
    def _():
        tell().wait_send()
        for s, own in ((fsdp, True), (other, False)):
            grad_hop(rep, s, own, False).wait_send()
            grad_hop(edge, s, False, True).wait_send()
            for r in (edge, far, far_edge):
                sent_shares(r, s)
            for r in (far, far_edge):
                grad_hop(r, s, False, False).wait_send()

        def sent(ch):
            for r in (rep, edge):
                hop(r, ch, True).wait_send()
            for r in (rep, far, far_edge):
                hop(r, ch, False).wait_send()
            for r in (far, far_edge):
                cross(r, ch).wait_send()
        chunks_from(0, count, sent)


def by_kernel(n_rep, n_tp, entry_count, gate_pre, up_pre, out_grad):
    rows, columns = gate_pre.shape
    tokens = rows * n_rep * 2
    half = out_grad.shape[1] // 2
    count = chunking(columns)[1]
    dma = pltpu.SemaphoreType.DMA
    block, piece = dma((n_rep, 2)), dma((n_rep, count))
    return pl.pallas_call(
        functools.partial(gather_multiply, entry_count),
        out_shape=(
            pltpu.VMEM((half, columns), jnp.bfloat16),
            pltpu.VMEM((8, LANES), jnp.float32),
        ),
        in_specs=[pl.BlockSpec(memory_space=pl.ANY)] * 3,
        out_specs=(pl.BlockSpec(memory_space=pltpu.VMEM), pl.BlockSpec(memory_space=pltpu.VMEM)),
        scratch_shapes=[
            pltpu.VMEM((tokens, columns), jnp.bfloat16),
            pltpu.VMEM((tokens, half), jnp.bfloat16),
            pltpu.VMEM((half, tokens), jnp.bfloat16),
            pltpu.VMEM((rows, columns), jnp.bfloat16),
            pltpu.VMEM((rows, columns), jnp.bfloat16),
            pltpu.VMEM((2 * n_tp, 8, LANES), jnp.float32),
            pltpu.VMEM((8, LANES), jnp.float32),
            dma((3,)), dma, dma, block, block, block, block, block,
            block, block, block, block,
            piece, piece, piece, dma((count,)), dma((count,)), piece, piece,
            dma((2 * n_tp - 1,)), dma((2 * n_tp - 1,)), dma, dma,
        ],
        compiler_params=pltpu.CompilerParams(
            collective_id=0, has_side_effects=True, vmem_limit_bytes=VMEM_LIMIT * 3 // 4
        ),
    )(gate_pre, up_pre, out_grad)


def scale(summed, factors):
    half, columns = summed.shape
    rows = 128

    def body(summed_ref, factor_ref, out_ref, ready, sems):
        steps = half // rows
        depth = ready.shape[0]

        def leave(m):
            slot = lax.rem(m, depth)
            spot = pl.ds(pl.multiple_of(m * rows, rows), rows)
            return pltpu.make_async_copy(ready.at[slot], out_ref.at[spot, :], sems.at[slot])

        @pl.loop(0, steps)
        def _(m):
            slot = lax.rem(m, depth)
            spot = pl.ds(pl.multiple_of(m * rows, rows), rows)

            @pl.when(m >= depth)
            def _():
                leave(m - depth).wait()
            for at in range(0, columns, LANES):
                cols = pl.ds(at, LANES)
                scaled = summed_ref[spot, cols].astype(jnp.float32) * factor_ref[0:1, :]
                ready[slot, :, cols] = scaled.astype(ready.dtype)
            leave(m).start()

        @pl.loop(max(steps - depth, 0), steps)
        def _(m):
            leave(m).wait()

    return pl.pallas_call(
        body,
        out_shape=jax.ShapeDtypeStruct((half, columns), jnp.bfloat16),
        in_specs=[pl.BlockSpec(memory_space=pltpu.VMEM)] * 2,
        out_specs=pl.BlockSpec(memory_space=pl.ANY),
        scratch_shapes=[pltpu.VMEM((4, rows, columns), jnp.bfloat16), pltpu.SemaphoreType.DMA((4,))],
        compiler_params=pltpu.CompilerParams(vmem_limit_bytes=16 * 1024 * 1024),
    )(summed, factors)


def by_xla(gate_pre, up_pre, out_grad):
    hidden = (jax.nn.silu(gate_pre.astype(jnp.float32)) * up_pre.astype(jnp.float32)).astype(
        jnp.bfloat16
    )
    spread = lax.all_to_all(out_grad, "fsdp", split_axis=1, concat_axis=0, tiled=True)
    grad_rows = lax.all_gather(spread, "rep", axis=0, tiled=True)
    hidden_rows = lax.all_gather(hidden, ("rep", "fsdp"), axis=0, tiled=True)
    summed = lax.dot_general(
        grad_rows, hidden_rows, (((0,), (0,)), ((), ())), preferred_element_type=jnp.float32
    )
    return summed, jnp.sum(summed * summed)


def kernel_fits(n_rep, n_fsdp, n_tp, rows, columns, features):
    tokens, half = rows * n_rep * n_fsdp, features // n_fsdp
    held_bytes = 2 * (tokens * columns + 2 * tokens * half + half * columns + 2 * rows * columns)
    aligned = rows % 128 == 0 and columns % LANES == 0 and half % (LANES * n_tp) == 0
    shaped = (n_rep, n_fsdp, n_tp) == (4, 2, 4) and columns >= 4 * WIDTH
    return shaped and aligned and half % TILE == 0 and held_bytes < VMEM_LIMIT * 3 // 4


def solution(mesh):
    n_rep, n_fsdp, n_tp = (mesh.shape[axis] for axis in ("rep", "fsdp", "tp"))

    def on_device(gate_pre, up_pre, out_grad):
        half, columns = out_grad.shape[1] // n_fsdp, gate_pre.shape[1]
        entry_count = half * n_fsdp * columns * n_tp
        if kernel_fits(n_rep, n_fsdp, n_tp, *gate_pre.shape, out_grad.shape[1]):
            summed, factors = by_kernel(n_rep, n_tp, entry_count, gate_pre, up_pre, out_grad)
            return scale(summed, factors)
        summed, square_sum = by_xla(gate_pre, up_pre, out_grad)
        square_total = lax.psum(square_sum, ("fsdp", "tp"))
        factor = 1.0 / jnp.sqrt(square_total / entry_count + 1e-06)
        return (summed * factor).astype(jnp.bfloat16)

    return jax.shard_map(
        on_device,
        mesh=mesh,
        in_specs=(P(("rep", "fsdp"), "tp"), P(("rep", "fsdp"), "tp"), P(("rep", "fsdp"), None)),
        out_specs=P("fsdp", "tp"),
        check_vma=False,
    )
```

```python
import functools

import jax
import jax.numpy as jnp
from jax import lax
from jax.experimental import pallas as pl
from jax.experimental.pallas import tpu as pltpu
from jax.sharding import PartitionSpec as P

MESH = pl.DeviceIdType.MESH
LANES = 128
VMEM_LIMIT = 60 * 1024 * 1024
WIDTH = 256
TILE = 1024
LAG = 4
AHEAD = 4


class Chunk:
    def __init__(self, index, start, size):
        self.index, self.start, self.size = index, start, size

    @property
    def cols(self):
        start = self.start
        return pl.ds(start if isinstance(start, int) else pl.multiple_of(start, LANES), self.size)


def chunking(columns):
    head = columns % WIDTH
    first = 1 if head else 0
    count = first + columns // WIDTH

    def chunk(index):
        if isinstance(index, int) and index < first:
            return Chunk(index, 0, head)
        return Chunk(index, head + (index - first) * WIDTH, WIDTH)

    return first, count, chunk


def gather_multiply(
    entry_count, gate_ref, up_ref, grad_ref, out_ref, factor_ref,
    held, grads, turned, gate_in, up_in, sums, total_out,
    local_sem, gx_send, gx_recv, gz_recv, gz_out, gz_in, gy_send, gy_recv,
    gs_send, gs_recv, gf_send, gf_recv,
    z_recv, z_out, z_in, zo_recv, zo_send, x_send, x_recv,
    sq_send, sq_recv, fa_send, fa_recv,
):
    rep = lax.axis_index("rep")
    fsdp = lax.axis_index("fsdp")
    tp = lax.axis_index("tp")
    rows, columns = gate_ref.shape
    half = grads.shape[1]
    n_tp = 4
    quarter = half // n_tp
    first, count, chunk = chunking(columns)
    other = 1 - fsdp
    side = rep // 2
    edge, near, far, far_edge = 3 * side, 1 + side, 2 - side, 3 - 3 * side
    is_edge = rep == edge
    inner = jnp.where(is_edge, near, far)
    sibling = tp + 1 - 2 * lax.rem(tp, 2)
    opposite = lax.rem(tp + 2, n_tp)
    past = lax.rem(sibling + 2, n_tp)

    def rows_of(r, s):
        return pl.ds(pl.multiple_of((r * 2 + s) * rows, rows), rows)

    def quarter_of(t):
        return pl.ds(pl.multiple_of(t * quarter, LANES), quarter)

    def remote(src, dst, send, recv, device):
        return pltpu.make_async_remote_copy(
            src_ref=src, dst_ref=dst, send_sem=send, recv_sem=recv,
            device_id=device, device_id_type=MESH,
        )

    loads = [
        pltpu.make_async_copy(gate_ref, gate_in, local_sem.at[0]),
        pltpu.make_async_copy(up_ref, up_in, local_sem.at[1]),
        pltpu.make_async_copy(
            grad_ref.at[:, pl.ds(pl.multiple_of(fsdp * half, LANES), half)],
            grads.at[rows_of(rep, fsdp), :], local_sem.at[2],
        ),
    ]
    for load in loads:
        load.start()

    barrier = pltpu.get_barrier_semaphore()
    for k in range(n_tp):
        if k:
            pl.semaphore_signal(
                barrier, inc=1, device_id={"tp": lax.rem(tp + k, n_tp)}, device_id_type=MESH
            )
        pl.semaphore_signal(
            barrier, inc=1, device_id={"fsdp": other, "tp": lax.rem(tp + k, n_tp)},
            device_id_type=MESH,
        )
    pl.semaphore_signal(barrier, inc=1, device_id={"rep": inner}, device_id_type=MESH)

    @pl.when(jnp.logical_not(is_edge))
    def _():
        pl.semaphore_signal(barrier, inc=1, device_id={"rep": edge}, device_id_type=MESH)

    with jax.named_scope("load"):
        loads[0].wait()
        loads[1].wait()

    @pl.loop(0, columns // LANES)
    def _(at):
        cols = pl.ds(pl.multiple_of(at * LANES, LANES), LANES)
        gate = gate_in[:, cols].astype(jnp.float32)
        held[rows_of(rep, fsdp), cols] = (
            jax.nn.silu(gate) * up_in[:, cols].astype(jnp.float32)
        ).astype(held.dtype)

    with jax.named_scope("barrier"):
        pl.semaphore_wait(barrier, 2 * n_tp + jnp.where(is_edge, 0, 1))

    def grad_across():
        src = grad_ref.at[:, pl.ds(pl.multiple_of(other * half + tp * quarter, LANES), quarter)]
        return remote(src, grads.at[rows_of(rep, fsdp), quarter_of(tp)], gx_send, gx_recv, {"fsdp": other})

    def grad_spot(r, s, t):
        return grads.at[rows_of(r, s), quarter_of(t)]

    def grad_hop(r, s, own, inward):
        spot = grad_spot(r, s, tp)
        src = spot
        if own:
            src = grad_ref.at[:, pl.ds(pl.multiple_of(fsdp * half + tp * quarter, LANES), quarter)]
        to = inner if inward else edge
        return remote(src, spot, (gz_in if inward else gz_out).at[r, s], gz_recv.at[r, s], {"rep": to})

    def grad_got(r, s):
        spot = grad_spot(r, s, tp)
        return remote(spot, spot, gz_in.at[r, s], gz_recv.at[r, s], {"rep": inner})

    def over_y(r, s, t):
        spot = grad_spot(r, s, t)
        return remote(spot, spot, gy_send.at[r, s], gy_recv.at[r, s], {"tp": opposite})

    def to_sibling(r, s, t):
        spot = grad_spot(r, s, t)
        return remote(spot, spot, gs_send.at[r, s], gs_recv.at[r, s], {"tp": sibling})

    def pass_sibling(r, s, t):
        spot = grad_spot(r, s, t)
        return remote(spot, spot, gf_send.at[r, s], gf_recv.at[r, s], {"tp": sibling})

    def hop(r, ch, inward):
        spot = held.at[rows_of(r, fsdp), ch.cols]
        to = inner if inward else edge
        return remote(spot, spot, (z_in if inward else z_out).at[r, ch.index], z_recv.at[r, ch.index], {"rep": to})

    def hop_got(r, ch):
        spot = held.at[rows_of(r, fsdp), ch.cols]
        return remote(spot, spot, z_in.at[r, ch.index], z_recv.at[r, ch.index], {"rep": inner})

    def hop_other(ch):
        spot = held.at[rows_of(edge, other), ch.cols]
        return remote(spot, spot, zo_send.at[ch.index], zo_recv.at[ch.index], {"rep": inner})

    def cross(r, ch):
        spot = held.at[rows_of(r, fsdp), ch.cols]
        return remote(spot, spot, x_send.at[r, ch.index], x_recv.at[r, ch.index], {"fsdp": other})

    def crossed(r, ch):
        spot = held.at[rows_of(r, other), ch.cols]
        return remote(spot, spot, x_send.at[r, ch.index], x_recv.at[r, ch.index], {"fsdp": other})

    def on_edge(act):
        pl.when(is_edge)(act)

    def on_middle(act):
        pl.when(jnp.logical_not(is_edge))(act)

    def chunks_from(low, high, act):
        while low < high and low < first:
            act(chunk(low))
            low += 1
        if low < high:
            @pl.loop(low, high)
            def _(index):
                act(chunk(index))

    grad_across().start()
    grad_hop(rep, fsdp, True, True).start()
    on_middle(lambda: grad_hop(rep, fsdp, True, False).start())

    chunks_from(0, count, lambda ch: cross(rep, ch).start())
    early = first + 1
    chunks_from(0, early, lambda ch: hop(rep, ch, True).start())
    on_middle(lambda: chunks_from(0, early, lambda ch: hop(rep, ch, False).start()))

    def share(r, s):
        over_y(r, s, tp).start()
        to_sibling(r, s, tp).start()

    def pass_on(r, s):
        over_y(r, s, opposite).wait_recv()
        pass_sibling(r, s, opposite).start()

    def settle(r, s):
        to_sibling(r, s, sibling).wait_recv()
        pass_sibling(r, s, past).wait_recv()

    tile = 256

    def turn(r):
        spot = pl.ds(pl.multiple_of(r * 2 * rows, 2 * rows), 2 * rows)

        @pl.loop(0, half // tile)
        def _(m):
            part = pl.ds(pl.multiple_of(m * tile, tile), tile)
            turned[part, spot] = grads[spot, part].T

    def take_own():
        grad_across().wait_recv()
        grad_hop(rep, other, False, True).start()
        on_middle(lambda: grad_hop(rep, other, False, False).start())
        share(rep, other)

    def perform(plan, acts):
        for at, (name, *args) in enumerate(plan):
            with jax.named_scope(f"{name}{at}"):
                acts[name](*args)

    loads[2].wait()

    def clear():
        sums[fsdp * n_tp + tp] = jnp.zeros(sums.shape[1:], sums.dtype)

    def multiply_tile(ch, m, squared):
        spot = pl.ds(pl.multiple_of(m * TILE, TILE), TILE)
        product = jnp.dot(turned[spot, :], held[:, ch.cols], preferred_element_type=jnp.float32)
        out_ref[spot, ch.cols] = product.astype(out_ref.dtype)
        if squared:
            squares = jnp.sum((product * product).reshape(TILE // 8, 8, ch.size), axis=0)
            total = squares[:, :LANES]
            for at in range(LANES, ch.size, LANES):
                total = total + squares[:, at:at + LANES]
            sums[fsdp * n_tp + tp] += total

    tiles = half // TILE

    def sweep(events, arrived, squared):
        places = [at * tiles // len(events) for at in range(len(events))]

        def step(index):
            ch, lagging = chunk(index), chunk(index - LAG)
            with jax.named_scope("arrived"):
                arrived(lagging)

            @pl.loop(0, tiles)
            def _(m):
                for at, (place, event) in enumerate(zip(places, events)):
                    def run():
                        with jax.named_scope(f"event{at}"):
                            event(ch)
                    pl.when(m == place)(run)
                with jax.named_scope("multiply"):
                    multiply_tile(lagging, m, squared)

        for index in range(LAG, LAG + first):
            step(index)
        pl.loop(LAG + first, count)(step)

        @pl.loop(count - LAG, count)
        def _(index):
            with jax.named_scope("arrived_last"):
                arrived(chunk(index))
            with jax.named_scope("multiply_last"):
                pl.loop(0, tiles)(lambda m: multiply_tile(chunk(index), m, squared))

    @on_edge
    def _():
        places = {"near": near, "far": far, "last": far_edge}
        sides = {"own": fsdp, "other": other}

        def take(name, s):
            grad_got(places[name], sides[s]).wait_recv()
            share(places[name], sides[s])

        def land(name, s, whole):
            r = rep if name == "rep" else places[name]
            pass_on(r, sides[s])
            settle_later.append((r, sides[s]))
            if whole:
                for pair in settle_later:
                    settle(*pair)
                settle_later.clear()
                turn(r)

        settle_later = []

        def relay(*indices):
            for index in indices:
                if index + early < count:
                    hop(rep, chunk(index + early), True).start()
                if index < count:
                    crossed(edge, chunk(index)).wait_recv()
                    hop_other(chunk(index)).start()

        def pull(r):
            def event(ch):
                hop_got(r, ch).wait_recv()
                cross(r, ch).start()
            return event

        events = [pull(near), pull(far), pull(far_edge)]

        def early_events(*indices):
            for index in indices:
                for event in events:
                    event(chunk(index))

        def batch(k):
            return range(k * count // 8, (k + 1) * count // 8)

        perform(
            [
                ("own",), ("take", "near", "own"), ("relay", *batch(0)),
                ("take", "near", "other"), ("land", "rep", "other", True), ("relay", *batch(1)),
                ("take", "far", "own"), ("land", "near", "own", False), ("relay", *batch(2)),
                ("take", "far", "other"), ("land", "near", "other", True), ("relay", *batch(3)),
                ("take", "last", "own"), ("land", "far", "own", False), ("relay", *batch(4)),
                ("take", "last", "other"), ("land", "far", "other", True), ("relay", *batch(5)),
                ("early", 0, 1), ("land", "last", "own", False), ("relay", *batch(6)),
                ("early", 2), ("land", "last", "other", True), ("relay", *batch(7)),
                ("early", 3),
            ],
            {"own": take_own, "take": take, "land": land, "relay": relay, "early": early_events},
        )

        def arrived(ch):
            for r in (near, far, far_edge):
                crossed(r, ch).wait_recv()

        sweep(events, arrived, False)

    @on_middle
    def _():
        places = {"edge": edge, "far": far, "last": far_edge}
        sides = {"own": fsdp, "other": other}

        def take(name, s):
            r, s = places[name], sides[s]
            grad_got(r, s).wait_recv()
            grad_hop(r, s, False, name == "edge").start()
            share(r, s)

        settle_later = {}

        def land(name, s):
            r = rep if name == "rep" else places[name]
            pass_on(r, sides[s])
            settle_later.setdefault(name, []).append((r, sides[s]))
            if len(settle_later[name]) == (1 if name == "rep" else 2):
                for pair in settle_later[name]:
                    settle(*pair)
                turn(r)

        def inward(*indices):
            for index in indices:
                ch = chunk(index)
                if index >= early:
                    hop(rep, ch, True).start()
                hop_got(edge, ch).wait_recv()
                hop(edge, ch, True).start()

        def outer(ch):
            hop(rep, ch, False).start()

            @pl.when(ch.index + AHEAD < count)
            def _():
                ahead = chunk(ch.index + AHEAD)
                hop(rep, ahead, True).start()
                hop_got(edge, ahead).wait_recv()
                hop(edge, ahead, True).start()

        def pull(r):
            def event(ch):
                hop_got(r, ch).wait_recv()
                hop(r, ch, False).start()
                cross(r, ch).start()
            return event

        pulls = [pull(far), pull(far_edge)]

        def early_events(*indices):
            for index in indices:
                if index >= early:
                    hop(rep, chunk(index), False).start()
                for event in pulls:
                    event(chunk(index))

        perform(
            [
                ("own",), ("take", "far", "own"), ("take", "edge", "own"),
                ("take", "edge", "other"), ("inward", *range(early)), ("take", "far", "other"),
                ("land", "rep", "other"), ("take", "last", "own"), ("land", "far", "own"),
                ("inward", *range(early, LAG)), ("take", "last", "other"), ("land", "edge", "own"),
                ("early", 0, 1), ("inward", *range(LAG, LAG + 2)), ("land", "edge", "other"),
                ("land", "far", "other"), ("early", 2), ("inward", LAG + 2), ("land", "last", "own"),
                ("early", 3), ("inward", LAG + 3), ("land", "last", "other"),
            ],
            {"own": take_own, "take": take, "land": land, "inward": inward, "early": early_events},
        )

        def arrived(ch):
            hop_other(ch).wait_recv()
            for r in (rep, far, far_edge):
                crossed(r, ch).wait_recv()

        clear()
        sweep([outer, *pulls], arrived, True)

        mine = fsdp * n_tp + tp
        peers = [(a, k) for a in range(2) for k in range(n_tp) if a or k]

        def exchange(at, towards):
            a, k = peers[at]
            to_side = other if a else fsdp
            to_tp = lax.rem(tp + (k if towards else n_tp - k), n_tp)
            spot = sums.at[mine if towards else to_side * n_tp + to_tp]
            return remote(spot, spot, sq_send.at[at], sq_recv.at[at], {"fsdp": to_side, "tp": to_tp})

        for at in range(len(peers)):
            exchange(at, True).start()
        with jax.named_scope("exchange"):
            for at in range(len(peers)):
                exchange(at, False).wait_recv()
        square_total = jnp.sum(jnp.sum(sums[...], axis=0), keepdims=True)
        factor = 1.0 / jnp.sqrt(square_total / entry_count + 1e-06)
        total_out[...] = jnp.broadcast_to(factor, total_out.shape)
        for at in range(len(peers)):
            exchange(at, True).wait_send()

    def tell():
        return remote(total_out, total_out, fa_send, fa_recv, {"rep": jnp.where(is_edge, near, edge)})

    on_middle(lambda: tell().start())
    with jax.named_scope("told"):
        on_edge(lambda: tell().wait_recv())
    factor_ref[...] = total_out[...]

    with jax.named_scope("sent"):
        grad_across().wait_send()

    def sent_shares(r, s):
        over_y(r, s, tp).wait_send()
        to_sibling(r, s, tp).wait_send()
        pass_sibling(r, s, opposite).wait_send()

    sent_shares(rep, other)
    grad_hop(rep, fsdp, True, True).wait_send()
    grad_hop(rep, other, False, True).wait_send()
    chunks_from(0, count, lambda ch: cross(rep, ch).wait_send())

    @on_edge
    def _():
        for r in (near, far, far_edge):
            for s in (fsdp, other):
                sent_shares(r, s)

        def sent(ch):
            hop(rep, ch, True).wait_send()
            hop_other(ch).wait_send()
            for r in (near, far, far_edge):
                cross(r, ch).wait_send()
        chunks_from(0, count, sent)

    @on_middle
    def _():
        tell().wait_send()
        for s, own in ((fsdp, True), (other, False)):
            grad_hop(rep, s, own, False).wait_send()
            grad_hop(edge, s, False, True).wait_send()
            for r in (edge, far, far_edge):
                sent_shares(r, s)
            for r in (far, far_edge):
                grad_hop(r, s, False, False).wait_send()

        def sent(ch):
            for r in (rep, edge):
                hop(r, ch, True).wait_send()
            for r in (rep, far, far_edge):
                hop(r, ch, False).wait_send()
            for r in (far, far_edge):
                cross(r, ch).wait_send()
        chunks_from(0, count, sent)


def by_kernel(n_rep, n_tp, entry_count, gate_pre, up_pre, out_grad):
    rows, columns = gate_pre.shape
    tokens = rows * n_rep * 2
    half = out_grad.shape[1] // 2
    count = chunking(columns)[1]
    dma = pltpu.SemaphoreType.DMA
    block, piece = dma((n_rep, 2)), dma((n_rep, count))
    return pl.pallas_call(
        functools.partial(gather_multiply, entry_count),
        out_shape=(
            pltpu.VMEM((half, columns), jnp.bfloat16),
            pltpu.VMEM((8, LANES), jnp.float32),
        ),
        in_specs=[pl.BlockSpec(memory_space=pl.ANY)] * 3,
        out_specs=(pl.BlockSpec(memory_space=pltpu.VMEM), pl.BlockSpec(memory_space=pltpu.VMEM)),
        scratch_shapes=[
            pltpu.VMEM((tokens, columns), jnp.bfloat16),
            pltpu.VMEM((tokens, half), jnp.bfloat16),
            pltpu.VMEM((half, tokens), jnp.bfloat16),
            pltpu.VMEM((rows, columns), jnp.bfloat16),
            pltpu.VMEM((rows, columns), jnp.bfloat16),
            pltpu.VMEM((2 * n_tp, 8, LANES), jnp.float32),
            pltpu.VMEM((8, LANES), jnp.float32),
            dma((3,)), dma, dma, block, block, block, block, block,
            block, block, block, block,
            piece, piece, piece, dma((count,)), dma((count,)), piece, piece,
            dma((2 * n_tp - 1,)), dma((2 * n_tp - 1,)), dma, dma,
        ],
        compiler_params=pltpu.CompilerParams(
            collective_id=0, has_side_effects=True, vmem_limit_bytes=VMEM_LIMIT * 3 // 4
        ),
    )(gate_pre, up_pre, out_grad)


def scale(summed, factors):
    half, columns = summed.shape
    rows = 128

    def body(summed_ref, factor_ref, out_ref, ready, sems):
        steps = half // rows
        depth = ready.shape[0]

        def leave(m):
            slot = lax.rem(m, depth)
            spot = pl.ds(pl.multiple_of(m * rows, rows), rows)
            return pltpu.make_async_copy(ready.at[slot], out_ref.at[spot, :], sems.at[slot])

        @pl.loop(0, steps)
        def _(m):
            slot = lax.rem(m, depth)
            spot = pl.ds(pl.multiple_of(m * rows, rows), rows)

            @pl.when(m >= depth)
            def _():
                leave(m - depth).wait()
            for at in range(0, columns, LANES):
                cols = pl.ds(at, LANES)
                scaled = summed_ref[spot, cols].astype(jnp.float32) * factor_ref[0:1, :]
                ready[slot, :, cols] = scaled.astype(ready.dtype)
            leave(m).start()

        @pl.loop(max(steps - depth, 0), steps)
        def _(m):
            leave(m).wait()

    return pl.pallas_call(
        body,
        out_shape=jax.ShapeDtypeStruct((half, columns), jnp.bfloat16),
        in_specs=[pl.BlockSpec(memory_space=pltpu.VMEM)] * 2,
        out_specs=pl.BlockSpec(memory_space=pl.ANY),
        scratch_shapes=[pltpu.VMEM((4, rows, columns), jnp.bfloat16), pltpu.SemaphoreType.DMA((4,))],
        compiler_params=pltpu.CompilerParams(vmem_limit_bytes=16 * 1024 * 1024),
    )(summed, factors)


def by_xla(gate_pre, up_pre, out_grad):
    hidden = (jax.nn.silu(gate_pre.astype(jnp.float32)) * up_pre.astype(jnp.float32)).astype(
        jnp.bfloat16
    )
    spread = lax.all_to_all(out_grad, "fsdp", split_axis=1, concat_axis=0, tiled=True)
    grad_rows = lax.all_gather(spread, "rep", axis=0, tiled=True)
    hidden_rows = lax.all_gather(hidden, ("rep", "fsdp"), axis=0, tiled=True)
    summed = lax.dot_general(
        grad_rows, hidden_rows, (((0,), (0,)), ((), ())), preferred_element_type=jnp.float32
    )
    return summed, jnp.sum(summed * summed)


def kernel_fits(n_rep, n_fsdp, n_tp, rows, columns, features):
    tokens, half = rows * n_rep * n_fsdp, features // n_fsdp
    held_bytes = 2 * (tokens * columns + 2 * tokens * half + half * columns + 2 * rows * columns)
    aligned = rows % 128 == 0 and columns % LANES == 0 and half % (LANES * n_tp) == 0
    shaped = (n_rep, n_fsdp, n_tp) == (4, 2, 4) and columns >= 12 * WIDTH
    return shaped and aligned and half % TILE == 0 and held_bytes < VMEM_LIMIT * 3 // 4


def solution(mesh):
    n_rep, n_fsdp, n_tp = (mesh.shape[axis] for axis in ("rep", "fsdp", "tp"))

    def on_device(gate_pre, up_pre, out_grad):
        half, columns = out_grad.shape[1] // n_fsdp, gate_pre.shape[1]
        entry_count = half * n_fsdp * columns * n_tp
        if kernel_fits(n_rep, n_fsdp, n_tp, *gate_pre.shape, out_grad.shape[1]):
            summed, factors = by_kernel(n_rep, n_tp, entry_count, gate_pre, up_pre, out_grad)
            return scale(summed, factors)
        summed, square_sum = by_xla(gate_pre, up_pre, out_grad)
        square_total = lax.psum(square_sum, ("fsdp", "tp"))
        factor = 1.0 / jnp.sqrt(square_total / entry_count + 1e-06)
        return (summed * factor).astype(jnp.bfloat16)

    return jax.shard_map(
        on_device,
        mesh=mesh,
        in_specs=(P(("rep", "fsdp"), "tp"), P(("rep", "fsdp"), "tp"), P(("rep", "fsdp"), None)),
        out_specs=P("fsdp", "tp"),
        check_vma=False,
    )
```

```python
import functools

import jax
import jax.numpy as jnp
from jax import lax
from jax.experimental import pallas as pl
from jax.experimental.pallas import tpu as pltpu
from jax.sharding import PartitionSpec as P

MESH = pl.DeviceIdType.MESH
LANES = 128
VMEM_LIMIT = 60 * 1024 * 1024
WIDTH = 256
TILE = 1024
LAG = 4
AHEAD = 4
FILL = 3
EXTRA = (6, 10)


class Chunk:
    def __init__(self, index, start, size):
        self.index, self.start, self.size = index, start, size

    @property
    def cols(self):
        start = self.start
        return pl.ds(start if isinstance(start, int) else pl.multiple_of(start, LANES), self.size)


def chunking(columns):
    full, rest = columns // WIDTH, columns % WIDTH

    def chunk(index):
        if isinstance(index, int) and index == full:
            return Chunk(index, full * WIDTH, rest)
        return Chunk(index, index * WIDTH, WIDTH)

    return full, full + (1 if rest else 0), chunk


def gather_multiply(
    entry_count, gate_ref, up_ref, grad_ref, out_ref, factor_ref,
    held, grads, turned, gate_in, up_in, across_in, sums, total_out,
    local_sem, gx_send, gx_recv, gz_recv, gz_out, gz_in, gy_send, gy_recv,
    gs_send, gs_recv, gf_send, gf_recv,
    z_recv, z_out, z_in, zo_recv, zo_send, ze_recv, ze_send, x_send, x_recv,
    sq_send, sq_recv, fa_send, fa_recv,
):
    rep = lax.axis_index("rep")
    fsdp = lax.axis_index("fsdp")
    tp = lax.axis_index("tp")
    rows, columns = gate_ref.shape
    half = grads.shape[1]
    n_tp = 4
    quarter = half // n_tp
    full, count, chunk = chunking(columns)
    other = 1 - fsdp
    side = rep // 2
    edge, near, far, far_edge = 3 * side, 1 + side, 2 - side, 3 - 3 * side
    is_edge = rep == edge
    inner = jnp.where(is_edge, near, far)
    sibling = tp + 1 - 2 * lax.rem(tp, 2)
    opposite = lax.rem(tp + 2, n_tp)
    past = lax.rem(sibling + 2, n_tp)

    def rows_of(r, s):
        return pl.ds(pl.multiple_of((r * 2 + s) * rows, rows), rows)

    def quarter_of(t):
        return pl.ds(pl.multiple_of(t * quarter, LANES), quarter)

    def remote(src, dst, send, recv, device):
        return pltpu.make_async_remote_copy(
            src_ref=src, dst_ref=dst, send_sem=send, recv_sem=recv,
            device_id=device, device_id_type=MESH,
        )

    loads = [
        pltpu.make_async_copy(gate_ref, gate_in, local_sem.at[0]),
        pltpu.make_async_copy(up_ref, up_in, local_sem.at[1]),
        pltpu.make_async_copy(
            grad_ref.at[:, pl.ds(pl.multiple_of(fsdp * half, LANES), half)],
            grads.at[rows_of(rep, fsdp), :], local_sem.at[2],
        ),
        pltpu.make_async_copy(
            grad_ref.at[:, pl.ds(pl.multiple_of(other * half + tp * quarter, LANES), quarter)],
            across_in, local_sem.at[3],
        ),
    ]
    for load in loads:
        load.start()

    barrier = pltpu.get_barrier_semaphore()
    for peer in ({"fsdp": other}, {"tp": sibling}, {"tp": opposite}):
        pl.semaphore_signal(barrier, inc=1, device_id=peer, device_id_type=MESH)
    pl.semaphore_signal(barrier, inc=1, device_id={"rep": inner}, device_id_type=MESH)

    @pl.when(jnp.logical_not(is_edge))
    def _():
        pl.semaphore_signal(barrier, inc=1, device_id={"rep": edge}, device_id_type=MESH)

    with jax.named_scope("load"):
        for load in loads:
            load.wait()

    @pl.loop(0, columns // LANES)
    def _(at):
        cols = pl.ds(pl.multiple_of(at * LANES, LANES), LANES)
        gate = gate_in[:, cols].astype(jnp.float32)
        held[rows_of(rep, fsdp), cols] = (
            jax.nn.silu(gate) * up_in[:, cols].astype(jnp.float32)
        ).astype(held.dtype)

    with jax.named_scope("barrier"):
        pl.semaphore_wait(barrier, 4 + jnp.where(is_edge, 0, 1))

    def grad_across():
        return remote(across_in, grads.at[rows_of(rep, fsdp), quarter_of(tp)], gx_send, gx_recv, {"fsdp": other})

    def grad_spot(r, s, t):
        return grads.at[rows_of(r, s), quarter_of(t)]

    def grad_hop(r, s, inward):
        spot = grad_spot(r, s, tp)
        to = inner if inward else edge
        return remote(spot, spot, (gz_in if inward else gz_out).at[r, s], gz_recv.at[r, s], {"rep": to})

    def grad_got(r, s):
        spot = grad_spot(r, s, tp)
        return remote(spot, spot, gz_in.at[r, s], gz_recv.at[r, s], {"rep": inner})

    def over_y(r, s, t):
        spot = grad_spot(r, s, t)
        return remote(spot, spot, gy_send.at[r, s], gy_recv.at[r, s], {"tp": opposite})

    def to_sibling(r, s, t):
        spot = grad_spot(r, s, t)
        return remote(spot, spot, gs_send.at[r, s], gs_recv.at[r, s], {"tp": sibling})

    def pass_sibling(r, s, t):
        spot = grad_spot(r, s, t)
        return remote(spot, spot, gf_send.at[r, s], gf_recv.at[r, s], {"tp": sibling})

    def hop(r, ch, inward):
        spot = held.at[rows_of(r, fsdp), ch.cols]
        to = inner if inward else edge
        return remote(spot, spot, (z_in if inward else z_out).at[r], z_recv.at[r, ch.index], {"rep": to})

    def hop_got(r, ch):
        spot = held.at[rows_of(r, fsdp), ch.cols]
        return remote(spot, spot, z_in.at[r], z_recv.at[r, ch.index], {"rep": inner})

    def hop_other(ch):
        spot = held.at[rows_of(edge, other), ch.cols]
        return remote(spot, spot, zo_send, zo_recv.at[ch.index], {"rep": inner})

    def cross(r, ch):
        spot = held.at[rows_of(r, fsdp), ch.cols]
        return remote(spot, spot, x_send.at[r], x_recv.at[r, ch.index], {"fsdp": other})

    def crossed(r, ch):
        spot = held.at[rows_of(r, other), ch.cols]
        return remote(spot, spot, x_send.at[r], x_recv.at[r, ch.index], {"fsdp": other})

    def hop_extra(ch):
        spot = held.at[rows_of(near, other), ch.cols]
        return remote(spot, spot, ze_send, ze_recv.at[ch.index], {"rep": jnp.where(is_edge, near, edge)})

    def all_sent(r, s, width, send):
        spot = held.at[rows_of(r, s), pl.ds(0, width)]
        remote(spot, spot, send, gx_recv, {"fsdp": other}).wait_send()

    def when_extra(ch, act, otherwise=None):
        if isinstance(ch.index, int):
            if ch.index in EXTRA:
                act()
            elif otherwise is not None:
                otherwise()
            return
        hit = ch.index == EXTRA[0]
        for index in EXTRA[1:]:
            hit = jnp.logical_or(hit, ch.index == index)
        pl.when(hit)(act)
        if otherwise is not None:
            pl.when(jnp.logical_not(hit))(otherwise)

    def on_edge(act):
        pl.when(is_edge)(act)

    def on_middle(act):
        pl.when(jnp.logical_not(is_edge))(act)

    def chunks_from(low, high, act):
        if low < min(high, full):
            @pl.loop(low, min(high, full))
            def _(index):
                act(chunk(index))
        if full < count == high:
            act(chunk(full))

    grad_across().start()
    grad_hop(rep, fsdp, True).start()
    on_middle(lambda: grad_hop(rep, fsdp, False).start())

    chunks_from(0, count, lambda ch: cross(rep, ch).start())
    early = 2
    chunks_from(0, early, lambda ch: hop(rep, ch, True).start())
    on_middle(lambda: chunks_from(0, early, lambda ch: hop(rep, ch, False).start()))

    def share(r, s):
        over_y(r, s, tp).start()
        to_sibling(r, s, tp).start()

    def pass_on(r, s):
        over_y(r, s, opposite).wait_recv()
        pass_sibling(r, s, opposite).start()

    def settle(r, s):
        to_sibling(r, s, sibling).wait_recv()
        pass_sibling(r, s, past).wait_recv()

    tile = 256

    def turn(r):
        spot = pl.ds(pl.multiple_of(r * 2 * rows, 2 * rows), 2 * rows)

        @pl.loop(0, half // tile)
        def _(m):
            part = pl.ds(pl.multiple_of(m * tile, tile), tile)
            turned[part, spot] = grads[spot, part].T

    def take_own():
        grad_across().wait_recv()
        grad_hop(rep, other, True).start()
        on_middle(lambda: grad_hop(rep, other, False).start())
        share(rep, other)

    def perform(plan, acts):
        for at, (name, *args) in enumerate(plan):
            with jax.named_scope(f"{name}{at}"):
                acts[name](*args)

    def sent_shares(r, s):
        over_y(r, s, tp).wait_send()
        to_sibling(r, s, tp).wait_send()
        pass_sibling(r, s, opposite).wait_send()

    def sent_first():
        grad_across().wait_send()
        sent_shares(rep, other)
        grad_hop(rep, fsdp, True).wait_send()
        grad_hop(rep, other, True).wait_send()
        all_sent(rep, fsdp, columns, x_send.at[rep])
        all_sent(rep, fsdp, columns, z_in.at[rep])

    def clear():
        sums[fsdp * n_tp + tp] = jnp.zeros(sums.shape[1:], sums.dtype)

    def multiply_tile(ch, m, squared):
        spot = pl.ds(pl.multiple_of(m * TILE, TILE), TILE)
        product = jnp.dot(turned[spot, :], held[:, ch.cols], preferred_element_type=jnp.float32)
        out_ref[spot, ch.cols] = product.astype(out_ref.dtype)
        if squared:
            squares = jnp.sum((product * product).reshape(TILE // 8, 8, ch.size), axis=0)
            total = squares[:, :LANES]
            for at in range(LANES, ch.size, LANES):
                total = total + squares[:, at:at + LANES]
            sums[fsdp * n_tp + tp] += total

    tiles = half // TILE

    def sweep(events, arrived, between, squared):
        places = [at * tiles // len(events) for at in range(len(events))]

        def step(index):
            ch, lagging = chunk(index), chunk(index - LAG)
            with jax.named_scope("arrived"):
                arrived(lagging)

            @pl.loop(0, tiles)
            def _(m):
                for at, (place, event) in enumerate(zip(places, events)):
                    def run():
                        with jax.named_scope(f"event{at}"):
                            event(ch)
                    pl.when(m == place)(run)
                with jax.named_scope("multiply"):
                    multiply_tile(lagging, m, squared)

        pl.loop(LAG, full - 1)(step)
        between()
        for index in range(full - 1, count):
            step(index)

        def finish(ch):
            with jax.named_scope("arrived_last"):
                arrived(ch)
            with jax.named_scope("multiply_last"):
                pl.loop(0, tiles)(lambda m: multiply_tile(ch, m, squared))
        chunks_from(count - LAG, count, finish)

    @on_edge
    def _():
        places = {"near": near, "far": far, "last": far_edge}
        sides = {"own": fsdp, "other": other}

        def take(name, s):
            grad_got(places[name], sides[s]).wait_recv()
            share(places[name], sides[s])

        def land(name, s, whole):
            r = rep if name == "rep" else places[name]
            pass_on(r, sides[s])
            settle_later.append((r, sides[s]))
            if whole:
                for pair in settle_later:
                    settle(*pair)
                settle_later.clear()
                turn(r)

        settle_later = []

        def relay(*indices):
            for index in indices:
                if index + early < count:
                    hop(rep, chunk(index + early), True).start()
                if index < count:
                    crossed(edge, chunk(index)).wait_recv()
                    hop_other(chunk(index)).start()

        def pull(r):
            def event(ch):
                hop_got(r, ch).wait_recv()
                cross(r, ch).start()
            return event

        def pull_near(ch):
            hop_got(near, ch).wait_recv()
            when_extra(ch, lambda: None, lambda: cross(near, ch).start())

        events = [pull_near, pull(far), pull(far_edge)]

        def early_events(*indices):
            for index in indices:
                for event in events:
                    event(chunk(index))

        def batch(k):
            return range(k * count // 8, (k + 1) * count // 8)

        perform(
            [
                ("own",), ("take", "near", "own"), ("relay", *batch(0)),
                ("take", "near", "other"), ("land", "rep", "other", True), ("relay", *batch(1)),
                ("take", "far", "own"), ("land", "near", "own", False), ("relay", *batch(2)),
                ("take", "far", "other"), ("land", "near", "other", True), ("relay", *batch(3)),
                ("take", "last", "own"), ("land", "far", "own", False), ("relay", *batch(4)),
                ("take", "last", "other"), ("land", "far", "other", True), ("relay", *batch(5)),
                ("early", 0, 1), ("land", "last", "own", False), ("relay", *batch(6)),
                ("early", 2), ("land", "last", "other", True), ("relay", *batch(7)),
                ("early", 3),
            ],
            {"own": take_own, "take": take, "land": land, "relay": relay, "early": early_events},
        )

        def arrived(ch):
            when_extra(
                ch, lambda: hop_extra(ch).wait_recv(), lambda: crossed(near, ch).wait_recv()
            )
            for r in (far, far_edge):
                crossed(r, ch).wait_recv()

        def between():
            sent_first()
            for r in (near, far, far_edge):
                for s in (fsdp, other):
                    sent_shares(r, s)
            all_sent(rep, other, columns, zo_send)

        sweep(events, arrived, between, False)
        all_sent(near, fsdp, columns - len(EXTRA) * WIDTH, x_send.at[near])
        for r in (far, far_edge):
            all_sent(r, fsdp, columns, x_send.at[r])

    @on_middle
    def _():
        places = {"edge": edge, "far": far, "last": far_edge}
        sides = {"own": fsdp, "other": other}

        def take(name, s):
            r, s = places[name], sides[s]
            grad_got(r, s).wait_recv()
            grad_hop(r, s, name == "edge").start()
            share(r, s)

        settle_later = {}

        def land(name, s):
            r = rep if name == "rep" else places[name]
            pass_on(r, sides[s])
            settle_later.setdefault(name, []).append((r, sides[s]))
            if len(settle_later[name]) == (1 if name == "rep" else 2):
                for pair in settle_later[name]:
                    settle(*pair)
                turn(r)

        def inward(*indices):
            for index in indices:
                ch = chunk(index)
                if not isinstance(index, int) or index >= early:
                    hop(rep, ch, True).start()
                hop_got(edge, ch).wait_recv()
                hop(edge, ch, True).start()

        def fill(*indices):
            for index in indices:
                hop(rep, chunk(index), False).start()

        def outer(ch):
            if isinstance(ch.index, int):
                if ch.index + FILL < count:
                    fill(ch.index + FILL)
            else:
                pl.when(ch.index + FILL < full)(lambda: fill(ch.index + FILL))
                if full < count:
                    pl.when(ch.index + FILL == full)(lambda: fill(full))
            when_extra(ch, lambda: (crossed(rep, ch).wait_recv(), hop_extra(ch).start()) and None)
            follow(ch.index + AHEAD)

        def follow(index):
            if isinstance(index, int):
                if index < count:
                    inward(index)
                return
            pl.when(index < full)(lambda: inward(index))
            if full < count:
                pl.when(index == full)(lambda: inward(full))

        def pull(r):
            def event(ch):
                hop_got(r, ch).wait_recv()
                hop(r, ch, False).start()
                cross(r, ch).start()
            return event

        pulls = [pull(far), pull(far_edge)]

        def early_events(*indices):
            for index in indices:
                if index >= early:
                    fill(index + FILL)
                for event in pulls:
                    event(chunk(index))

        perform(
            [
                ("own",), ("take", "far", "own"), ("fill", early), ("take", "edge", "own"),
                ("take", "edge", "other"), ("inward", *range(early)), ("take", "far", "other"),
                ("fill", early + 1), ("land", "rep", "other"), ("take", "last", "own"),
                ("fill", early + 2), ("land", "far", "own"),
                ("inward", *range(early, LAG)), ("take", "last", "other"), ("land", "edge", "own"),
                ("early", 0, 1), ("inward", *range(LAG, LAG + 2)), ("land", "edge", "other"),
                ("land", "far", "other"), ("early", 2), ("inward", LAG + 2), ("land", "last", "own"),
                ("early", 3), ("inward", LAG + 3), ("land", "last", "other"),
            ],
            {"own": take_own, "take": take, "land": land, "inward": inward, "early": early_events, "fill": fill},
        )

        def arrived(ch):
            hop_other(ch).wait_recv()
            when_extra(ch, lambda: None, lambda: crossed(rep, ch).wait_recv())
            for r in (far, far_edge):
                crossed(r, ch).wait_recv()

        clear()
        sweep([outer, *pulls], arrived, lambda: None, True)

        mine = fsdp * n_tp + tp
        peers = [(a, k) for a in range(2) for k in range(n_tp) if a or k]

        def exchange(at, towards):
            a, k = peers[at]
            to_side = other if a else fsdp
            to_tp = lax.rem(tp + (k if towards else n_tp - k), n_tp)
            spot = sums.at[mine if towards else to_side * n_tp + to_tp]
            return remote(spot, spot, sq_send.at[at], sq_recv.at[at], {"fsdp": to_side, "tp": to_tp})

        for at in range(len(peers)):
            exchange(at, True).start()
        with jax.named_scope("exchange"):
            for at in range(len(peers)):
                exchange(at, False).wait_recv()
        square_total = jnp.sum(jnp.sum(sums[...], axis=0), keepdims=True)
        factor = 1.0 / jnp.sqrt(square_total / entry_count + 1e-06)
        total_out[...] = jnp.broadcast_to(factor, total_out.shape)
        for at in range(len(peers)):
            exchange(at, True).wait_send()

    def tell():
        return remote(total_out, total_out, fa_send, fa_recv, {"rep": jnp.where(is_edge, near, edge)})

    on_middle(lambda: tell().start())
    with jax.named_scope("told"):
        on_edge(lambda: tell().wait_recv())
    factor_ref[...] = total_out[...]

    @on_middle
    def _():
        tell().wait_send()
        sent_first()
        for s in (fsdp, other):
            grad_hop(rep, s, False).wait_send()
            grad_hop(edge, s, True).wait_send()
            for r in (edge, far, far_edge):
                sent_shares(r, s)
            for r in (far, far_edge):
                grad_hop(r, s, False).wait_send()
        all_sent(edge, fsdp, columns, z_in.at[edge])
        for r in (rep, far, far_edge):
            all_sent(r, fsdp, columns, z_out.at[r])
        for r in (far, far_edge):
            all_sent(r, fsdp, columns, x_send.at[r])
        all_sent(rep, other, len(EXTRA) * WIDTH, ze_send)


def by_kernel(n_rep, n_tp, entry_count, gate_pre, up_pre, out_grad):
    rows, columns = gate_pre.shape
    tokens = rows * n_rep * 2
    half = out_grad.shape[1] // 2
    quarter = half // n_tp
    count = chunking(columns)[1]
    dma = pltpu.SemaphoreType.DMA
    block, piece, line = dma((n_rep, 2)), dma((n_rep, count)), dma((count,))
    whole = dma((n_rep,))
    return pl.pallas_call(
        functools.partial(gather_multiply, entry_count),
        out_shape=(
            pltpu.VMEM((half, columns), jnp.bfloat16),
            pltpu.VMEM((8, LANES), jnp.float32),
        ),
        in_specs=[pl.BlockSpec(memory_space=pl.ANY)] * 3,
        out_specs=(pl.BlockSpec(memory_space=pltpu.VMEM), pl.BlockSpec(memory_space=pltpu.VMEM)),
        scratch_shapes=[
            pltpu.VMEM((tokens, columns), jnp.bfloat16),
            pltpu.VMEM((tokens, half), jnp.bfloat16),
            pltpu.VMEM((half, tokens), jnp.bfloat16),
            pltpu.VMEM((rows, columns), jnp.bfloat16),
            pltpu.VMEM((rows, columns), jnp.bfloat16),
            pltpu.VMEM((rows, quarter), jnp.bfloat16),
            pltpu.VMEM((2 * n_tp, 8, LANES), jnp.float32),
            pltpu.VMEM((8, LANES), jnp.float32),
            dma((4,)), dma, dma, block, block, block, block, block,
            block, block, block, block,
            piece, whole, whole, line, dma, line, dma, whole, piece,
            dma((2 * n_tp - 1,)), dma((2 * n_tp - 1,)), dma, dma,
        ],
        compiler_params=pltpu.CompilerParams(
            collective_id=0, has_side_effects=True, vmem_limit_bytes=VMEM_LIMIT * 3 // 4
        ),
    )(gate_pre, up_pre, out_grad)


def scale(summed, factors):
    half, columns = summed.shape
    rows = 128

    def body(summed_ref, factor_ref, out_ref, ready, sems):
        steps = half // rows
        depth = ready.shape[0]

        def leave(m):
            slot = lax.rem(m, depth)
            spot = pl.ds(pl.multiple_of(m * rows, rows), rows)
            return pltpu.make_async_copy(ready.at[slot], out_ref.at[spot, :], sems.at[slot])

        @pl.loop(0, steps)
        def _(m):
            slot = lax.rem(m, depth)
            spot = pl.ds(pl.multiple_of(m * rows, rows), rows)

            @pl.when(m >= depth)
            def _():
                leave(m - depth).wait()
            for at in range(0, columns, LANES):
                cols = pl.ds(at, LANES)
                scaled = summed_ref[spot, cols].astype(jnp.float32) * factor_ref[0:1, :]
                ready[slot, :, cols] = scaled.astype(ready.dtype)
            leave(m).start()

        @pl.loop(max(steps - depth, 0), steps)
        def _(m):
            leave(m).wait()

    return pl.pallas_call(
        body,
        out_shape=jax.ShapeDtypeStruct((half, columns), jnp.bfloat16),
        in_specs=[pl.BlockSpec(memory_space=pltpu.VMEM)] * 2,
        out_specs=pl.BlockSpec(memory_space=pl.ANY),
        scratch_shapes=[pltpu.VMEM((4, rows, columns), jnp.bfloat16), pltpu.SemaphoreType.DMA((4,))],
        compiler_params=pltpu.CompilerParams(vmem_limit_bytes=16 * 1024 * 1024),
    )(summed, factors)


def by_xla(gate_pre, up_pre, out_grad):
    hidden = (jax.nn.silu(gate_pre.astype(jnp.float32)) * up_pre.astype(jnp.float32)).astype(
        jnp.bfloat16
    )
    spread = lax.all_to_all(out_grad, "fsdp", split_axis=1, concat_axis=0, tiled=True)
    grad_rows = lax.all_gather(spread, "rep", axis=0, tiled=True)
    hidden_rows = lax.all_gather(hidden, ("rep", "fsdp"), axis=0, tiled=True)
    summed = lax.dot_general(
        grad_rows, hidden_rows, (((0,), (0,)), ((), ())), preferred_element_type=jnp.float32
    )
    return summed, jnp.sum(summed * summed)


def kernel_fits(n_rep, n_fsdp, n_tp, rows, columns, features):
    tokens, half = rows * n_rep * n_fsdp, features // n_fsdp
    held_bytes = 2 * (tokens * columns + 2 * tokens * half + half * columns + 2 * rows * columns)
    aligned = rows % 128 == 0 and columns % LANES == 0 and half % (LANES * n_tp) == 0
    shaped = (n_rep, n_fsdp, n_tp) == (4, 2, 4) and columns >= 12 * WIDTH
    return shaped and aligned and half % TILE == 0 and held_bytes < VMEM_LIMIT * 3 // 4


def solution(mesh):
    n_rep, n_fsdp, n_tp = (mesh.shape[axis] for axis in ("rep", "fsdp", "tp"))

    def on_device(gate_pre, up_pre, out_grad):
        half, columns = out_grad.shape[1] // n_fsdp, gate_pre.shape[1]
        entry_count = half * n_fsdp * columns * n_tp
        if kernel_fits(n_rep, n_fsdp, n_tp, *gate_pre.shape, out_grad.shape[1]):
            summed, factors = by_kernel(n_rep, n_tp, entry_count, gate_pre, up_pre, out_grad)
            return scale(summed, factors)
        summed, square_sum = by_xla(gate_pre, up_pre, out_grad)
        square_total = lax.psum(square_sum, ("fsdp", "tp"))
        factor = 1.0 / jnp.sqrt(square_total / entry_count + 1e-06)
        return (summed * factor).astype(jnp.bfloat16)

    return jax.shard_map(
        on_device,
        mesh=mesh,
        in_specs=(P(("rep", "fsdp"), "tp"), P(("rep", "fsdp"), "tp"), P(("rep", "fsdp"), None)),
        out_specs=P("fsdp", "tp"),
        check_vma=False,
    )
```

```python
import functools

import jax
import jax.numpy as jnp
from jax import lax
from jax.experimental import pallas as pl
from jax.experimental.pallas import tpu as pltpu
from jax.sharding import PartitionSpec as P

MESH = pl.DeviceIdType.MESH
LANES = 128
VMEM_LIMIT = 60 * 1024 * 1024
WIDTH = 256
TILE = 1024
LAG = 4
AHEAD = 4
FILL = 3
EXTRA = (8,)


class Chunk:
    def __init__(self, index, start, size):
        self.index, self.start, self.size = index, start, size

    @property
    def cols(self):
        start = self.start
        return pl.ds(start if isinstance(start, int) else pl.multiple_of(start, LANES), self.size)


def chunking(columns):
    full, rest = columns // WIDTH, columns % WIDTH

    def chunk(index):
        if isinstance(index, int) and index == full:
            return Chunk(index, full * WIDTH, rest)
        return Chunk(index, index * WIDTH, WIDTH)

    return full, full + (1 if rest else 0), chunk


def gather_multiply(
    entry_count, gate_ref, up_ref, grad_ref, out_ref, factor_ref,
    held, grads, turned, gate_in, up_in, across_in, sums, total_out,
    local_sem, gx_send, gx_recv, gz_recv, gz_out, gz_in, gy_send, gy_recv,
    gs_send, gs_recv, gf_send, gf_recv,
    z_recv, z_out, z_in, zo_recv, zo_send, ze_recv, ze_send, x_send, x_recv,
    sq_send, sq_recv, fa_send, fa_recv,
):
    rep = lax.axis_index("rep")
    fsdp = lax.axis_index("fsdp")
    tp = lax.axis_index("tp")
    rows, columns = gate_ref.shape
    half = grads.shape[1]
    n_tp = 4
    quarter = half // n_tp
    full, count, chunk = chunking(columns)
    other = 1 - fsdp
    side = rep // 2
    edge, near, far, far_edge = 3 * side, 1 + side, 2 - side, 3 - 3 * side
    is_edge = rep == edge
    inner = jnp.where(is_edge, near, far)
    sibling = tp + 1 - 2 * lax.rem(tp, 2)
    opposite = lax.rem(tp + 2, n_tp)
    past = lax.rem(sibling + 2, n_tp)

    def rows_of(r, s):
        return pl.ds(pl.multiple_of((r * 2 + s) * rows, rows), rows)

    def quarter_of(t):
        return pl.ds(pl.multiple_of(t * quarter, LANES), quarter)

    def remote(src, dst, send, recv, device):
        return pltpu.make_async_remote_copy(
            src_ref=src, dst_ref=dst, send_sem=send, recv_sem=recv,
            device_id=device, device_id_type=MESH,
        )

    loads = [
        pltpu.make_async_copy(gate_ref, gate_in, local_sem.at[0]),
        pltpu.make_async_copy(up_ref, up_in, local_sem.at[1]),
        pltpu.make_async_copy(
            grad_ref.at[:, pl.ds(pl.multiple_of(fsdp * half, LANES), half)],
            grads.at[rows_of(rep, fsdp), :], local_sem.at[2],
        ),
        pltpu.make_async_copy(
            grad_ref.at[:, pl.ds(pl.multiple_of(other * half + tp * quarter, LANES), quarter)],
            across_in, local_sem.at[3],
        ),
    ]
    for load in loads:
        load.start()

    barrier = pltpu.get_barrier_semaphore()
    for peer in ({"fsdp": other}, {"tp": sibling}, {"tp": opposite}):
        pl.semaphore_signal(barrier, inc=1, device_id=peer, device_id_type=MESH)
    pl.semaphore_signal(barrier, inc=1, device_id={"rep": inner}, device_id_type=MESH)

    @pl.when(jnp.logical_not(is_edge))
    def _():
        pl.semaphore_signal(barrier, inc=1, device_id={"rep": edge}, device_id_type=MESH)

    with jax.named_scope("load"):
        for load in loads:
            load.wait()

    @pl.loop(0, columns // LANES)
    def _(at):
        cols = pl.ds(pl.multiple_of(at * LANES, LANES), LANES)
        gate = gate_in[:, cols].astype(jnp.float32)
        held[rows_of(rep, fsdp), cols] = (
            jax.nn.silu(gate) * up_in[:, cols].astype(jnp.float32)
        ).astype(held.dtype)

    with jax.named_scope("barrier"):
        pl.semaphore_wait(barrier, 4 + jnp.where(is_edge, 0, 1))

    def grad_across():
        return remote(across_in, grads.at[rows_of(rep, fsdp), quarter_of(tp)], gx_send, gx_recv, {"fsdp": other})

    def grad_spot(r, s, t):
        return grads.at[rows_of(r, s), quarter_of(t)]

    def grad_hop(r, s, inward):
        spot = grad_spot(r, s, tp)
        to = inner if inward else edge
        return remote(spot, spot, (gz_in if inward else gz_out).at[r, s], gz_recv.at[r, s], {"rep": to})

    def grad_got(r, s):
        spot = grad_spot(r, s, tp)
        return remote(spot, spot, gz_in.at[r, s], gz_recv.at[r, s], {"rep": inner})

    def over_y(r, s, t):
        spot = grad_spot(r, s, t)
        return remote(spot, spot, gy_send.at[r, s], gy_recv.at[r, s], {"tp": opposite})

    def to_sibling(r, s, t):
        spot = grad_spot(r, s, t)
        return remote(spot, spot, gs_send.at[r, s], gs_recv.at[r, s], {"tp": sibling})

    def pass_sibling(r, s, t):
        spot = grad_spot(r, s, t)
        return remote(spot, spot, gf_send.at[r, s], gf_recv.at[r, s], {"tp": sibling})

    def hop(r, ch, inward):
        spot = held.at[rows_of(r, fsdp), ch.cols]
        to = inner if inward else edge
        return remote(spot, spot, (z_in if inward else z_out).at[r], z_recv.at[r, ch.index], {"rep": to})

    def hop_got(r, ch):
        spot = held.at[rows_of(r, fsdp), ch.cols]
        return remote(spot, spot, z_in.at[r], z_recv.at[r, ch.index], {"rep": inner})

    def hop_other(ch):
        spot = held.at[rows_of(edge, other), ch.cols]
        return remote(spot, spot, zo_send, zo_recv.at[ch.index], {"rep": inner})

    def cross(r, ch):
        spot = held.at[rows_of(r, fsdp), ch.cols]
        return remote(spot, spot, x_send.at[r], x_recv.at[r, ch.index], {"fsdp": other})

    def crossed(r, ch):
        spot = held.at[rows_of(r, other), ch.cols]
        return remote(spot, spot, x_send.at[r], x_recv.at[r, ch.index], {"fsdp": other})

    def hop_extra(ch):
        spot = held.at[rows_of(near, other), ch.cols]
        return remote(spot, spot, ze_send, ze_recv.at[ch.index], {"rep": jnp.where(is_edge, near, edge)})

    def all_sent(r, s, width, send):
        spot = held.at[rows_of(r, s), pl.ds(0, width)]
        remote(spot, spot, send, gx_recv, {"fsdp": other}).wait_send()

    def when_extra(ch, act, otherwise=None):
        if isinstance(ch.index, int):
            if ch.index in EXTRA:
                act()
            elif otherwise is not None:
                otherwise()
            return
        hit = ch.index == EXTRA[0]
        for index in EXTRA[1:]:
            hit = jnp.logical_or(hit, ch.index == index)
        pl.when(hit)(act)
        if otherwise is not None:
            pl.when(jnp.logical_not(hit))(otherwise)

    def on_edge(act):
        pl.when(is_edge)(act)

    def on_middle(act):
        pl.when(jnp.logical_not(is_edge))(act)

    def chunks_from(low, high, act):
        if low < min(high, full):
            @pl.loop(low, min(high, full))
            def _(index):
                act(chunk(index))
        if full < count == high:
            act(chunk(full))

    grad_across().start()
    grad_hop(rep, fsdp, True).start()
    on_middle(lambda: grad_hop(rep, fsdp, False).start())

    chunks_from(0, count, lambda ch: cross(rep, ch).start())
    early = 2
    chunks_from(0, early, lambda ch: hop(rep, ch, True).start())
    on_middle(lambda: chunks_from(0, early, lambda ch: hop(rep, ch, False).start()))

    def share(r, s):
        over_y(r, s, tp).start()
        to_sibling(r, s, tp).start()

    def pass_on(r, s):
        over_y(r, s, opposite).wait_recv()
        pass_sibling(r, s, opposite).start()

    def settle(r, s):
        to_sibling(r, s, sibling).wait_recv()
        pass_sibling(r, s, past).wait_recv()

    tile = 256

    def turn(r):
        spot = pl.ds(pl.multiple_of(r * 2 * rows, 2 * rows), 2 * rows)

        @pl.loop(0, half // tile)
        def _(m):
            part = pl.ds(pl.multiple_of(m * tile, tile), tile)
            turned[part, spot] = grads[spot, part].T

    def take_own():
        grad_across().wait_recv()
        grad_hop(rep, other, True).start()
        on_middle(lambda: grad_hop(rep, other, False).start())
        share(rep, other)

    def perform(plan, acts):
        for at, (name, *args) in enumerate(plan):
            with jax.named_scope(f"{name}{at}"):
                acts[name](*args)

    def sent_shares(r, s):
        over_y(r, s, tp).wait_send()
        to_sibling(r, s, tp).wait_send()
        pass_sibling(r, s, opposite).wait_send()

    def sent_first():
        grad_across().wait_send()
        sent_shares(rep, other)
        grad_hop(rep, fsdp, True).wait_send()
        grad_hop(rep, other, True).wait_send()
        all_sent(rep, fsdp, columns, x_send.at[rep])
        all_sent(rep, fsdp, columns, z_in.at[rep])

    def clear():
        sums[fsdp * n_tp + tp] = jnp.zeros(sums.shape[1:], sums.dtype)

    def multiply_tile(ch, m, squared):
        spot = pl.ds(pl.multiple_of(m * TILE, TILE), TILE)
        product = jnp.dot(turned[spot, :], held[:, ch.cols], preferred_element_type=jnp.float32)
        out_ref[spot, ch.cols] = product.astype(out_ref.dtype)
        if squared:
            squares = jnp.sum((product * product).reshape(TILE // 8, 8, ch.size), axis=0)
            total = squares[:, :LANES]
            for at in range(LANES, ch.size, LANES):
                total = total + squares[:, at:at + LANES]
            sums[fsdp * n_tp + tp] += total

    tiles = half // TILE

    def sweep(events, arrived, between, squared):
        places = [at * tiles // len(events) for at in range(len(events))]

        def step(index):
            ch, lagging = chunk(index), chunk(index - LAG)
            with jax.named_scope("arrived"):
                arrived(lagging)

            @pl.loop(0, tiles)
            def _(m):
                for at, (place, event) in enumerate(zip(places, events)):
                    def run():
                        with jax.named_scope(f"event{at}"):
                            event(ch)
                    pl.when(m == place)(run)
                with jax.named_scope("multiply"):
                    multiply_tile(lagging, m, squared)

        pl.loop(LAG, full - 1)(step)
        between()
        for index in range(full - 1, count):
            step(index)

        def finish(ch):
            with jax.named_scope("arrived_last"):
                arrived(ch)
            with jax.named_scope("multiply_last"):
                pl.loop(0, tiles)(lambda m: multiply_tile(ch, m, squared))
        chunks_from(count - LAG, count, finish)

    @on_edge
    def _():
        places = {"near": near, "far": far, "last": far_edge}
        sides = {"own": fsdp, "other": other}

        def take(name, s):
            grad_got(places[name], sides[s]).wait_recv()
            share(places[name], sides[s])

        def land(name, s, whole):
            r = rep if name == "rep" else places[name]
            pass_on(r, sides[s])
            settle_later.append((r, sides[s]))
            if whole:
                for pair in settle_later:
                    settle(*pair)
                settle_later.clear()
                turn(r)

        settle_later = []

        def relay(*indices):
            for index in indices:
                if index + early < count:
                    hop(rep, chunk(index + early), True).start()
                if index < count:
                    crossed(edge, chunk(index)).wait_recv()
                    hop_other(chunk(index)).start()

        def pull(r):
            def event(ch):
                hop_got(r, ch).wait_recv()
                cross(r, ch).start()
            return event

        def pull_near(ch):
            hop_got(near, ch).wait_recv()
            when_extra(ch, lambda: None, lambda: cross(near, ch).start())

        pulls = [pull(far), pull(far_edge)]

        def near_at(*indices):
            for index in indices:
                pull_near(chunk(index))

        def near_ahead(ch):
            index = ch.index + FILL
            if isinstance(index, int):
                if index < count:
                    near_at(index)
                return
            pl.when(index < full)(lambda: near_at(index))
            if full < count:
                pl.when(index == full)(lambda: near_at(full))

        def early_events(*indices):
            for index in indices:
                if index >= early:
                    near_at(index + FILL)
                for event in pulls:
                    event(chunk(index))

        def batch(k):
            return range(k * count // 8, (k + 1) * count // 8)

        perform(
            [
                ("own",), ("take", "near", "own"), ("relay", *batch(0)), ("near", *range(early)),
                ("take", "near", "other"), ("land", "rep", "other", True), ("relay", *batch(1)),
                ("take", "far", "own"), ("near", early), ("land", "near", "own", False),
                ("relay", *batch(2)), ("take", "far", "other"), ("near", early + 1),
                ("land", "near", "other", True), ("relay", *batch(3)), ("take", "last", "own"),
                ("near", early + 2), ("land", "far", "own", False), ("relay", *batch(4)),
                ("take", "last", "other"), ("land", "far", "other", True), ("relay", *batch(5)),
                ("early", 0), ("relay", *batch(6)), ("early", 1), ("land", "last", "own", False),
                ("relay", *batch(7)), ("early", 2), ("land", "last", "other", True), ("early", 3),
            ],
            {"own": take_own, "take": take, "land": land, "relay": relay, "early": early_events, "near": near_at},
        )

        def arrived(ch):
            when_extra(
                ch, lambda: hop_extra(ch).wait_recv(), lambda: crossed(near, ch).wait_recv()
            )
            for r in (far, far_edge):
                crossed(r, ch).wait_recv()

        def between():
            sent_first()
            for r in (near, far, far_edge):
                for s in (fsdp, other):
                    sent_shares(r, s)
            all_sent(rep, other, columns, zo_send)

        sweep([near_ahead, *pulls], arrived, between, False)
        all_sent(near, fsdp, columns - len(EXTRA) * WIDTH, x_send.at[near])
        for r in (far, far_edge):
            all_sent(r, fsdp, columns, x_send.at[r])

    @on_middle
    def _():
        places = {"edge": edge, "far": far, "last": far_edge}
        sides = {"own": fsdp, "other": other}

        def take(name, s):
            r, s = places[name], sides[s]
            grad_got(r, s).wait_recv()
            grad_hop(r, s, name == "edge").start()
            share(r, s)

        settle_later = {}

        def land(name, s):
            r = rep if name == "rep" else places[name]
            pass_on(r, sides[s])
            settle_later.setdefault(name, []).append((r, sides[s]))
            if len(settle_later[name]) == (1 if name == "rep" else 2):
                for pair in settle_later[name]:
                    settle(*pair)
                turn(r)

        def inward(*indices):
            for index in indices:
                ch = chunk(index)
                if not isinstance(index, int) or index >= early:
                    hop(rep, ch, True).start()
                hop_got(edge, ch).wait_recv()
                hop(edge, ch, True).start()

        def fill(*indices):
            for index in indices:
                hop(rep, chunk(index), False).start()

        def outer(ch):
            if isinstance(ch.index, int):
                if ch.index + FILL < count:
                    fill(ch.index + FILL)
            else:
                pl.when(ch.index + FILL < full)(lambda: fill(ch.index + FILL))
                if full < count:
                    pl.when(ch.index + FILL == full)(lambda: fill(full))
            when_extra(ch, lambda: (crossed(rep, ch).wait_recv(), hop_extra(ch).start()) and None)
            follow(ch.index + AHEAD)

        def follow(index):
            if isinstance(index, int):
                if index < count:
                    inward(index)
                return
            pl.when(index < full)(lambda: inward(index))
            if full < count:
                pl.when(index == full)(lambda: inward(full))

        def pull(r):
            def event(ch):
                hop_got(r, ch).wait_recv()
                hop(r, ch, False).start()
                cross(r, ch).start()
            return event

        pulls = [pull(far), pull(far_edge)]

        def early_events(*indices):
            for index in indices:
                if index >= early:
                    fill(index + FILL)
                for event in pulls:
                    event(chunk(index))

        perform(
            [
                ("own",), ("take", "far", "own"), ("fill", early), ("take", "edge", "own"),
                ("take", "edge", "other"), ("inward", *range(early)), ("take", "far", "other"),
                ("fill", early + 1), ("land", "rep", "other"), ("take", "last", "own"),
                ("fill", early + 2), ("land", "far", "own"),
                ("inward", *range(early, LAG)), ("take", "last", "other"), ("land", "edge", "own"),
                ("early", 0, 1), ("inward", *range(LAG, LAG + 2)), ("land", "edge", "other"),
                ("land", "far", "other"), ("early", 2), ("inward", LAG + 2), ("land", "last", "own"),
                ("early", 3), ("inward", LAG + 3), ("land", "last", "other"),
            ],
            {"own": take_own, "take": take, "land": land, "inward": inward, "early": early_events, "fill": fill},
        )

        def arrived(ch):
            hop_other(ch).wait_recv()
            when_extra(ch, lambda: None, lambda: crossed(rep, ch).wait_recv())
            for r in (far, far_edge):
                crossed(r, ch).wait_recv()

        clear()
        sweep([outer, *pulls], arrived, lambda: None, True)

        mine = fsdp * n_tp + tp
        peers = [(a, k) for a in range(2) for k in range(n_tp) if a or k]

        def exchange(at, towards):
            a, k = peers[at]
            to_side = other if a else fsdp
            to_tp = lax.rem(tp + (k if towards else n_tp - k), n_tp)
            spot = sums.at[mine if towards else to_side * n_tp + to_tp]
            return remote(spot, spot, sq_send.at[at], sq_recv.at[at], {"fsdp": to_side, "tp": to_tp})

        for at in range(len(peers)):
            exchange(at, True).start()
        with jax.named_scope("exchange"):
            for at in range(len(peers)):
                exchange(at, False).wait_recv()
        square_total = jnp.sum(jnp.sum(sums[...], axis=0), keepdims=True)
        factor = 1.0 / jnp.sqrt(square_total / entry_count + 1e-06)
        total_out[...] = jnp.broadcast_to(factor, total_out.shape)
        for at in range(len(peers)):
            exchange(at, True).wait_send()

    def tell():
        return remote(total_out, total_out, fa_send, fa_recv, {"rep": jnp.where(is_edge, near, edge)})

    on_middle(lambda: tell().start())
    with jax.named_scope("told"):
        on_edge(lambda: tell().wait_recv())
    factor_ref[...] = total_out[...]

    @on_middle
    def _():
        tell().wait_send()
        sent_first()
        for s in (fsdp, other):
            grad_hop(rep, s, False).wait_send()
            grad_hop(edge, s, True).wait_send()
            for r in (edge, far, far_edge):
                sent_shares(r, s)
            for r in (far, far_edge):
                grad_hop(r, s, False).wait_send()
        all_sent(edge, fsdp, columns, z_in.at[edge])
        for r in (rep, far, far_edge):
            all_sent(r, fsdp, columns, z_out.at[r])
        for r in (far, far_edge):
            all_sent(r, fsdp, columns, x_send.at[r])
        all_sent(rep, other, len(EXTRA) * WIDTH, ze_send)


def by_kernel(n_rep, n_tp, entry_count, gate_pre, up_pre, out_grad):
    rows, columns = gate_pre.shape
    tokens = rows * n_rep * 2
    half = out_grad.shape[1] // 2
    quarter = half // n_tp
    count = chunking(columns)[1]
    dma = pltpu.SemaphoreType.DMA
    block, piece, line = dma((n_rep, 2)), dma((n_rep, count)), dma((count,))
    whole = dma((n_rep,))
    return pl.pallas_call(
        functools.partial(gather_multiply, entry_count),
        out_shape=(
            pltpu.VMEM((half, columns), jnp.bfloat16),
            pltpu.VMEM((8, LANES), jnp.float32),
        ),
        in_specs=[pl.BlockSpec(memory_space=pl.ANY)] * 3,
        out_specs=(pl.BlockSpec(memory_space=pltpu.VMEM), pl.BlockSpec(memory_space=pltpu.VMEM)),
        scratch_shapes=[
            pltpu.VMEM((tokens, columns), jnp.bfloat16),
            pltpu.VMEM((tokens, half), jnp.bfloat16),
            pltpu.VMEM((half, tokens), jnp.bfloat16),
            pltpu.VMEM((rows, columns), jnp.bfloat16),
            pltpu.VMEM((rows, columns), jnp.bfloat16),
            pltpu.VMEM((rows, quarter), jnp.bfloat16),
            pltpu.VMEM((2 * n_tp, 8, LANES), jnp.float32),
            pltpu.VMEM((8, LANES), jnp.float32),
            dma((4,)), dma, dma, block, block, block, block, block,
            block, block, block, block,
            piece, whole, whole, line, dma, line, dma, whole, piece,
            dma((2 * n_tp - 1,)), dma((2 * n_tp - 1,)), dma, dma,
        ],
        compiler_params=pltpu.CompilerParams(
            collective_id=0, has_side_effects=True, vmem_limit_bytes=VMEM_LIMIT * 3 // 4
        ),
    )(gate_pre, up_pre, out_grad)


def scale(summed, factors):
    half, columns = summed.shape
    rows = 128

    def body(summed_ref, factor_ref, out_ref, ready, sems):
        steps = half // rows
        depth = ready.shape[0]

        def leave(m):
            slot = lax.rem(m, depth)
            spot = pl.ds(pl.multiple_of(m * rows, rows), rows)
            return pltpu.make_async_copy(ready.at[slot], out_ref.at[spot, :], sems.at[slot])

        @pl.loop(0, steps)
        def _(m):
            slot = lax.rem(m, depth)
            spot = pl.ds(pl.multiple_of(m * rows, rows), rows)

            @pl.when(m >= depth)
            def _():
                leave(m - depth).wait()
            for at in range(0, columns, LANES):
                cols = pl.ds(at, LANES)
                scaled = summed_ref[spot, cols].astype(jnp.float32) * factor_ref[0:1, :]
                ready[slot, :, cols] = scaled.astype(ready.dtype)
            leave(m).start()

        @pl.loop(max(steps - depth, 0), steps)
        def _(m):
            leave(m).wait()

    return pl.pallas_call(
        body,
        out_shape=jax.ShapeDtypeStruct((half, columns), jnp.bfloat16),
        in_specs=[pl.BlockSpec(memory_space=pltpu.VMEM)] * 2,
        out_specs=pl.BlockSpec(memory_space=pl.ANY),
        scratch_shapes=[pltpu.VMEM((4, rows, columns), jnp.bfloat16), pltpu.SemaphoreType.DMA((4,))],
        compiler_params=pltpu.CompilerParams(vmem_limit_bytes=16 * 1024 * 1024),
    )(summed, factors)


def by_xla(gate_pre, up_pre, out_grad):
    hidden = (jax.nn.silu(gate_pre.astype(jnp.float32)) * up_pre.astype(jnp.float32)).astype(
        jnp.bfloat16
    )
    spread = lax.all_to_all(out_grad, "fsdp", split_axis=1, concat_axis=0, tiled=True)
    grad_rows = lax.all_gather(spread, "rep", axis=0, tiled=True)
    hidden_rows = lax.all_gather(hidden, ("rep", "fsdp"), axis=0, tiled=True)
    summed = lax.dot_general(
        grad_rows, hidden_rows, (((0,), (0,)), ((), ())), preferred_element_type=jnp.float32
    )
    return summed, jnp.sum(summed * summed)


def kernel_fits(n_rep, n_fsdp, n_tp, rows, columns, features):
    tokens, half = rows * n_rep * n_fsdp, features // n_fsdp
    held_bytes = 2 * (tokens * columns + 2 * tokens * half + half * columns + 2 * rows * columns)
    aligned = rows % 128 == 0 and columns % LANES == 0 and half % (LANES * n_tp) == 0
    shaped = (n_rep, n_fsdp, n_tp) == (4, 2, 4) and columns >= 12 * WIDTH
    return shaped and aligned and half % TILE == 0 and held_bytes < VMEM_LIMIT * 3 // 4


def solution(mesh):
    n_rep, n_fsdp, n_tp = (mesh.shape[axis] for axis in ("rep", "fsdp", "tp"))

    def on_device(gate_pre, up_pre, out_grad):
        half, columns = out_grad.shape[1] // n_fsdp, gate_pre.shape[1]
        entry_count = half * n_fsdp * columns * n_tp
        if kernel_fits(n_rep, n_fsdp, n_tp, *gate_pre.shape, out_grad.shape[1]):
            summed, factors = by_kernel(n_rep, n_tp, entry_count, gate_pre, up_pre, out_grad)
            return scale(summed, factors)
        summed, square_sum = by_xla(gate_pre, up_pre, out_grad)
        square_total = lax.psum(square_sum, ("fsdp", "tp"))
        factor = 1.0 / jnp.sqrt(square_total / entry_count + 1e-06)
        return (summed * factor).astype(jnp.bfloat16)

    return jax.shard_map(
        on_device,
        mesh=mesh,
        in_specs=(P(("rep", "fsdp"), "tp"), P(("rep", "fsdp"), "tp"), P(("rep", "fsdp"), None)),
        out_specs=P("fsdp", "tp"),
        check_vma=False,
    )
```

```python
import functools

import jax
import jax.numpy as jnp
from jax import lax
from jax.experimental import pallas as pl
from jax.experimental.pallas import tpu as pltpu
from jax.sharding import PartitionSpec as P

MESH = pl.DeviceIdType.MESH
LANES = 128
VMEM_LIMIT = 60 * 1024 * 1024
WIDTH = 256
TILE = 1024
LAG = 4
EDGE_LAG = 2
AHEAD = 4
FILL = 3
EXTRAS = 2


class Chunk:
    def __init__(self, index, start, size):
        self.index, self.start, self.size = index, start, size

    @property
    def cols(self):
        start = self.start
        return pl.ds(start if isinstance(start, int) else pl.multiple_of(start, LANES), self.size)


def chunking(columns):
    full, rest = columns // WIDTH, columns % WIDTH

    def chunk(index):
        if isinstance(index, int) and index == full:
            return Chunk(index, full * WIDTH, rest)
        return Chunk(index, index * WIDTH, WIDTH)

    return full, full + (1 if rest else 0), chunk


def gather_multiply(
    entry_count, gate_ref, up_ref, grad_ref, out_ref, factor_ref,
    held, grads, turned, gate_in, up_in, across_in, sums, total_out,
    local_sem, gx_send, gx_recv, gz_recv, gz_out, gz_in, gy_send, gy_recv,
    gs_send, gs_recv, gf_send, gf_recv,
    z_recv, z_out, z_in, zo_recv, zo_send, ze_recv, ze_send, x_send, x_recv,
    sq_send, sq_recv, fa_send, fa_recv,
):
    rep = lax.axis_index("rep")
    fsdp = lax.axis_index("fsdp")
    tp = lax.axis_index("tp")
    rows, columns = gate_ref.shape
    half = grads.shape[1]
    n_tp = 4
    quarter = half // n_tp
    full, count, chunk = chunking(columns)
    extras = range(count - EXTRAS, count)
    extra_columns = columns - extras[0] * WIDTH
    other = 1 - fsdp
    side = rep // 2
    edge, near, far, far_edge = 3 * side, 1 + side, 2 - side, 3 - 3 * side
    is_edge = rep == edge
    inner = jnp.where(is_edge, near, far)
    sibling = tp + 1 - 2 * lax.rem(tp, 2)
    opposite = lax.rem(tp + 2, n_tp)
    past = lax.rem(sibling + 2, n_tp)

    def rows_of(r, s):
        return pl.ds(pl.multiple_of((r * 2 + s) * rows, rows), rows)

    def quarter_of(t):
        return pl.ds(pl.multiple_of(t * quarter, LANES), quarter)

    def remote(src, dst, send, recv, device):
        return pltpu.make_async_remote_copy(
            src_ref=src, dst_ref=dst, send_sem=send, recv_sem=recv,
            device_id=device, device_id_type=MESH,
        )

    loads = [
        pltpu.make_async_copy(gate_ref, gate_in, local_sem.at[0]),
        pltpu.make_async_copy(up_ref, up_in, local_sem.at[1]),
        pltpu.make_async_copy(
            grad_ref.at[:, pl.ds(pl.multiple_of(fsdp * half, LANES), half)],
            grads.at[rows_of(rep, fsdp), :], local_sem.at[2],
        ),
        pltpu.make_async_copy(
            grad_ref.at[:, pl.ds(pl.multiple_of(other * half + tp * quarter, LANES), quarter)],
            across_in, local_sem.at[3],
        ),
    ]
    for load in loads:
        load.start()

    barrier = pltpu.get_barrier_semaphore()
    for peer in ({"fsdp": other}, {"tp": sibling}, {"tp": opposite}):
        pl.semaphore_signal(barrier, inc=1, device_id=peer, device_id_type=MESH)
    pl.semaphore_signal(barrier, inc=1, device_id={"rep": inner}, device_id_type=MESH)

    @pl.when(jnp.logical_not(is_edge))
    def _():
        pl.semaphore_signal(barrier, inc=1, device_id={"rep": edge}, device_id_type=MESH)

    with jax.named_scope("load"):
        for load in loads:
            load.wait()

    @pl.loop(0, columns // LANES)
    def _(at):
        cols = pl.ds(pl.multiple_of(at * LANES, LANES), LANES)
        gate = gate_in[:, cols].astype(jnp.float32)
        held[rows_of(rep, fsdp), cols] = (
            jax.nn.silu(gate) * up_in[:, cols].astype(jnp.float32)
        ).astype(held.dtype)

    with jax.named_scope("barrier"):
        pl.semaphore_wait(barrier, 4 + jnp.where(is_edge, 0, 1))

    def grad_across():
        return remote(across_in, grads.at[rows_of(rep, fsdp), quarter_of(tp)], gx_send, gx_recv, {"fsdp": other})

    def grad_spot(r, s, t):
        return grads.at[rows_of(r, s), quarter_of(t)]

    def grad_hop(r, s, inward):
        spot = grad_spot(r, s, tp)
        to = inner if inward else edge
        return remote(spot, spot, (gz_in if inward else gz_out).at[r, s], gz_recv.at[r, s], {"rep": to})

    def grad_got(r, s):
        spot = grad_spot(r, s, tp)
        return remote(spot, spot, gz_in.at[r, s], gz_recv.at[r, s], {"rep": inner})

    def over_y(r, s, t):
        spot = grad_spot(r, s, t)
        return remote(spot, spot, gy_send.at[r, s], gy_recv.at[r, s], {"tp": opposite})

    def to_sibling(r, s, t):
        spot = grad_spot(r, s, t)
        return remote(spot, spot, gs_send.at[r, s], gs_recv.at[r, s], {"tp": sibling})

    def pass_sibling(r, s, t):
        spot = grad_spot(r, s, t)
        return remote(spot, spot, gf_send.at[r, s], gf_recv.at[r, s], {"tp": sibling})

    def hop(r, ch, inward):
        spot = held.at[rows_of(r, fsdp), ch.cols]
        to = inner if inward else edge
        return remote(spot, spot, (z_in if inward else z_out).at[r], z_recv.at[r, ch.index], {"rep": to})

    def hop_got(r, ch):
        spot = held.at[rows_of(r, fsdp), ch.cols]
        return remote(spot, spot, z_in.at[r], z_recv.at[r, ch.index], {"rep": inner})

    def hop_other(ch):
        spot = held.at[rows_of(edge, other), ch.cols]
        return remote(spot, spot, zo_send, zo_recv.at[ch.index], {"rep": inner})

    def cross(r, ch):
        spot = held.at[rows_of(r, fsdp), ch.cols]
        return remote(spot, spot, x_send.at[r], x_recv.at[r, ch.index], {"fsdp": other})

    def crossed(r, ch):
        spot = held.at[rows_of(r, other), ch.cols]
        return remote(spot, spot, x_send.at[r], x_recv.at[r, ch.index], {"fsdp": other})

    def hop_extra(ch):
        spot = held.at[rows_of(near, other), ch.cols]
        return remote(spot, spot, ze_send, ze_recv.at[ch.index], {"rep": jnp.where(is_edge, near, edge)})

    def all_sent(r, s, width, send):
        spot = held.at[rows_of(r, s), pl.ds(0, width)]
        remote(spot, spot, send, gx_recv, {"fsdp": other}).wait_send()

    def when_extra(ch, act, otherwise):
        if isinstance(ch.index, int):
            act() if ch.index in extras else otherwise()
            return
        pl.when(ch.index >= extras[0])(act)
        pl.when(ch.index < extras[0])(otherwise)

    def on_edge(act):
        pl.when(is_edge)(act)

    def on_middle(act):
        pl.when(jnp.logical_not(is_edge))(act)

    def chunks_from(low, high, act):
        if low < min(high, full):
            @pl.loop(low, min(high, full))
            def _(index):
                act(chunk(index))
        if full < count == high:
            act(chunk(full))

    grad_across().start()
    grad_hop(rep, fsdp, True).start()
    on_middle(lambda: grad_hop(rep, fsdp, False).start())

    chunks_from(0, count, lambda ch: cross(rep, ch).start())
    early = 2
    chunks_from(0, early, lambda ch: hop(rep, ch, True).start())
    on_middle(lambda: chunks_from(0, early, lambda ch: hop(rep, ch, False).start()))

    def share(r, s):
        over_y(r, s, tp).start()
        to_sibling(r, s, tp).start()

    def pass_on(r, s):
        over_y(r, s, opposite).wait_recv()
        pass_sibling(r, s, opposite).start()

    def settle(r, s):
        to_sibling(r, s, sibling).wait_recv()
        pass_sibling(r, s, past).wait_recv()

    tile = 256

    def turn(r):
        spot = pl.ds(pl.multiple_of(r * 2 * rows, 2 * rows), 2 * rows)

        @pl.loop(0, half // tile)
        def _(m):
            part = pl.ds(pl.multiple_of(m * tile, tile), tile)
            turned[part, spot] = grads[spot, part].T

    def take_own():
        grad_across().wait_recv()
        grad_hop(rep, other, True).start()
        on_middle(lambda: grad_hop(rep, other, False).start())
        share(rep, other)

    def perform(plan, acts):
        for at, (name, *args) in enumerate(plan):
            with jax.named_scope(f"{name}{at}"):
                acts[name](*args)

    def sent_shares(r, s):
        over_y(r, s, tp).wait_send()
        to_sibling(r, s, tp).wait_send()
        pass_sibling(r, s, opposite).wait_send()

    def sent_first():
        grad_across().wait_send()
        sent_shares(rep, other)
        grad_hop(rep, fsdp, True).wait_send()
        grad_hop(rep, other, True).wait_send()
        all_sent(rep, fsdp, columns, x_send.at[rep])
        all_sent(rep, fsdp, columns, z_in.at[rep])

    def clear():
        sums[fsdp * n_tp + tp] = jnp.zeros(sums.shape[1:], sums.dtype)

    def multiply_tile(ch, m, squared):
        spot = pl.ds(pl.multiple_of(m * TILE, TILE), TILE)
        product = jnp.dot(turned[spot, :], held[:, ch.cols], preferred_element_type=jnp.float32)
        out_ref[spot, ch.cols] = product.astype(out_ref.dtype)
        if squared:
            squares = jnp.sum((product * product).reshape(TILE // 8, 8, ch.size), axis=0)
            total = squares[:, :LANES]
            for at in range(LANES, ch.size, LANES):
                total = total + squares[:, at:at + LANES]
            sums[fsdp * n_tp + tp] += total

    tiles = half // TILE

    def finish(ch, arrived, squared):
        with jax.named_scope("arrived_last"):
            arrived(ch)
        with jax.named_scope("multiply_last"):
            pl.loop(0, tiles)(lambda m: multiply_tile(ch, m, squared))

    def sweep(events, arrived, between, ended, lag, squared):
        places = [at * tiles // len(events) for at in range(len(events))]

        def step(index):
            ch, lagging = chunk(index), chunk(index - lag)
            with jax.named_scope("arrived"):
                arrived(lagging)

            @pl.loop(0, tiles)
            def _(m):
                for at, (place, event) in enumerate(zip(places, events)):
                    def run():
                        with jax.named_scope(f"event{at}"):
                            event(ch)
                    pl.when(m == place)(run)
                with jax.named_scope("multiply"):
                    multiply_tile(lagging, m, squared)

        pl.loop(LAG, full - 1)(step)
        between()
        for index in range(full - 1, count):
            step(index)
        ended()
        chunks_from(count - lag, count, lambda ch: finish(ch, arrived, squared))

    @on_edge
    def _():
        places = {"near": near, "far": far, "last": far_edge}
        sides = {"own": fsdp, "other": other}

        def take(name, s):
            grad_got(places[name], sides[s]).wait_recv()
            share(places[name], sides[s])

        def land(name, s, whole):
            r = rep if name == "rep" else places[name]
            pass_on(r, sides[s])
            settle_later.append((r, sides[s]))
            if whole:
                for pair in settle_later:
                    settle(*pair)
                settle_later.clear()
                turn(r)

        settle_later = []

        def relay(*indices):
            for index in indices:
                if index + early < count:
                    hop(rep, chunk(index + early), True).start()
                if index < count:
                    crossed(edge, chunk(index)).wait_recv()
                    hop_other(chunk(index)).start()

        def pull(r):
            def event(ch):
                hop_got(r, ch).wait_recv()
                cross(r, ch).start()
            return event

        def pull_near(ch):
            hop_got(near, ch).wait_recv()
            when_extra(ch, lambda: None, lambda: cross(near, ch).start())

        pulls = [pull(far), pull(far_edge)]

        def near_at(*indices):
            for index in indices:
                pull_near(chunk(index))

        def near_ahead(ch):
            index = ch.index + FILL
            if isinstance(index, int):
                if index < count:
                    near_at(index)
                return
            pl.when(index < full)(lambda: near_at(index))
            if full < count:
                pl.when(index == full)(lambda: near_at(full))

        def early_events(*indices):
            for index in indices:
                if index >= early:
                    near_at(index + FILL)
                for event in pulls:
                    event(chunk(index))

        def arrived(ch):
            when_extra(
                ch, lambda: hop_extra(ch).wait_recv(), lambda: crossed(near, ch).wait_recv()
            )
            for r in (far, far_edge):
                crossed(r, ch).wait_recv()

        def compute(index):
            finish(chunk(index), arrived, False)

        def batch(k):
            return range(k * count // 8, (k + 1) * count // 8)

        perform(
            [
                ("own",), ("take", "near", "own"), ("relay", *batch(0)), ("near", *range(early)),
                ("take", "near", "other"), ("land", "rep", "other", True), ("relay", *batch(1)),
                ("take", "far", "own"), ("near", early), ("land", "near", "own", False),
                ("relay", *batch(2)), ("take", "far", "other"), ("near", early + 1),
                ("land", "near", "other", True), ("relay", *batch(3)), ("take", "last", "own"),
                ("near", early + 2), ("land", "far", "own", False), ("relay", *batch(4)),
                ("take", "last", "other"), ("land", "far", "other", True), ("relay", *batch(5)),
                ("early", 0), ("relay", *batch(6)), ("early", 1), ("land", "last", "own", False),
                ("relay", *batch(7)), ("early", 2), ("land", "last", "other", True),
                ("compute", 0), ("early", 3), ("compute", 1),
            ],
            {"own": take_own, "take": take, "land": land, "relay": relay, "early": early_events, "near": near_at,
             "compute": compute},
        )

        def between():
            sent_first()
            for r in (near, far, far_edge):
                for s in (fsdp, other):
                    sent_shares(r, s)
            all_sent(rep, other, columns, zo_send)

        sweep([near_ahead, *pulls], arrived, between, lambda: None, EDGE_LAG, False)
        all_sent(near, fsdp, columns - extra_columns, x_send.at[near])
        for r in (far, far_edge):
            all_sent(r, fsdp, columns, x_send.at[r])

    @on_middle
    def _():
        places = {"edge": edge, "far": far, "last": far_edge}
        sides = {"own": fsdp, "other": other}

        def take(name, s):
            r, s = places[name], sides[s]
            grad_got(r, s).wait_recv()
            grad_hop(r, s, name == "edge").start()
            share(r, s)

        settle_later = {}

        def land(name, s):
            r = rep if name == "rep" else places[name]
            pass_on(r, sides[s])
            settle_later.setdefault(name, []).append((r, sides[s]))
            if len(settle_later[name]) == (1 if name == "rep" else 2):
                for pair in settle_later[name]:
                    settle(*pair)
                turn(r)

        def inward(*indices):
            for index in indices:
                ch = chunk(index)
                if not isinstance(index, int) or index >= early:
                    hop(rep, ch, True).start()
                hop_got(edge, ch).wait_recv()
                hop(edge, ch, True).start()

        def fill(*indices):
            for index in indices:
                hop(rep, chunk(index), False).start()

        def outer(ch):
            if isinstance(ch.index, int):
                if ch.index + FILL < count:
                    fill(ch.index + FILL)
            else:
                pl.when(ch.index + FILL < full)(lambda: fill(ch.index + FILL))
                if full < count:
                    pl.when(ch.index + FILL == full)(lambda: fill(full))
            follow(ch.index + AHEAD)

        def follow(index):
            if isinstance(index, int):
                if index < count:
                    inward(index)
                return
            pl.when(index < full)(lambda: inward(index))
            if full < count:
                pl.when(index == full)(lambda: inward(full))

        def pull(r):
            def event(ch):
                hop_got(r, ch).wait_recv()
                hop(r, ch, False).start()
                cross(r, ch).start()
            return event

        pulls = [pull(far), pull(far_edge)]

        def early_events(*indices):
            for index in indices:
                if index >= early:
                    fill(index + FILL)
                for event in pulls:
                    event(chunk(index))

        perform(
            [
                ("own",), ("take", "far", "own"), ("fill", early), ("take", "edge", "own"),
                ("take", "edge", "other"), ("inward", *range(early)), ("take", "far", "other"),
                ("fill", early + 1), ("land", "rep", "other"), ("take", "last", "own"),
                ("fill", early + 2), ("land", "far", "own"),
                ("inward", *range(early, LAG)), ("take", "last", "other"), ("land", "edge", "own"),
                ("early", 0, 1), ("inward", *range(LAG, LAG + 2)), ("land", "edge", "other"),
                ("land", "far", "other"), ("early", 2), ("inward", LAG + 2), ("land", "last", "own"),
                ("early", 3), ("inward", LAG + 3), ("land", "last", "other"),
            ],
            {"own": take_own, "take": take, "land": land, "inward": inward, "early": early_events, "fill": fill},
        )

        def arrived(ch):
            hop_other(ch).wait_recv()
            when_extra(ch, lambda: None, lambda: crossed(rep, ch).wait_recv())
            for r in (far, far_edge):
                crossed(r, ch).wait_recv()

        clear()

        def ended():
            for index in extras:
                crossed(rep, chunk(index)).wait_recv()
                hop_extra(chunk(index)).start()

        sweep([outer, *pulls], arrived, lambda: None, ended, LAG, True)

        mine = fsdp * n_tp + tp
        peers = [(a, k) for a in range(2) for k in range(n_tp) if a or k]

        def exchange(at, towards):
            a, k = peers[at]
            to_side = other if a else fsdp
            to_tp = lax.rem(tp + (k if towards else n_tp - k), n_tp)
            spot = sums.at[mine if towards else to_side * n_tp + to_tp]
            return remote(spot, spot, sq_send.at[at], sq_recv.at[at], {"fsdp": to_side, "tp": to_tp})

        for at in range(len(peers)):
            exchange(at, True).start()
        with jax.named_scope("exchange"):
            for at in range(len(peers)):
                exchange(at, False).wait_recv()
        square_total = jnp.sum(jnp.sum(sums[...], axis=0), keepdims=True)
        factor = 1.0 / jnp.sqrt(square_total / entry_count + 1e-06)
        total_out[...] = jnp.broadcast_to(factor, total_out.shape)
        for at in range(len(peers)):
            exchange(at, True).wait_send()

    def tell():
        return remote(total_out, total_out, fa_send, fa_recv, {"rep": jnp.where(is_edge, near, edge)})

    on_middle(lambda: tell().start())
    with jax.named_scope("told"):
        on_edge(lambda: tell().wait_recv())
    factor_ref[...] = total_out[...]

    @on_middle
    def _():
        tell().wait_send()
        sent_first()
        for s in (fsdp, other):
            grad_hop(rep, s, False).wait_send()
            grad_hop(edge, s, True).wait_send()
            for r in (edge, far, far_edge):
                sent_shares(r, s)
            for r in (far, far_edge):
                grad_hop(r, s, False).wait_send()
        all_sent(edge, fsdp, columns, z_in.at[edge])
        for r in (rep, far, far_edge):
            all_sent(r, fsdp, columns, z_out.at[r])
        for r in (far, far_edge):
            all_sent(r, fsdp, columns, x_send.at[r])
        all_sent(rep, other, extra_columns, ze_send)


def by_kernel(n_rep, n_tp, entry_count, gate_pre, up_pre, out_grad):
    rows, columns = gate_pre.shape
    tokens = rows * n_rep * 2
    half = out_grad.shape[1] // 2
    quarter = half // n_tp
    count = chunking(columns)[1]
    dma = pltpu.SemaphoreType.DMA
    block, piece, line = dma((n_rep, 2)), dma((n_rep, count)), dma((count,))
    whole = dma((n_rep,))
    return pl.pallas_call(
        functools.partial(gather_multiply, entry_count),
        out_shape=(
            pltpu.VMEM((half, columns), jnp.bfloat16),
            pltpu.VMEM((8, LANES), jnp.float32),
        ),
        in_specs=[pl.BlockSpec(memory_space=pl.ANY)] * 3,
        out_specs=(pl.BlockSpec(memory_space=pltpu.VMEM), pl.BlockSpec(memory_space=pltpu.VMEM)),
        scratch_shapes=[
            pltpu.VMEM((tokens, columns), jnp.bfloat16),
            pltpu.VMEM((tokens, half), jnp.bfloat16),
            pltpu.VMEM((half, tokens), jnp.bfloat16),
            pltpu.VMEM((rows, columns), jnp.bfloat16),
            pltpu.VMEM((rows, columns), jnp.bfloat16),
            pltpu.VMEM((rows, quarter), jnp.bfloat16),
            pltpu.VMEM((2 * n_tp, 8, LANES), jnp.float32),
            pltpu.VMEM((8, LANES), jnp.float32),
            dma((4,)), dma, dma, block, block, block, block, block,
            block, block, block, block,
            piece, whole, whole, line, dma, line, dma, whole, piece,
            dma((2 * n_tp - 1,)), dma((2 * n_tp - 1,)), dma, dma,
        ],
        compiler_params=pltpu.CompilerParams(
            collective_id=0, has_side_effects=True, vmem_limit_bytes=VMEM_LIMIT * 3 // 4
        ),
    )(gate_pre, up_pre, out_grad)


def scale(summed, factors):
    half, columns = summed.shape
    rows = 128

    def body(summed_ref, factor_ref, out_ref, ready, sems):
        steps = half // rows
        depth = ready.shape[0]

        def leave(m):
            slot = lax.rem(m, depth)
            spot = pl.ds(pl.multiple_of(m * rows, rows), rows)
            return pltpu.make_async_copy(ready.at[slot], out_ref.at[spot, :], sems.at[slot])

        @pl.loop(0, steps)
        def _(m):
            slot = lax.rem(m, depth)
            spot = pl.ds(pl.multiple_of(m * rows, rows), rows)

            @pl.when(m >= depth)
            def _():
                leave(m - depth).wait()
            for at in range(0, columns, LANES):
                cols = pl.ds(at, LANES)
                scaled = summed_ref[spot, cols].astype(jnp.float32) * factor_ref[0:1, :]
                ready[slot, :, cols] = scaled.astype(ready.dtype)
            leave(m).start()

        @pl.loop(max(steps - depth, 0), steps)
        def _(m):
            leave(m).wait()

    return pl.pallas_call(
        body,
        out_shape=jax.ShapeDtypeStruct((half, columns), jnp.bfloat16),
        in_specs=[pl.BlockSpec(memory_space=pltpu.VMEM)] * 2,
        out_specs=pl.BlockSpec(memory_space=pl.ANY),
        scratch_shapes=[pltpu.VMEM((4, rows, columns), jnp.bfloat16), pltpu.SemaphoreType.DMA((4,))],
        compiler_params=pltpu.CompilerParams(vmem_limit_bytes=16 * 1024 * 1024),
    )(summed, factors)


def by_xla(gate_pre, up_pre, out_grad):
    hidden = (jax.nn.silu(gate_pre.astype(jnp.float32)) * up_pre.astype(jnp.float32)).astype(
        jnp.bfloat16
    )
    spread = lax.all_to_all(out_grad, "fsdp", split_axis=1, concat_axis=0, tiled=True)
    grad_rows = lax.all_gather(spread, "rep", axis=0, tiled=True)
    hidden_rows = lax.all_gather(hidden, ("rep", "fsdp"), axis=0, tiled=True)
    summed = lax.dot_general(
        grad_rows, hidden_rows, (((0,), (0,)), ((), ())), preferred_element_type=jnp.float32
    )
    return summed, jnp.sum(summed * summed)


def kernel_fits(n_rep, n_fsdp, n_tp, rows, columns, features):
    tokens, half = rows * n_rep * n_fsdp, features // n_fsdp
    held_bytes = 2 * (tokens * columns + 2 * tokens * half + half * columns + 2 * rows * columns)
    aligned = rows % 128 == 0 and columns % LANES == 0 and half % (LANES * n_tp) == 0
    shaped = (n_rep, n_fsdp, n_tp) == (4, 2, 4) and columns >= 12 * WIDTH
    return shaped and aligned and half % TILE == 0 and held_bytes < VMEM_LIMIT * 3 // 4


def solution(mesh):
    n_rep, n_fsdp, n_tp = (mesh.shape[axis] for axis in ("rep", "fsdp", "tp"))

    def on_device(gate_pre, up_pre, out_grad):
        half, columns = out_grad.shape[1] // n_fsdp, gate_pre.shape[1]
        entry_count = half * n_fsdp * columns * n_tp
        if kernel_fits(n_rep, n_fsdp, n_tp, *gate_pre.shape, out_grad.shape[1]):
            summed, factors = by_kernel(n_rep, n_tp, entry_count, gate_pre, up_pre, out_grad)
            return scale(summed, factors)
        summed, square_sum = by_xla(gate_pre, up_pre, out_grad)
        square_total = lax.psum(square_sum, ("fsdp", "tp"))
        factor = 1.0 / jnp.sqrt(square_total / entry_count + 1e-06)
        return (summed * factor).astype(jnp.bfloat16)

    return jax.shard_map(
        on_device,
        mesh=mesh,
        in_specs=(P(("rep", "fsdp"), "tp"), P(("rep", "fsdp"), "tp"), P(("rep", "fsdp"), None)),
        out_specs=P("fsdp", "tp"),
        check_vma=False,
    )
```

```python
import functools

import jax
import jax.numpy as jnp
from jax import lax
from jax.experimental import pallas as pl
from jax.experimental.pallas import tpu as pltpu
from jax.sharding import PartitionSpec as P

MESH = pl.DeviceIdType.MESH
LANES = 128
VMEM_LIMIT = 60 * 1024 * 1024
WIDTH = 256
TILE = 1024
LAG = 4
EDGE_LAG = 2
AHEAD = 4
FILL = 3
EXTRA = 8


class Chunk:
    def __init__(self, index, start, size):
        self.index, self.start, self.size = index, start, size

    @property
    def cols(self):
        start = self.start
        return pl.ds(start if isinstance(start, int) else pl.multiple_of(start, LANES), self.size)


def chunking(columns):
    full, rest = columns // WIDTH, columns % WIDTH

    def chunk(index):
        if isinstance(index, int) and index == full:
            return Chunk(index, full * WIDTH, rest)
        return Chunk(index, index * WIDTH, WIDTH)

    return full, full + (1 if rest else 0), chunk


def gather_multiply(
    entry_count, gate_ref, up_ref, grad_ref, out_ref, factor_ref,
    held, grads, turned, gate_in, up_in, across_in, sums, total_out,
    middle_part, end_part,
    local_sem, gx_send, gx_recv, gz_recv, gz_out, gz_in, gy_send, gy_recv,
    gs_send, gs_recv, gf_send, gf_recv,
    z_recv, z_out, z_in, zo_send, ze_send, x_send, xn_send, x_recv,
    sq_send, sq_recv, fa_send, fa_recv,
):
    rep = lax.axis_index("rep")
    fsdp = lax.axis_index("fsdp")
    tp = lax.axis_index("tp")
    rows, columns = gate_ref.shape
    half = grads.shape[1]
    n_tp = 4
    quarter = half // n_tp
    full, count, chunk = chunking(columns)
    extras = (EXTRA, count - 1)
    extra_columns = WIDTH + chunk(count - 1).size
    other = 1 - fsdp
    side = rep // 2
    edge, near, far, far_edge = 3 * side, 1 + side, 2 - side, 3 - 3 * side
    is_edge = rep == edge
    inner = jnp.where(is_edge, near, far)
    sibling = tp + 1 - 2 * lax.rem(tp, 2)
    opposite = lax.rem(tp + 2, n_tp)
    past = lax.rem(sibling + 2, n_tp)

    def rows_of(r, s):
        return pl.ds(pl.multiple_of((r * 2 + s) * rows, rows), rows)

    def quarter_of(t):
        return pl.ds(pl.multiple_of(t * quarter, LANES), quarter)

    def remote(src, dst, send, recv, device):
        return pltpu.make_async_remote_copy(
            src_ref=src, dst_ref=dst, send_sem=send, recv_sem=recv,
            device_id=device, device_id_type=MESH,
        )

    loads = [
        pltpu.make_async_copy(gate_ref, gate_in, local_sem.at[0]),
        pltpu.make_async_copy(up_ref, up_in, local_sem.at[1]),
        pltpu.make_async_copy(
            grad_ref.at[:, pl.ds(pl.multiple_of(fsdp * half, LANES), half)],
            grads.at[rows_of(rep, fsdp), :], local_sem.at[2],
        ),
        pltpu.make_async_copy(
            grad_ref.at[:, pl.ds(pl.multiple_of(other * half + tp * quarter, LANES), quarter)],
            across_in, local_sem.at[3],
        ),
    ]
    for load in loads:
        load.start()

    barrier = pltpu.get_barrier_semaphore()
    for peer in ({"fsdp": other}, {"tp": sibling}, {"tp": opposite}):
        pl.semaphore_signal(barrier, inc=1, device_id=peer, device_id_type=MESH)
    pl.semaphore_signal(barrier, inc=1, device_id={"rep": inner}, device_id_type=MESH)

    @pl.when(jnp.logical_not(is_edge))
    def _():
        pl.semaphore_signal(barrier, inc=1, device_id={"rep": edge}, device_id_type=MESH)

    with jax.named_scope("load"):
        for load in loads:
            load.wait()

    @pl.loop(0, columns // LANES)
    def _(at):
        cols = pl.ds(pl.multiple_of(at * LANES, LANES), LANES)
        gate = gate_in[:, cols].astype(jnp.float32)
        held[rows_of(rep, fsdp), cols] = (
            jax.nn.silu(gate) * up_in[:, cols].astype(jnp.float32)
        ).astype(held.dtype)

    with jax.named_scope("barrier"):
        pl.semaphore_wait(barrier, 4 + jnp.where(is_edge, 0, 1))

    def grad_across():
        return remote(across_in, grads.at[rows_of(rep, fsdp), quarter_of(tp)], gx_send, gx_recv, {"fsdp": other})

    def grad_spot(r, s, t):
        return grads.at[rows_of(r, s), quarter_of(t)]

    def grad_hop(r, s, inward):
        spot = grad_spot(r, s, tp)
        to = inner if inward else edge
        return remote(spot, spot, (gz_in if inward else gz_out), gz_recv.at[r, s], {"rep": to})

    def grad_got(r, s):
        spot = grad_spot(r, s, tp)
        return remote(spot, spot, gz_in, gz_recv.at[r, s], {"rep": inner})

    def over_y(r, s, t):
        spot = grad_spot(r, s, t)
        return remote(spot, spot, gy_send, gy_recv.at[r, s], {"tp": opposite})

    def to_sibling(r, s, t):
        spot = grad_spot(r, s, t)
        return remote(spot, spot, gs_send, gs_recv.at[r], {"tp": sibling})

    def pass_sibling(r, s, t):
        spot = grad_spot(r, s, t)
        return remote(spot, spot, gf_send, gf_recv.at[r], {"tp": sibling})

    def hop(r, ch, inward, slot):
        spot = held.at[rows_of(r, fsdp), ch.cols]
        to = inner if inward else edge
        return remote(spot, spot, z_in if inward else z_out, z_recv.at[slot, ch.index], {"rep": to})

    def hop_got(slot, ch):
        spot = held.at[pl.ds(0, rows), ch.cols]
        return remote(spot, spot, z_in, z_recv.at[slot, ch.index], {"rep": inner})

    def hop_other(ch):
        spot = held.at[rows_of(edge, other), ch.cols]
        return remote(spot, spot, zo_send, x_recv.at[edge, ch.index], {"rep": inner})

    def cross(r, ch, send=None):
        spot = held.at[rows_of(r, fsdp), ch.cols]
        return remote(spot, spot, x_send if send is None else send, x_recv.at[r, ch.index], {"fsdp": other})

    def crossed(r, ch):
        spot = held.at[rows_of(r, other), ch.cols]
        return remote(spot, spot, x_send, x_recv.at[r, ch.index], {"fsdp": other})

    def hop_extra(ch):
        spot = held.at[rows_of(near, other), ch.cols]
        return remote(spot, spot, ze_send, x_recv.at[near, ch.index], {"rep": jnp.where(is_edge, near, edge)})

    def all_sent(blocks, width, send):
        spot = held.at[pl.ds(0, blocks * rows), pl.ds(0, width)]
        remote(spot, spot, send, gx_recv, {"fsdp": other}).wait_send()

    def when_extra(ch, act, otherwise):
        if isinstance(ch.index, int):
            act() if ch.index in extras else otherwise()
            return
        pl.when(ch.index == extras[0])(act)
        pl.when(ch.index != extras[0])(otherwise)

    def on_edge(act):
        pl.when(is_edge)(act)

    def on_middle(act):
        pl.when(jnp.logical_not(is_edge))(act)

    def chunks_from(low, high, act):
        if low < min(high, full):
            @pl.loop(low, min(high, full))
            def _(index):
                act(chunk(index))
        if full < count == high:
            act(chunk(full))

    grad_across().start()
    grad_hop(rep, fsdp, True).start()
    on_middle(lambda: grad_hop(rep, fsdp, False).start())

    chunks_from(0, count, lambda ch: cross(rep, ch).start())
    early = 2

    def own_inward(ch):
        hop(rep, ch, True, jnp.where(is_edge, 0, 1)).start()

    chunks_from(0, early, own_inward)
    on_middle(lambda: chunks_from(0, early, lambda ch: hop(rep, ch, False, 0).start()))

    def share(r, s):
        over_y(r, s, tp).start()
        to_sibling(r, s, tp).start()

    def pass_on(r, s):
        over_y(r, s, opposite).wait_recv()
        pass_sibling(r, s, opposite).start()

    def settle(r, pairs):
        spots = grads.at[pl.ds(0, pairs * rows), pl.ds(0, quarter)]
        remote(spots, spots, gs_send, gs_recv.at[r], {"tp": sibling}).wait_recv()
        remote(spots, spots, gf_send, gf_recv.at[r], {"tp": sibling}).wait_recv()

    tile = 256

    def turn(r):
        spot = pl.ds(pl.multiple_of(r * 2 * rows, 2 * rows), 2 * rows)

        @pl.loop(0, half // tile)
        def _(m):
            part = pl.ds(pl.multiple_of(m * tile, tile), tile)
            turned[part, spot] = grads[spot, part].T

    def take_own():
        grad_across().wait_recv()
        grad_hop(rep, other, True).start()
        on_middle(lambda: grad_hop(rep, other, False).start())
        share(rep, other)

    def perform(plan, acts):
        for at, (name, *args) in enumerate(plan):
            with jax.named_scope(f"{name}{at}"):
                acts[name](*args)

    def grads_sent(blocks, send):
        all_sent(1, blocks * quarter, send)

    def shares_sent():
        grad_across().wait_send()
        for send in (gy_send, gs_send, gf_send):
            grads_sent(7, send)

    def clear():
        sums[fsdp * n_tp + tp] = jnp.zeros(sums.shape[1:], sums.dtype)

    def leave(product, spot, ch, squared):
        out_ref[spot, ch.cols] = product.astype(out_ref.dtype)
        if squared:
            squares = jnp.sum((product * product).reshape(TILE // 8, 8, ch.size), axis=0)
            total = squares[:, :LANES]
            for at in range(LANES, ch.size, LANES):
                total = total + squares[:, at:at + LANES]
            sums[fsdp * n_tp + tp] += total

    def tile_of(m):
        return pl.ds(pl.multiple_of(m * TILE, TILE), TILE)

    def multiply_tile(ch, m, squared):
        spot = tile_of(m)
        product = jnp.dot(turned[spot, :], held[:, ch.cols], preferred_element_type=jnp.float32)
        leave(product, spot, ch, squared)

    pair = 2 * rows
    ends = {"first": pl.multiple_of(edge * pair, pair), "late": pl.multiple_of(far_edge * pair, pair)}

    def part(spot, ch, start, size):
        tokens = pl.ds(start, size)
        return jnp.dot(turned[spot, tokens], held[tokens, ch.cols], preferred_element_type=jnp.float32)

    def kept(ch):
        return pl.ds((ch.index - (count - 2)) * WIDTH, ch.size)

    def begin(ch):
        @pl.loop(0, tiles)
        def _(m):
            spot = tile_of(m)
            middle_part[spot, kept(ch)] = part(spot, ch, pair, 2 * pair)
            end_part[spot, kept(ch)] = part(spot, ch, ends["first"], pair)

    def complete(ch, squared):
        @pl.loop(0, tiles)
        def _(m):
            spot = tile_of(m)
            both = end_part[spot, kept(ch)] + part(spot, ch, ends["late"], pair)
            leave(middle_part[spot, kept(ch)] + both, spot, ch, squared)

    tiles = half // TILE

    def finish(ch, arrived, squared):
        with jax.named_scope("arrived_last"):
            arrived(ch)
        with jax.named_scope("multiply_last"):
            pl.loop(0, tiles)(lambda m: multiply_tile(ch, m, squared))

    def sweep(events, arrived_but_last, between, ended, lag, squared):
        def arrived(ch):
            arrived_but_last(ch)
            crossed(far_edge, ch).wait_recv()

        places = [at * tiles // len(events) for at in range(len(events))]

        def step(index, events=events):
            ch, lagging = chunk(index), chunk(index - lag)
            with jax.named_scope("arrived"):
                arrived(lagging)

            @pl.loop(0, tiles)
            def _(m):
                for at, (place, event) in enumerate(zip(places, events)):
                    def run():
                        with jax.named_scope(f"event{at}"):
                            event(ch)
                    pl.when(m == place)(run)
                with jax.named_scope("multiply"):
                    multiply_tile(lagging, m, squared)

        pl.loop(LAG, count - 2)(step)
        between()
        ahead, far_pull, last_pull = events
        last_two = chunk(count - 2), chunk(count - 1)
        for at, pull in ((0, far_pull), (1, last_pull)):
            step(count - 2 + at, [lambda ch: ahead(ch), lambda ch: pull(last_two[0]), lambda ch: pull(last_two[1])])
        ended()
        chunks_from(count - lag, count - 2, lambda ch: finish(ch, arrived, squared))
        for ch in last_two:
            with jax.named_scope("begin"):
                arrived_but_last(ch)
                begin(ch)
        for ch in last_two:
            with jax.named_scope("late"):
                crossed(far_edge, ch).wait_recv()
                complete(ch, squared)

    @on_edge
    def _():
        places = {"near": near, "far": far, "last": far_edge}
        sides = {"own": fsdp, "other": other}

        def take(name, s):
            grad_got(places[name], sides[s]).wait_recv()
            share(places[name], sides[s])

        def land(name, s, whole):
            r = rep if name == "rep" else places[name]
            pass_on(r, sides[s])
            if whole:
                settle(r, 1 if name == "rep" else 2)
                turn(r)

        def relay(*indices):
            for index in indices:
                if index + early < count:
                    own_inward(chunk(index + early))
                if index < count:
                    crossed(edge, chunk(index)).wait_recv()
                    hop_other(chunk(index)).start()

        def pull(slot, r):
            def event(ch):
                hop_got(slot, ch).wait_recv()
                cross(r, ch).start()
            return event

        def pull_near(ch):
            hop_got(0, ch).wait_recv()
            when_extra(ch, lambda: None, lambda: cross(near, ch, xn_send).start())

        pulls = [pull(1, far), pull(2, far_edge)]

        def near_at(*indices):
            for index in indices:
                pull_near(chunk(index))

        def near_ahead(ch):
            index = ch.index + FILL
            if isinstance(index, int):
                if index < count:
                    near_at(index)
                return
            pl.when(index < full)(lambda: near_at(index))
            if full < count:
                pl.when(index == full)(lambda: near_at(full))

        def early_events(*indices):
            for index in indices:
                if index >= early:
                    near_at(index + FILL)
                for event in pulls:
                    event(chunk(index))

        def arrived(ch):
            crossed(near, ch).wait_recv()
            crossed(far, ch).wait_recv()

        def compute(index):
            def whole(ch):
                arrived(ch)
                crossed(far_edge, ch).wait_recv()
            finish(chunk(index), whole, False)

        def batch(k):
            return range(k * count // 8, (k + 1) * count // 8)

        perform(
            [
                ("own",), ("take", "near", "own"), ("relay", *batch(0)), ("near", *range(early)),
                ("take", "near", "other"), ("land", "rep", "other", True), ("relay", *batch(1)),
                ("take", "far", "own"), ("near", early), ("land", "near", "own", False),
                ("relay", *batch(2)), ("take", "far", "other"), ("near", early + 1),
                ("land", "near", "other", True), ("relay", *batch(3)), ("take", "last", "own"),
                ("near", early + 2), ("land", "far", "own", False), ("relay", *batch(4)),
                ("take", "last", "other"), ("land", "far", "other", True), ("relay", *batch(5)),
                ("early", 0), ("relay", *batch(6)), ("early", 1), ("land", "last", "own", False),
                ("relay", *batch(7)), ("early", 2), ("land", "last", "other", True),
                ("compute", 0), ("early", 3), ("compute", 1),
            ],
            {"own": take_own, "take": take, "land": land, "relay": relay, "early": early_events, "near": near_at,
             "compute": compute},
        )

        def between():
            shares_sent()
            grads_sent(2, gz_in)
            all_sent(1, columns, z_in)
            all_sent(1, columns, zo_send)

        sweep([near_ahead, *pulls], arrived, between, lambda: None, EDGE_LAG, False)
        all_sent(1, columns - extra_columns, xn_send)
        all_sent(3, columns, x_send)

    @on_middle
    def _():
        places = {"edge": edge, "far": far, "last": far_edge}
        sides = {"own": fsdp, "other": other}

        def take(name, s):
            r, s = places[name], sides[s]
            grad_got(r, s).wait_recv()
            grad_hop(r, s, name == "edge").start()
            share(r, s)

        def land(name, s, whole=True):
            r = rep if name == "rep" else places[name]
            pass_on(r, sides[s])
            if whole:
                settle(r, 1 if name == "rep" else 2)
                turn(r)

        def inward(*indices):
            for index in indices:
                ch = chunk(index)
                if not isinstance(index, int) or index >= early:
                    own_inward(ch)
                hop_got(0, ch).wait_recv()
                hop(edge, ch, True, 2).start()

        def fill(*indices):
            for index in indices:
                hop(rep, chunk(index), False, 0).start()

        def outer(ch):
            if isinstance(ch.index, int):
                if ch.index + FILL < count:
                    fill(ch.index + FILL)
            else:
                pl.when(ch.index + FILL < full)(lambda: fill(ch.index + FILL))
                if full < count:
                    pl.when(ch.index + FILL == full)(lambda: fill(full))
            follow(ch.index + AHEAD)
            if not isinstance(ch.index, int):
                pl.when(ch.index == EXTRA)(lambda: send_extra(ch))

        def send_extra(ch):
            crossed(rep, ch).wait_recv()
            hop_extra(ch).start()

        def follow(index):
            if isinstance(index, int):
                if index < count:
                    inward(index)
                return
            pl.when(index < full)(lambda: inward(index))
            if full < count:
                pl.when(index == full)(lambda: inward(full))

        def pull(slot, r):
            def event(ch):
                hop_got(slot, ch).wait_recv()
                hop(r, ch, False, slot).start()
                cross(r, ch).start()
            return event

        pulls = [pull(1, far), pull(2, far_edge)]

        def early_events(*indices):
            for index in indices:
                if index >= early:
                    fill(index + FILL)
                for event in pulls:
                    event(chunk(index))

        perform(
            [
                ("own",), ("take", "far", "own"), ("fill", early), ("take", "edge", "own"),
                ("take", "edge", "other"), ("inward", *range(early)), ("take", "far", "other"),
                ("fill", early + 1), ("land", "rep", "other"), ("take", "last", "own"),
                ("fill", early + 2), ("land", "far", "own", False),
                ("inward", *range(early, LAG)), ("take", "last", "other"), ("land", "edge", "own", False),
                ("early", 0, 1), ("inward", *range(LAG, LAG + 2)), ("land", "edge", "other"),
                ("land", "far", "other"), ("early", 2), ("inward", LAG + 2), ("land", "last", "own", False),
                ("early", 3), ("inward", LAG + 3), ("land", "last", "other"),
            ],
            {"own": take_own, "take": take, "land": land, "inward": inward, "early": early_events, "fill": fill},
        )

        def arrived(ch):
            hop_other(ch).wait_recv()
            when_extra(ch, lambda: None, lambda: crossed(rep, ch).wait_recv())
            crossed(far, ch).wait_recv()

        clear()

        def ended():
            send_extra(chunk(count - 1))

        sweep([outer, *pulls], arrived, lambda: None, ended, LAG, True)

        mine = fsdp * n_tp + tp
        peers = [(a, k) for a in range(2) for k in range(n_tp) if a or k]

        def exchange(at):
            a, k = peers[at]
            to_side = other if a else fsdp
            to_tp = lax.rem(tp + k, n_tp)
            spot = sums.at[mine]
            return remote(spot, spot, sq_send, sq_recv, {"fsdp": to_side, "tp": to_tp})

        for at in range(len(peers)):
            exchange(at).start()
        with jax.named_scope("exchange"):
            seven = sums.at[pl.ds(0, len(peers))]
            remote(seven, seven, sq_send, sq_recv, {"fsdp": other}).wait_recv()
        square_total = jnp.sum(jnp.sum(sums[...], axis=0), keepdims=True)
        factor = 1.0 / jnp.sqrt(square_total / entry_count + 1e-06)
        total_out[...] = jnp.broadcast_to(factor, total_out.shape)
        remote(seven, seven, sq_send, sq_recv, {"fsdp": other}).wait_send()

    def tell():
        return remote(total_out, total_out, fa_send, fa_recv, {"rep": jnp.where(is_edge, near, edge)})

    on_middle(lambda: tell().start())
    with jax.named_scope("told"):
        on_edge(lambda: tell().wait_recv())
    factor_ref[...] = total_out[...]

    @on_middle
    def _():
        tell().wait_send()
        shares_sent()
        grads_sent(4, gz_in)
        grads_sent(6, gz_out)
        all_sent(2, columns, z_in)
        all_sent(3, columns, z_out)
        all_sent(3, columns, x_send)
        all_sent(1, extra_columns, ze_send)


def by_kernel(n_rep, n_tp, entry_count, gate_pre, up_pre, out_grad):
    rows, columns = gate_pre.shape
    tokens = rows * n_rep * 2
    half = out_grad.shape[1] // 2
    quarter = half // n_tp
    count = chunking(columns)[1]
    dma = pltpu.SemaphoreType.DMA
    block, whole = dma((n_rep, 2)), dma((n_rep,))
    return pl.pallas_call(
        functools.partial(gather_multiply, entry_count),
        out_shape=(
            pltpu.VMEM((half, columns), jnp.bfloat16),
            pltpu.VMEM((8, LANES), jnp.float32),
        ),
        in_specs=[pl.BlockSpec(memory_space=pl.ANY)] * 3,
        out_specs=(pl.BlockSpec(memory_space=pltpu.VMEM), pl.BlockSpec(memory_space=pltpu.VMEM)),
        scratch_shapes=[
            pltpu.VMEM((tokens, columns), jnp.bfloat16),
            pltpu.VMEM((tokens, half), jnp.bfloat16),
            pltpu.VMEM((half, tokens), jnp.bfloat16),
            pltpu.VMEM((rows, columns), jnp.bfloat16),
            pltpu.VMEM((rows, columns), jnp.bfloat16),
            pltpu.VMEM((rows, quarter), jnp.bfloat16),
            pltpu.VMEM((2 * n_tp, 8, LANES), jnp.float32),
            pltpu.VMEM((8, LANES), jnp.float32),
            pltpu.VMEM((half, 2 * WIDTH), jnp.float32),
            pltpu.VMEM((half, 2 * WIDTH), jnp.float32),
            dma((4,)), dma, dma, block, dma, dma, dma, block,
            dma, whole, dma, whole,
            dma((3, count)), dma, dma, dma, dma, dma, dma, dma((n_rep, count)),
            dma, dma, dma, dma,
        ],
        compiler_params=pltpu.CompilerParams(
            collective_id=0, has_side_effects=True, vmem_limit_bytes=VMEM_LIMIT * 3 // 4
        ),
    )(gate_pre, up_pre, out_grad)


def scale(summed, factors):
    half, columns = summed.shape
    rows = 128

    def body(summed_ref, factor_ref, out_ref, ready, sems):
        steps = half // rows
        depth = ready.shape[0]

        def leave(m):
            slot = lax.rem(m, depth)
            spot = pl.ds(pl.multiple_of(m * rows, rows), rows)
            return pltpu.make_async_copy(ready.at[slot], out_ref.at[spot, :], sems.at[slot])

        @pl.loop(0, steps)
        def _(m):
            slot = lax.rem(m, depth)
            spot = pl.ds(pl.multiple_of(m * rows, rows), rows)

            @pl.when(m >= depth)
            def _():
                leave(m - depth).wait()
            for at in range(0, columns, LANES):
                cols = pl.ds(at, LANES)
                scaled = summed_ref[spot, cols].astype(jnp.float32) * factor_ref[0:1, :]
                ready[slot, :, cols] = scaled.astype(ready.dtype)
            leave(m).start()

        @pl.loop(max(steps - depth, 0), steps)
        def _(m):
            leave(m).wait()

    return pl.pallas_call(
        body,
        out_shape=jax.ShapeDtypeStruct((half, columns), jnp.bfloat16),
        in_specs=[pl.BlockSpec(memory_space=pltpu.VMEM)] * 2,
        out_specs=pl.BlockSpec(memory_space=pl.ANY),
        scratch_shapes=[pltpu.VMEM((4, rows, columns), jnp.bfloat16), pltpu.SemaphoreType.DMA((4,))],
        compiler_params=pltpu.CompilerParams(vmem_limit_bytes=16 * 1024 * 1024),
    )(summed, factors)


def by_xla(gate_pre, up_pre, out_grad):
    hidden = (jax.nn.silu(gate_pre.astype(jnp.float32)) * up_pre.astype(jnp.float32)).astype(
        jnp.bfloat16
    )
    spread = lax.all_to_all(out_grad, "fsdp", split_axis=1, concat_axis=0, tiled=True)
    grad_rows = lax.all_gather(spread, "rep", axis=0, tiled=True)
    hidden_rows = lax.all_gather(hidden, ("rep", "fsdp"), axis=0, tiled=True)
    summed = lax.dot_general(
        grad_rows, hidden_rows, (((0,), (0,)), ((), ())), preferred_element_type=jnp.float32
    )
    return summed, jnp.sum(summed * summed)


def kernel_fits(n_rep, n_fsdp, n_tp, rows, columns, features):
    tokens, half = rows * n_rep * n_fsdp, features // n_fsdp
    held_bytes = 2 * (tokens * columns + 2 * tokens * half + half * columns + 2 * rows * columns)
    held_bytes += 16 * half * WIDTH
    aligned = rows % 128 == 0 and columns % LANES == 0 and half % (LANES * n_tp) == 0
    shaped = (n_rep, n_fsdp, n_tp) == (4, 2, 4) and columns >= max(12 * WIDTH, 7 * half // n_tp)
    return shaped and aligned and half % TILE == 0 and held_bytes < VMEM_LIMIT * 3 // 4


def solution(mesh):
    n_rep, n_fsdp, n_tp = (mesh.shape[axis] for axis in ("rep", "fsdp", "tp"))

    def on_device(gate_pre, up_pre, out_grad):
        half, columns = out_grad.shape[1] // n_fsdp, gate_pre.shape[1]
        entry_count = half * n_fsdp * columns * n_tp
        if kernel_fits(n_rep, n_fsdp, n_tp, *gate_pre.shape, out_grad.shape[1]):
            summed, factors = by_kernel(n_rep, n_tp, entry_count, gate_pre, up_pre, out_grad)
            return scale(summed, factors)
        summed, square_sum = by_xla(gate_pre, up_pre, out_grad)
        square_total = lax.psum(square_sum, ("fsdp", "tp"))
        factor = 1.0 / jnp.sqrt(square_total / entry_count + 1e-06)
        return (summed * factor).astype(jnp.bfloat16)

    return jax.shard_map(
        on_device,
        mesh=mesh,
        in_specs=(P(("rep", "fsdp"), "tp"), P(("rep", "fsdp"), "tp"), P(("rep", "fsdp"), None)),
        out_specs=P("fsdp", "tp"),
        check_vma=False,
    )
```

```python
import functools

import jax
import jax.numpy as jnp
from jax import lax
from jax.experimental import pallas as pl
from jax.experimental.pallas import tpu as pltpu
from jax.sharding import PartitionSpec as P

MESH = pl.DeviceIdType.MESH
LANES = 128
VMEM_LIMIT = 60 * 1024 * 1024
WIDTH = 256
TILE = 1024
LAG = 4
EDGE_LAG = 2
AHEAD = 4
FILL = 3
EXTRA = (5, 9)


class Chunk:
    def __init__(self, index, start, size):
        self.index, self.start, self.size = index, start, size

    @property
    def cols(self):
        start = self.start
        return pl.ds(start if isinstance(start, int) else pl.multiple_of(start, LANES), self.size)


def chunking(columns):
    full, rest = columns // WIDTH, columns % WIDTH

    def chunk(index):
        if isinstance(index, int) and index == full:
            return Chunk(index, full * WIDTH, rest)
        return Chunk(index, index * WIDTH, WIDTH)

    return full, full + (1 if rest else 0), chunk


def gather_multiply(
    entry_count, gate_ref, up_ref, grad_ref, out_ref, factor_ref,
    held, grads, turned, gate_in, up_in, across_in, sums, total_out,
    middle_part, end_part,
    local_sem, gx_send, gx_recv, gz_recv, gz_out, gz_in, gy_send, gy_recv,
    gs_send, gs_recv, gf_send, gf_recv,
    z_recv, z_out, z_in, zo_send, ze_send, x_send, xn_send, x_recv,
    sq_send, sq_recv, fa_send, fa_recv,
):
    rep = lax.axis_index("rep")
    fsdp = lax.axis_index("fsdp")
    tp = lax.axis_index("tp")
    rows, columns = gate_ref.shape
    half = grads.shape[1]
    n_tp = 4
    quarter = half // n_tp
    full, count, chunk = chunking(columns)
    extras = (*EXTRA, count - 1)
    extra_columns = len(EXTRA) * WIDTH + chunk(count - 1).size
    other = 1 - fsdp
    side = rep // 2
    edge, near, far, far_edge = 3 * side, 1 + side, 2 - side, 3 - 3 * side
    is_edge = rep == edge
    inner = jnp.where(is_edge, near, far)
    sibling = tp + 1 - 2 * lax.rem(tp, 2)
    opposite = lax.rem(tp + 2, n_tp)
    past = lax.rem(sibling + 2, n_tp)

    def rows_of(r, s):
        return pl.ds(pl.multiple_of((r * 2 + s) * rows, rows), rows)

    def quarter_of(t):
        return pl.ds(pl.multiple_of(t * quarter, LANES), quarter)

    def remote(src, dst, send, recv, device):
        return pltpu.make_async_remote_copy(
            src_ref=src, dst_ref=dst, send_sem=send, recv_sem=recv,
            device_id=device, device_id_type=MESH,
        )

    loads = [
        pltpu.make_async_copy(gate_ref, gate_in, local_sem.at[0]),
        pltpu.make_async_copy(up_ref, up_in, local_sem.at[1]),
        pltpu.make_async_copy(
            grad_ref.at[:, pl.ds(pl.multiple_of(fsdp * half, LANES), half)],
            grads.at[rows_of(rep, fsdp), :], local_sem.at[2],
        ),
        pltpu.make_async_copy(
            grad_ref.at[:, pl.ds(pl.multiple_of(other * half + tp * quarter, LANES), quarter)],
            across_in, local_sem.at[3],
        ),
    ]
    for load in loads:
        load.start()

    barrier = pltpu.get_barrier_semaphore()
    for peer in ({"fsdp": other}, {"tp": sibling}, {"tp": opposite}):
        pl.semaphore_signal(barrier, inc=1, device_id=peer, device_id_type=MESH)
    pl.semaphore_signal(barrier, inc=1, device_id={"rep": inner}, device_id_type=MESH)

    @pl.when(jnp.logical_not(is_edge))
    def _():
        pl.semaphore_signal(barrier, inc=1, device_id={"rep": edge}, device_id_type=MESH)

    with jax.named_scope("load"):
        for load in loads:
            load.wait()

    @pl.loop(0, columns // LANES)
    def _(at):
        cols = pl.ds(pl.multiple_of(at * LANES, LANES), LANES)
        gate = gate_in[:, cols].astype(jnp.float32)
        held[rows_of(rep, fsdp), cols] = (
            jax.nn.silu(gate) * up_in[:, cols].astype(jnp.float32)
        ).astype(held.dtype)

    with jax.named_scope("barrier"):
        pl.semaphore_wait(barrier, 4 + jnp.where(is_edge, 0, 1))

    def grad_across():
        return remote(across_in, grads.at[rows_of(rep, fsdp), quarter_of(tp)], gx_send, gx_recv, {"fsdp": other})

    def grad_spot(r, s, t):
        return grads.at[rows_of(r, s), quarter_of(t)]

    def grad_hop(r, s, inward):
        spot = grad_spot(r, s, tp)
        to = inner if inward else edge
        return remote(spot, spot, (gz_in if inward else gz_out), gz_recv.at[r, s], {"rep": to})

    def grad_got(r, s):
        spot = grad_spot(r, s, tp)
        return remote(spot, spot, gz_in, gz_recv.at[r, s], {"rep": inner})

    def over_y(r, s, t):
        spot = grad_spot(r, s, t)
        return remote(spot, spot, gy_send, gy_recv.at[r, s], {"tp": opposite})

    def to_sibling(r, s, t):
        spot = grad_spot(r, s, t)
        return remote(spot, spot, gs_send, gs_recv.at[r], {"tp": sibling})

    def pass_sibling(r, s, t):
        spot = grad_spot(r, s, t)
        return remote(spot, spot, gf_send, gf_recv.at[r], {"tp": sibling})

    def hop(r, ch, inward, slot):
        spot = held.at[rows_of(r, fsdp), ch.cols]
        to = inner if inward else edge
        return remote(spot, spot, z_in if inward else z_out, z_recv.at[slot, ch.index], {"rep": to})

    def hop_got(slot, ch):
        spot = held.at[pl.ds(0, rows), ch.cols]
        return remote(spot, spot, z_in, z_recv.at[slot, ch.index], {"rep": inner})

    def hop_other(ch):
        spot = held.at[rows_of(edge, other), ch.cols]
        return remote(spot, spot, zo_send, x_recv.at[edge, ch.index], {"rep": inner})

    def cross(r, ch, send=None):
        spot = held.at[rows_of(r, fsdp), ch.cols]
        return remote(spot, spot, x_send if send is None else send, x_recv.at[r, ch.index], {"fsdp": other})

    def crossed(r, ch):
        spot = held.at[rows_of(r, other), ch.cols]
        return remote(spot, spot, x_send, x_recv.at[r, ch.index], {"fsdp": other})

    def hop_extra(ch):
        spot = held.at[rows_of(near, other), ch.cols]
        return remote(spot, spot, ze_send, x_recv.at[near, ch.index], {"rep": jnp.where(is_edge, near, edge)})

    def all_sent(blocks, width, send):
        spot = held.at[pl.ds(0, blocks * rows), pl.ds(0, width)]
        remote(spot, spot, send, gx_recv, {"fsdp": other}).wait_send()

    def among_extra(index):
        return functools.reduce(jnp.logical_or, [index == at for at in EXTRA])

    def when_extra(ch, act, otherwise):
        if isinstance(ch.index, int):
            act() if ch.index in extras else otherwise()
            return
        pl.when(among_extra(ch.index))(act)
        pl.when(jnp.logical_not(among_extra(ch.index)))(otherwise)

    def on_edge(act):
        pl.when(is_edge)(act)

    def on_middle(act):
        pl.when(jnp.logical_not(is_edge))(act)

    def chunks_from(low, high, act):
        if low < min(high, full):
            @pl.loop(low, min(high, full))
            def _(index):
                act(chunk(index))
        if full < count == high:
            act(chunk(full))

    grad_across().start()
    grad_hop(rep, fsdp, True).start()
    on_middle(lambda: grad_hop(rep, fsdp, False).start())

    chunks_from(0, count, lambda ch: cross(rep, ch).start())
    early = 2

    def own_inward(ch):
        hop(rep, ch, True, jnp.where(is_edge, 0, 1)).start()

    chunks_from(0, early, own_inward)
    on_middle(lambda: chunks_from(0, early, lambda ch: hop(rep, ch, False, 0).start()))

    def share(r, s):
        over_y(r, s, tp).start()
        to_sibling(r, s, tp).start()

    def pass_on(r, s):
        over_y(r, s, opposite).wait_recv()
        pass_sibling(r, s, opposite).start()

    def settle(r, pairs):
        spots = grads.at[pl.ds(0, pairs * rows), pl.ds(0, quarter)]
        remote(spots, spots, gs_send, gs_recv.at[r], {"tp": sibling}).wait_recv()
        remote(spots, spots, gf_send, gf_recv.at[r], {"tp": sibling}).wait_recv()

    tile = 256

    def turn(r):
        spot = pl.ds(pl.multiple_of(r * 2 * rows, 2 * rows), 2 * rows)

        @pl.loop(0, half // tile)
        def _(m):
            part = pl.ds(pl.multiple_of(m * tile, tile), tile)
            turned[part, spot] = grads[spot, part].T

    def take_own():
        grad_across().wait_recv()
        grad_hop(rep, other, True).start()
        on_middle(lambda: grad_hop(rep, other, False).start())
        share(rep, other)

    def perform(plan, acts):
        for at, (name, *args) in enumerate(plan):
            with jax.named_scope(f"{name}{at}"):
                acts[name](*args)

    def grads_sent(blocks, send):
        all_sent(1, blocks * quarter, send)

    def shares_sent():
        grad_across().wait_send()
        for send in (gy_send, gs_send, gf_send):
            grads_sent(7, send)

    def clear():
        sums[fsdp * n_tp + tp] = jnp.zeros(sums.shape[1:], sums.dtype)

    def leave(product, spot, ch, squared):
        out_ref[spot, ch.cols] = product.astype(out_ref.dtype)
        if squared:
            squares = jnp.sum((product * product).reshape(TILE // 8, 8, ch.size), axis=0)
            total = squares[:, :LANES]
            for at in range(LANES, ch.size, LANES):
                total = total + squares[:, at:at + LANES]
            sums[fsdp * n_tp + tp] += total

    def tile_of(m):
        return pl.ds(pl.multiple_of(m * TILE, TILE), TILE)

    def multiply_tile(ch, m, squared):
        spot = tile_of(m)
        product = jnp.dot(turned[spot, :], held[:, ch.cols], preferred_element_type=jnp.float32)
        leave(product, spot, ch, squared)

    pair = 2 * rows
    ends = {"first": pl.multiple_of(edge * pair, pair), "late": pl.multiple_of(far_edge * pair, pair)}

    def part(spot, ch, start, size):
        tokens = pl.ds(start, size)
        return jnp.dot(turned[spot, tokens], held[tokens, ch.cols], preferred_element_type=jnp.float32)

    def kept(ch):
        return pl.ds((ch.index - (count - 2)) * WIDTH, ch.size)

    def begin(ch):
        @pl.loop(0, tiles)
        def _(m):
            spot = tile_of(m)
            middle_part[spot, kept(ch)] = part(spot, ch, pair, 2 * pair)

    def begin_end(ch):
        @pl.loop(0, tiles)
        def _(m):
            spot = tile_of(m)
            end_part[spot, kept(ch)] = part(spot, ch, ends["first"], pair)

    def complete(ch, squared):
        @pl.loop(0, tiles)
        def _(m):
            spot = tile_of(m)
            both = end_part[spot, kept(ch)] + part(spot, ch, ends["late"], pair)
            leave(middle_part[spot, kept(ch)] + both, spot, ch, squared)

    tiles = half // TILE

    def finish(ch, arrived, squared):
        with jax.named_scope("arrived_last"):
            arrived(ch)
        with jax.named_scope("multiply_last"):
            pl.loop(0, tiles)(lambda m: multiply_tile(ch, m, squared))

    def sweep(events, arrived_but_last, between, ended, lag, squared):
        def arrived(ch):
            arrived_but_last(ch)
            crossed(far_edge, ch).wait_recv()

        places = [at * tiles // len(events) for at in range(len(events))]

        def step(index, events=events):
            ch, lagging = chunk(index), chunk(index - lag)
            with jax.named_scope("arrived"):
                arrived(lagging)

            @pl.loop(0, tiles)
            def _(m):
                for at, (place, event) in enumerate(zip(places, events)):
                    def run():
                        with jax.named_scope(f"event{at}"):
                            event(ch)
                    pl.when(m == place)(run)
                with jax.named_scope("multiply"):
                    multiply_tile(lagging, m, squared)

        pl.loop(LAG, count - 2)(step)
        between()
        ahead, far_pull, last_pull = events
        last_two = chunk(count - 2), chunk(count - 1)
        for at, pull in ((0, far_pull), (1, last_pull)):
            step(count - 2 + at, [lambda ch: ahead(ch), lambda ch: pull(last_two[0]), lambda ch: pull(last_two[1])])
        ended()
        chunks_from(count - lag, count - 2, lambda ch: finish(ch, arrived, squared))
        for ch in last_two:
            with jax.named_scope("begin"):
                arrived_but_last(ch)
                begin(ch)
                if squared:
                    begin_end(ch)
        for ch in last_two:
            with jax.named_scope("late"):
                crossed(far_edge, ch).wait_recv()
                complete(ch, squared)

    @on_edge
    def _():
        places = {"near": near, "far": far, "last": far_edge}
        sides = {"own": fsdp, "other": other}

        def take(name, s):
            grad_got(places[name], sides[s]).wait_recv()
            share(places[name], sides[s])

        def land(name, s, whole):
            r = rep if name == "rep" else places[name]
            pass_on(r, sides[s])
            if whole:
                settle(r, 1 if name == "rep" else 2)
                turn(r)

        def relay(*indices):
            for index in indices:
                if index + early < count:
                    own_inward(chunk(index + early))
                if index < count:
                    crossed(edge, chunk(index)).wait_recv()
                    hop_other(chunk(index)).start()

        def pull(slot, r):
            def event(ch):
                hop_got(slot, ch).wait_recv()
                cross(r, ch).start()
            return event

        def pull_near(ch):
            hop_got(0, ch).wait_recv()
            when_extra(ch, lambda: None, lambda: cross(near, ch, xn_send).start())

        pulls = [pull(1, far), pull(2, far_edge)]

        def near_at(*indices):
            for index in indices:
                pull_near(chunk(index))

        def near_ahead(ch):
            index = ch.index + FILL
            if isinstance(index, int):
                if index < count:
                    near_at(index)
                return
            pl.when(index < full)(lambda: near_at(index))
            if full < count:
                pl.when(index == full)(lambda: near_at(full))

        def early_events(*indices):
            for index in indices:
                if index >= early:
                    near_at(index + FILL)
                for event in pulls:
                    event(chunk(index))

        def arrived(ch):
            crossed(near, ch).wait_recv()
            crossed(far, ch).wait_recv()

        def compute(index):
            def whole(ch):
                arrived(ch)
                crossed(far_edge, ch).wait_recv()
            finish(chunk(index), whole, False)

        def batch(k):
            return range(k * count // 8, (k + 1) * count // 8)

        perform(
            [
                ("own",), ("take", "near", "own"), ("relay", *batch(0)), ("near", *range(early)),
                ("take", "near", "other"), ("land", "rep", "other", True), ("relay", *batch(1)),
                ("take", "far", "own"), ("near", early), ("land", "near", "own", False),
                ("relay", *batch(2)), ("take", "far", "other"), ("near", early + 1),
                ("land", "near", "other", True), ("relay", *batch(3)), ("take", "last", "own"),
                ("near", early + 2), ("land", "far", "own", False), ("relay", *batch(4)),
                ("take", "last", "other"), ("land", "far", "other", True), ("relay", *batch(5)),
                ("early", 0), ("relay", *batch(6)), ("early", 1), ("land", "last", "own", False),
                ("relay", *batch(7)), ("early", 2), ("land", "last", "other", True),
                ("compute", 0), ("early", 3), ("compute", 1),
            ],
            {"own": take_own, "take": take, "land": land, "relay": relay, "early": early_events, "near": near_at,
             "compute": compute},
        )

        def between():
            shares_sent()
            grads_sent(2, gz_in)
            all_sent(1, columns, z_in)
            all_sent(1, columns, zo_send)
            for index in (count - 2, count - 1):
                begin_end(chunk(index))

        sweep([near_ahead, *pulls], arrived, between, lambda: None, EDGE_LAG, False)
        all_sent(1, columns - extra_columns, xn_send)
        all_sent(3, columns, x_send)

    @on_middle
    def _():
        places = {"edge": edge, "far": far, "last": far_edge}
        sides = {"own": fsdp, "other": other}

        def take(name, s):
            r, s = places[name], sides[s]
            grad_got(r, s).wait_recv()
            grad_hop(r, s, name == "edge").start()
            share(r, s)

        def land(name, s, whole=True):
            r = rep if name == "rep" else places[name]
            pass_on(r, sides[s])
            if whole:
                settle(r, 1 if name == "rep" else 2)
                turn(r)

        def inward(*indices):
            for index in indices:
                ch = chunk(index)
                if not isinstance(index, int) or index >= early:
                    own_inward(ch)
                hop_got(0, ch).wait_recv()
                hop(edge, ch, True, 2).start()

        def fill(*indices):
            for index in indices:
                hop(rep, chunk(index), False, 0).start()

        def outer(ch):
            if isinstance(ch.index, int):
                if ch.index + FILL < count:
                    fill(ch.index + FILL)
            else:
                pl.when(ch.index + FILL < full)(lambda: fill(ch.index + FILL))
                if full < count:
                    pl.when(ch.index + FILL == full)(lambda: fill(full))
            follow(ch.index + AHEAD)
            if not isinstance(ch.index, int):
                pl.when(among_extra(ch.index))(lambda: send_extra(ch))

        def send_extra(ch):
            crossed(rep, ch).wait_recv()
            hop_extra(ch).start()

        def follow(index):
            if isinstance(index, int):
                if index < count:
                    inward(index)
                return
            pl.when(index < full)(lambda: inward(index))
            if full < count:
                pl.when(index == full)(lambda: inward(full))

        def pull(slot, r):
            def event(ch):
                hop_got(slot, ch).wait_recv()
                hop(r, ch, False, slot).start()
                cross(r, ch).start()
            return event

        pulls = [pull(1, far), pull(2, far_edge)]

        def early_events(*indices):
            for index in indices:
                if index >= early:
                    fill(index + FILL)
                for event in pulls:
                    event(chunk(index))

        perform(
            [
                ("own",), ("take", "far", "own"), ("fill", early), ("take", "edge", "own"),
                ("take", "edge", "other"), ("inward", *range(early)), ("take", "far", "other"),
                ("fill", early + 1), ("land", "rep", "other"), ("take", "last", "own"),
                ("fill", early + 2), ("land", "far", "own", False),
                ("inward", *range(early, LAG)), ("take", "last", "other"), ("land", "edge", "own", False),
                ("early", 0, 1), ("inward", *range(LAG, LAG + 2)), ("land", "edge", "other"),
                ("land", "far", "other"), ("early", 2), ("inward", LAG + 2), ("land", "last", "own", False),
                ("early", 3), ("inward", LAG + 3), ("land", "last", "other"),
            ],
            {"own": take_own, "take": take, "land": land, "inward": inward, "early": early_events, "fill": fill},
        )

        def arrived(ch):
            hop_other(ch).wait_recv()
            when_extra(ch, lambda: None, lambda: crossed(rep, ch).wait_recv())
            crossed(far, ch).wait_recv()

        clear()

        def ended():
            send_extra(chunk(count - 1))

        sweep([outer, *pulls], arrived, lambda: None, ended, LAG, True)

        mine = fsdp * n_tp + tp
        peers = [(a, k) for a in range(2) for k in range(n_tp) if a or k]

        def exchange(at):
            a, k = peers[at]
            to_side = other if a else fsdp
            to_tp = lax.rem(tp + k, n_tp)
            spot = sums.at[mine]
            return remote(spot, spot, sq_send, sq_recv, {"fsdp": to_side, "tp": to_tp})

        for at in range(len(peers)):
            exchange(at).start()
        with jax.named_scope("exchange"):
            seven = sums.at[pl.ds(0, len(peers))]
            remote(seven, seven, sq_send, sq_recv, {"fsdp": other}).wait_recv()
        square_total = jnp.sum(jnp.sum(sums[...], axis=0), keepdims=True)
        factor = 1.0 / jnp.sqrt(square_total / entry_count + 1e-06)
        total_out[...] = jnp.broadcast_to(factor, total_out.shape)
        remote(seven, seven, sq_send, sq_recv, {"fsdp": other}).wait_send()

    def tell():
        return remote(total_out, total_out, fa_send, fa_recv, {"rep": jnp.where(is_edge, near, edge)})

    on_middle(lambda: tell().start())
    with jax.named_scope("told"):
        on_edge(lambda: tell().wait_recv())
    factor_ref[...] = total_out[...]

    @on_middle
    def _():
        tell().wait_send()
        shares_sent()
        grads_sent(4, gz_in)
        grads_sent(6, gz_out)
        all_sent(2, columns, z_in)
        all_sent(3, columns, z_out)
        all_sent(3, columns, x_send)
        all_sent(1, extra_columns, ze_send)


def by_kernel(n_rep, n_tp, entry_count, gate_pre, up_pre, out_grad):
    rows, columns = gate_pre.shape
    tokens = rows * n_rep * 2
    half = out_grad.shape[1] // 2
    quarter = half // n_tp
    count = chunking(columns)[1]
    dma = pltpu.SemaphoreType.DMA
    block, whole = dma((n_rep, 2)), dma((n_rep,))
    return pl.pallas_call(
        functools.partial(gather_multiply, entry_count),
        out_shape=(
            pltpu.VMEM((half, columns), jnp.bfloat16),
            pltpu.VMEM((8, LANES), jnp.float32),
        ),
        in_specs=[pl.BlockSpec(memory_space=pl.ANY)] * 3,
        out_specs=(pl.BlockSpec(memory_space=pltpu.VMEM), pl.BlockSpec(memory_space=pltpu.VMEM)),
        scratch_shapes=[
            pltpu.VMEM((tokens, columns), jnp.bfloat16),
            pltpu.VMEM((tokens, half), jnp.bfloat16),
            pltpu.VMEM((half, tokens), jnp.bfloat16),
            pltpu.VMEM((rows, columns), jnp.bfloat16),
            pltpu.VMEM((rows, columns), jnp.bfloat16),
            pltpu.VMEM((rows, quarter), jnp.bfloat16),
            pltpu.VMEM((2 * n_tp, 8, LANES), jnp.float32),
            pltpu.VMEM((8, LANES), jnp.float32),
            pltpu.VMEM((half, 2 * WIDTH), jnp.float32),
            pltpu.VMEM((half, 2 * WIDTH), jnp.float32),
            dma((4,)), dma, dma, block, dma, dma, dma, block,
            dma, whole, dma, whole,
            dma((3, count)), dma, dma, dma, dma, dma, dma, dma((n_rep, count)),
            dma, dma, dma, dma,
        ],
        compiler_params=pltpu.CompilerParams(
            collective_id=0, has_side_effects=True, vmem_limit_bytes=VMEM_LIMIT * 3 // 4
        ),
    )(gate_pre, up_pre, out_grad)


def scale(summed, factors):
    half, columns = summed.shape
    rows = 128

    def body(summed_ref, factor_ref, out_ref, ready, sems):
        steps = half // rows
        depth = ready.shape[0]

        def leave(m):
            slot = lax.rem(m, depth)
            spot = pl.ds(pl.multiple_of(m * rows, rows), rows)
            return pltpu.make_async_copy(ready.at[slot], out_ref.at[spot, :], sems.at[slot])

        @pl.loop(0, steps)
        def _(m):
            slot = lax.rem(m, depth)
            spot = pl.ds(pl.multiple_of(m * rows, rows), rows)

            @pl.when(m >= depth)
            def _():
                leave(m - depth).wait()
            for at in range(0, columns, LANES):
                cols = pl.ds(at, LANES)
                scaled = summed_ref[spot, cols].astype(jnp.float32) * factor_ref[0:1, :]
                ready[slot, :, cols] = scaled.astype(ready.dtype)
            leave(m).start()

        @pl.loop(max(steps - depth, 0), steps)
        def _(m):
            leave(m).wait()

    return pl.pallas_call(
        body,
        out_shape=jax.ShapeDtypeStruct((half, columns), jnp.bfloat16),
        in_specs=[pl.BlockSpec(memory_space=pltpu.VMEM)] * 2,
        out_specs=pl.BlockSpec(memory_space=pl.ANY),
        scratch_shapes=[pltpu.VMEM((4, rows, columns), jnp.bfloat16), pltpu.SemaphoreType.DMA((4,))],
        compiler_params=pltpu.CompilerParams(vmem_limit_bytes=16 * 1024 * 1024),
    )(summed, factors)


def by_xla(gate_pre, up_pre, out_grad):
    hidden = (jax.nn.silu(gate_pre.astype(jnp.float32)) * up_pre.astype(jnp.float32)).astype(
        jnp.bfloat16
    )
    spread = lax.all_to_all(out_grad, "fsdp", split_axis=1, concat_axis=0, tiled=True)
    grad_rows = lax.all_gather(spread, "rep", axis=0, tiled=True)
    hidden_rows = lax.all_gather(hidden, ("rep", "fsdp"), axis=0, tiled=True)
    summed = lax.dot_general(
        grad_rows, hidden_rows, (((0,), (0,)), ((), ())), preferred_element_type=jnp.float32
    )
    return summed, jnp.sum(summed * summed)


def kernel_fits(n_rep, n_fsdp, n_tp, rows, columns, features):
    tokens, half = rows * n_rep * n_fsdp, features // n_fsdp
    held_bytes = 2 * (tokens * columns + 2 * tokens * half + half * columns + 2 * rows * columns)
    held_bytes += 16 * half * WIDTH
    aligned = rows % 128 == 0 and columns % LANES == 0 and half % (LANES * n_tp) == 0
    shaped = (n_rep, n_fsdp, n_tp) == (4, 2, 4) and columns >= max(12 * WIDTH, 7 * half // n_tp)
    return shaped and aligned and half % TILE == 0 and held_bytes < VMEM_LIMIT * 3 // 4


def solution(mesh):
    n_rep, n_fsdp, n_tp = (mesh.shape[axis] for axis in ("rep", "fsdp", "tp"))

    def on_device(gate_pre, up_pre, out_grad):
        half, columns = out_grad.shape[1] // n_fsdp, gate_pre.shape[1]
        entry_count = half * n_fsdp * columns * n_tp
        if kernel_fits(n_rep, n_fsdp, n_tp, *gate_pre.shape, out_grad.shape[1]):
            summed, factors = by_kernel(n_rep, n_tp, entry_count, gate_pre, up_pre, out_grad)
            return scale(summed, factors)
        summed, square_sum = by_xla(gate_pre, up_pre, out_grad)
        square_total = lax.psum(square_sum, ("fsdp", "tp"))
        factor = 1.0 / jnp.sqrt(square_total / entry_count + 1e-06)
        return (summed * factor).astype(jnp.bfloat16)

    return jax.shard_map(
        on_device,
        mesh=mesh,
        in_specs=(P(("rep", "fsdp"), "tp"), P(("rep", "fsdp"), "tp"), P(("rep", "fsdp"), None)),
        out_specs=P("fsdp", "tp"),
        check_vma=False,
    )
```

```python
import functools

import jax
import jax.numpy as jnp
from jax import lax
from jax.experimental import pallas as pl
from jax.experimental.pallas import tpu as pltpu
from jax.sharding import PartitionSpec as P

MESH = pl.DeviceIdType.MESH
LANES = 128
VMEM_LIMIT = 60 * 1024 * 1024
WIDTH = 256
TILE = 1024
LAG = 4
EDGE_LAG = 2
AHEAD = 4
FILL = 3
EXTRA = (8,)


class Chunk:
    def __init__(self, index, start, size):
        self.index, self.start, self.size = index, start, size

    @property
    def cols(self):
        start = self.start
        return pl.ds(start if isinstance(start, int) else pl.multiple_of(start, LANES), self.size)


def chunking(columns):
    full, rest = columns // WIDTH, columns % WIDTH

    def chunk(index):
        if isinstance(index, int) and index == full:
            return Chunk(index, full * WIDTH, rest)
        return Chunk(index, index * WIDTH, WIDTH)

    return full, full + (1 if rest else 0), chunk


def gather_multiply(
    entry_count, gate_ref, up_ref, grad_ref, out_ref, factor_ref,
    held, grads, turned, gate_in, up_in, across_in, sums, total_out,
    middle_part, end_part,
    local_sem, gx_send, gx_recv, gz_recv, gz_out, gz_in, gy_send, gy_recv,
    gs_send, gs_recv, gf_send, gf_recv,
    z_recv, z_out, z_in, zo_send, ze_send, x_send, xn_send, x_recv,
    sq_send, sq_recv, fa_send, fa_recv,
):
    rep = lax.axis_index("rep")
    fsdp = lax.axis_index("fsdp")
    tp = lax.axis_index("tp")
    rows, columns = gate_ref.shape
    half = grads.shape[1]
    n_tp = 4
    quarter = half // n_tp
    full, count, chunk = chunking(columns)
    extras = (*EXTRA, count - 1)
    extra_columns = len(EXTRA) * WIDTH + chunk(count - 1).size
    other = 1 - fsdp
    side = rep // 2
    edge, near, far, far_edge = 3 * side, 1 + side, 2 - side, 3 - 3 * side
    is_edge = rep == edge
    inner = jnp.where(is_edge, near, far)
    sibling = tp + 1 - 2 * lax.rem(tp, 2)
    opposite = lax.rem(tp + 2, n_tp)
    past = lax.rem(sibling + 2, n_tp)

    def rows_of(r, s):
        return pl.ds(pl.multiple_of((r * 2 + s) * rows, rows), rows)

    def quarter_of(t):
        return pl.ds(pl.multiple_of(t * quarter, LANES), quarter)

    def remote(src, dst, send, recv, device):
        return pltpu.make_async_remote_copy(
            src_ref=src, dst_ref=dst, send_sem=send, recv_sem=recv,
            device_id=device, device_id_type=MESH,
        )

    loads = [
        pltpu.make_async_copy(gate_ref, gate_in, local_sem.at[0]),
        pltpu.make_async_copy(up_ref, up_in, local_sem.at[1]),
        pltpu.make_async_copy(
            grad_ref.at[:, pl.ds(pl.multiple_of(fsdp * half, LANES), half)],
            grads.at[rows_of(rep, fsdp), :], local_sem.at[2],
        ),
        pltpu.make_async_copy(
            grad_ref.at[:, pl.ds(pl.multiple_of(other * half + tp * quarter, LANES), quarter)],
            across_in, local_sem.at[3],
        ),
    ]
    for load in loads:
        load.start()

    barrier = pltpu.get_barrier_semaphore()
    for peer in ({"fsdp": other}, {"tp": sibling}, {"tp": opposite}):
        pl.semaphore_signal(barrier, inc=1, device_id=peer, device_id_type=MESH)
    pl.semaphore_signal(barrier, inc=1, device_id={"rep": inner}, device_id_type=MESH)

    @pl.when(jnp.logical_not(is_edge))
    def _():
        pl.semaphore_signal(barrier, inc=1, device_id={"rep": edge}, device_id_type=MESH)

    with jax.named_scope("load"):
        for load in loads:
            load.wait()

    @pl.loop(0, columns // LANES)
    def _(at):
        cols = pl.ds(pl.multiple_of(at * LANES, LANES), LANES)
        gate = gate_in[:, cols].astype(jnp.float32)
        held[rows_of(rep, fsdp), cols] = (
            jax.nn.silu(gate) * up_in[:, cols].astype(jnp.float32)
        ).astype(held.dtype)

    with jax.named_scope("barrier"):
        pl.semaphore_wait(barrier, 4 + jnp.where(is_edge, 0, 1))

    def grad_across():
        return remote(across_in, grads.at[rows_of(rep, fsdp), quarter_of(tp)], gx_send, gx_recv, {"fsdp": other})

    def grad_spot(r, s, t):
        return grads.at[rows_of(r, s), quarter_of(t)]

    def grad_hop(r, s, inward):
        spot = grad_spot(r, s, tp)
        to = inner if inward else edge
        return remote(spot, spot, (gz_in if inward else gz_out), gz_recv.at[r, s], {"rep": to})

    def grad_got(r, s):
        spot = grad_spot(r, s, tp)
        return remote(spot, spot, gz_in, gz_recv.at[r, s], {"rep": inner})

    def over_y(r, s, t):
        spot = grad_spot(r, s, t)
        return remote(spot, spot, gy_send, gy_recv.at[r, s], {"tp": opposite})

    def to_sibling(r, s, t):
        spot = grad_spot(r, s, t)
        return remote(spot, spot, gs_send, gs_recv.at[r], {"tp": sibling})

    def pass_sibling(r, s, t):
        spot = grad_spot(r, s, t)
        return remote(spot, spot, gf_send, gf_recv.at[r], {"tp": sibling})

    def hop(r, ch, inward, slot):
        spot = held.at[rows_of(r, fsdp), ch.cols]
        to = inner if inward else edge
        return remote(spot, spot, z_in if inward else z_out, z_recv.at[slot, ch.index], {"rep": to})

    def hop_got(slot, ch):
        spot = held.at[pl.ds(0, rows), ch.cols]
        return remote(spot, spot, z_in, z_recv.at[slot, ch.index], {"rep": inner})

    def hop_other(ch):
        spot = held.at[rows_of(edge, other), ch.cols]
        return remote(spot, spot, zo_send, x_recv.at[edge, ch.index], {"rep": inner})

    def cross(r, ch, send=None):
        spot = held.at[rows_of(r, fsdp), ch.cols]
        return remote(spot, spot, x_send if send is None else send, x_recv.at[r, ch.index], {"fsdp": other})

    def crossed(r, ch):
        spot = held.at[rows_of(r, other), ch.cols]
        return remote(spot, spot, x_send, x_recv.at[r, ch.index], {"fsdp": other})

    def hop_extra(ch):
        spot = held.at[rows_of(near, other), ch.cols]
        return remote(spot, spot, ze_send, x_recv.at[near, ch.index], {"rep": jnp.where(is_edge, near, edge)})

    def all_sent(blocks, width, send):
        spot = held.at[pl.ds(0, blocks * rows), pl.ds(0, width)]
        remote(spot, spot, send, gx_recv, {"fsdp": other}).wait_send()

    def among_extra(index):
        return functools.reduce(jnp.logical_or, [index == at for at in EXTRA])

    def when_extra(ch, act, otherwise):
        if isinstance(ch.index, int):
            act() if ch.index in extras else otherwise()
            return
        pl.when(among_extra(ch.index))(act)
        pl.when(jnp.logical_not(among_extra(ch.index)))(otherwise)

    def on_edge(act):
        pl.when(is_edge)(act)

    def on_middle(act):
        pl.when(jnp.logical_not(is_edge))(act)

    def chunks_from(low, high, act):
        if low < min(high, full):
            @pl.loop(low, min(high, full))
            def _(index):
                act(chunk(index))
        if full < count == high:
            act(chunk(full))

    grad_across().start()
    grad_hop(rep, fsdp, True).start()
    on_middle(lambda: grad_hop(rep, fsdp, False).start())

    chunks_from(0, count, lambda ch: cross(rep, ch).start())
    early = 2

    def own_inward(ch):
        hop(rep, ch, True, jnp.where(is_edge, 0, 1)).start()

    chunks_from(0, early, own_inward)
    on_middle(lambda: chunks_from(0, early, lambda ch: hop(rep, ch, False, 0).start()))

    def share(r, s):
        over_y(r, s, tp).start()
        to_sibling(r, s, tp).start()

    def pass_on(r, s):
        over_y(r, s, opposite).wait_recv()
        pass_sibling(r, s, opposite).start()

    def settle(r, pairs):
        spots = grads.at[pl.ds(0, pairs * rows), pl.ds(0, quarter)]
        remote(spots, spots, gs_send, gs_recv.at[r], {"tp": sibling}).wait_recv()
        remote(spots, spots, gf_send, gf_recv.at[r], {"tp": sibling}).wait_recv()

    tile = 256

    def turn(r):
        spot = pl.ds(pl.multiple_of(r * 2 * rows, 2 * rows), 2 * rows)

        @pl.loop(0, half // tile)
        def _(m):
            part = pl.ds(pl.multiple_of(m * tile, tile), tile)
            turned[part, spot] = grads[spot, part].T

    def take_own():
        grad_across().wait_recv()
        grad_hop(rep, other, True).start()
        on_middle(lambda: grad_hop(rep, other, False).start())
        share(rep, other)

    def perform(plan, acts):
        for at, (name, *args) in enumerate(plan):
            with jax.named_scope(f"{name}{at}"):
                acts[name](*args)

    def grads_sent(blocks, send):
        all_sent(1, blocks * quarter, send)

    def shares_sent():
        grad_across().wait_send()
        for send in (gy_send, gs_send, gf_send):
            grads_sent(7, send)

    def clear():
        sums[fsdp * n_tp + tp] = jnp.zeros(sums.shape[1:], sums.dtype)

    def leave(product, spot, ch, squared):
        out_ref[spot, ch.cols] = product.astype(out_ref.dtype)
        if squared:
            squares = jnp.sum((product * product).reshape(TILE // 8, 8, ch.size), axis=0)
            total = squares[:, :LANES]
            for at in range(LANES, ch.size, LANES):
                total = total + squares[:, at:at + LANES]
            sums[fsdp * n_tp + tp] += total

    def tile_of(m):
        return pl.ds(pl.multiple_of(m * TILE, TILE), TILE)

    def multiply_tile(ch, m, squared):
        spot = tile_of(m)
        product = jnp.dot(turned[spot, :], held[:, ch.cols], preferred_element_type=jnp.float32)
        leave(product, spot, ch, squared)

    pair = 2 * rows
    ends = {"first": pl.multiple_of(edge * pair, pair), "late": pl.multiple_of(far_edge * pair, pair)}

    def part(spot, ch, start, size):
        tokens = pl.ds(start, size)
        return jnp.dot(turned[spot, tokens], held[tokens, ch.cols], preferred_element_type=jnp.float32)

    def kept(ch):
        return pl.ds((ch.index - (count - 2)) * WIDTH, ch.size)

    def begin(ch):
        @pl.loop(0, tiles)
        def _(m):
            spot = tile_of(m)
            middle_part[spot, kept(ch)] = part(spot, ch, pair, 2 * pair)

    def begin_end(ch):
        @pl.loop(0, tiles)
        def _(m):
            spot = tile_of(m)
            end_part[spot, kept(ch)] = part(spot, ch, ends["first"], pair)

    def complete(ch, squared):
        @pl.loop(0, tiles)
        def _(m):
            spot = tile_of(m)
            both = end_part[spot, kept(ch)] + part(spot, ch, ends["late"], pair)
            leave(middle_part[spot, kept(ch)] + both, spot, ch, squared)

    tiles = half // TILE

    def finish(ch, arrived, squared):
        with jax.named_scope("arrived_last"):
            arrived(ch)
        with jax.named_scope("multiply_last"):
            pl.loop(0, tiles)(lambda m: multiply_tile(ch, m, squared))

    def sweep(events, arrived_but_last, between, ended, lag, squared):
        def arrived(ch):
            arrived_but_last(ch)
            crossed(far_edge, ch).wait_recv()

        places = [at * tiles // len(events) for at in range(len(events))]

        def step(index):
            ch, lagging = chunk(index), chunk(index - lag)
            plan = [(place, event, ch) for place, event in zip(places, events)]
            plan.insert(sum(place == 0 for place in places), (0, arrived, lagging))

            @pl.loop(0, tiles)
            def _(m):
                for at, (place, event, subject) in enumerate(plan):
                    def run():
                        with jax.named_scope(f"event{at}"):
                            event(subject)
                    pl.when(m == place)(run)
                with jax.named_scope("multiply"):
                    multiply_tile(lagging, m, squared)

        pl.loop(LAG, count - 2)(step)
        between()
        ahead, far_pull, last_pull = events
        last_two = chunk(count - 2), chunk(count - 1)
        for index, pull in ((count - 2, far_pull), (count - 1, last_pull)):
            with jax.named_scope("pull_last"):
                ahead(chunk(index))
                for ch in last_two:
                    pull(ch)
            finish(chunk(index - lag), arrived, squared)
        ended()
        chunks_from(count - lag, count - 2, lambda ch: finish(ch, arrived, squared))
        for ch in last_two:
            with jax.named_scope("begin"):
                arrived_but_last(ch)
                begin(ch)
                if squared:
                    begin_end(ch)
        for ch in last_two:
            with jax.named_scope("late"):
                crossed(far_edge, ch).wait_recv()
                complete(ch, squared)

    @on_edge
    def _():
        places = {"near": near, "far": far, "last": far_edge}
        sides = {"own": fsdp, "other": other}

        def take(name, s):
            grad_got(places[name], sides[s]).wait_recv()
            share(places[name], sides[s])

        def land(name, s, whole):
            r = rep if name == "rep" else places[name]
            pass_on(r, sides[s])
            if whole:
                settle(r, 1 if name == "rep" else 2)
                turn(r)

        def relay(*indices):
            for index in indices:
                if index + early < count:
                    own_inward(chunk(index + early))
                if index < count:
                    crossed(edge, chunk(index)).wait_recv()
                    hop_other(chunk(index)).start()

        def pull(slot, r):
            def event(ch):
                hop_got(slot, ch).wait_recv()
                cross(r, ch).start()
            return event

        def pull_near(ch):
            hop_got(0, ch).wait_recv()
            when_extra(ch, lambda: None, lambda: cross(near, ch, xn_send).start())

        pulls = [pull(1, far), pull(2, far_edge)]

        def near_at(*indices):
            for index in indices:
                pull_near(chunk(index))

        def near_ahead(ch):
            index = ch.index + FILL
            if isinstance(index, int):
                if index < count:
                    near_at(index)
                return
            pl.when(index < full)(lambda: near_at(index))
            if full < count:
                pl.when(index == full)(lambda: near_at(full))

        def early_events(*indices):
            for index in indices:
                if index >= early:
                    near_at(index + FILL)
                for event in pulls:
                    event(chunk(index))

        def arrived(ch):
            crossed(near, ch).wait_recv()
            crossed(far, ch).wait_recv()

        def compute(index):
            def whole(ch):
                arrived(ch)
                crossed(far_edge, ch).wait_recv()
            finish(chunk(index), whole, False)

        def batch(k):
            return range(k * count // 8, (k + 1) * count // 8)

        perform(
            [
                ("own",), ("take", "near", "own"), ("relay", *batch(0)), ("near", *range(early)),
                ("take", "near", "other"), ("land", "rep", "other", True), ("relay", *batch(1)),
                ("take", "far", "own"), ("near", early), ("land", "near", "own", False),
                ("relay", *batch(2)), ("take", "far", "other"), ("near", early + 1),
                ("land", "near", "other", True), ("relay", *batch(3)), ("take", "last", "own"),
                ("near", early + 2), ("land", "far", "own", False), ("relay", *batch(4)),
                ("take", "last", "other"), ("land", "far", "other", True), ("relay", *batch(5)),
                ("early", 0), ("relay", *batch(6)), ("early", 1), ("land", "last", "own", False),
                ("relay", *batch(7)), ("early", 2), ("land", "last", "other", True),
                ("compute", 0), ("early", 3), ("compute", 1),
            ],
            {"own": take_own, "take": take, "land": land, "relay": relay, "early": early_events, "near": near_at,
             "compute": compute},
        )

        def between():
            shares_sent()
            grads_sent(2, gz_in)
            all_sent(1, columns, z_in)
            all_sent(1, columns, zo_send)
            for index in (count - 2, count - 1):
                begin_end(chunk(index))

        sweep([near_ahead, *pulls], arrived, between, lambda: None, EDGE_LAG, False)
        all_sent(1, columns - extra_columns, xn_send)
        all_sent(3, columns, x_send)

    @on_middle
    def _():
        places = {"edge": edge, "far": far, "last": far_edge}
        sides = {"own": fsdp, "other": other}

        def take(name, s):
            r, s = places[name], sides[s]
            grad_got(r, s).wait_recv()
            grad_hop(r, s, name == "edge").start()
            share(r, s)

        def land(name, s, whole=True):
            r = rep if name == "rep" else places[name]
            pass_on(r, sides[s])
            if whole:
                settle(r, 1 if name == "rep" else 2)
                turn(r)

        def inward(*indices):
            for index in indices:
                ch = chunk(index)
                if not isinstance(index, int) or index >= early:
                    own_inward(ch)
                hop_got(0, ch).wait_recv()
                hop(edge, ch, True, 2).start()

        def fill(*indices):
            for index in indices:
                hop(rep, chunk(index), False, 0).start()

        def outer(ch):
            if isinstance(ch.index, int):
                if ch.index + FILL < count:
                    fill(ch.index + FILL)
            else:
                pl.when(ch.index + FILL < full)(lambda: fill(ch.index + FILL))
                if full < count:
                    pl.when(ch.index + FILL == full)(lambda: fill(full))
            follow(ch.index + AHEAD)
            if not isinstance(ch.index, int):
                pl.when(among_extra(ch.index))(lambda: send_extra(ch))

        def send_extra(ch):
            crossed(rep, ch).wait_recv()
            hop_extra(ch).start()

        def follow(index):
            if isinstance(index, int):
                if index < count:
                    inward(index)
                return
            pl.when(index < full)(lambda: inward(index))
            if full < count:
                pl.when(index == full)(lambda: inward(full))

        def pull(slot, r):
            def event(ch):
                hop_got(slot, ch).wait_recv()
                hop(r, ch, False, slot).start()
                cross(r, ch).start()
            return event

        pulls = [pull(1, far), pull(2, far_edge)]

        def early_events(*indices):
            for index in indices:
                if index >= early:
                    fill(index + FILL)
                for event in pulls:
                    event(chunk(index))

        perform(
            [
                ("own",), ("take", "far", "own"), ("fill", early), ("take", "edge", "own"),
                ("take", "edge", "other"), ("inward", *range(early)), ("take", "far", "other"),
                ("fill", early + 1), ("land", "rep", "other"), ("take", "last", "own"),
                ("fill", early + 2), ("land", "far", "own", False),
                ("inward", *range(early, LAG)), ("take", "last", "other"), ("land", "edge", "own", False),
                ("early", 0, 1), ("inward", *range(LAG, LAG + 2)), ("land", "edge", "other"),
                ("land", "far", "other"), ("early", 2), ("inward", LAG + 2), ("land", "last", "own", False),
                ("early", 3), ("inward", LAG + 3), ("land", "last", "other"),
            ],
            {"own": take_own, "take": take, "land": land, "inward": inward, "early": early_events, "fill": fill},
        )

        def arrived(ch):
            hop_other(ch).wait_recv()
            when_extra(ch, lambda: None, lambda: crossed(rep, ch).wait_recv())
            crossed(far, ch).wait_recv()

        clear()

        def ended():
            send_extra(chunk(count - 1))

        sweep([outer, *pulls], arrived, lambda: None, ended, LAG, True)

        mine = fsdp * n_tp + tp
        peers = [(a, k) for a in range(2) for k in range(n_tp) if a or k]

        def exchange(at):
            a, k = peers[at]
            to_side = other if a else fsdp
            to_tp = lax.rem(tp + k, n_tp)
            spot = sums.at[mine]
            return remote(spot, spot, sq_send, sq_recv, {"fsdp": to_side, "tp": to_tp})

        for at in range(len(peers)):
            exchange(at).start()
        with jax.named_scope("exchange"):
            seven = sums.at[pl.ds(0, len(peers))]
            remote(seven, seven, sq_send, sq_recv, {"fsdp": other}).wait_recv()
        square_total = jnp.sum(jnp.sum(sums[...], axis=0), keepdims=True)
        factor = 1.0 / jnp.sqrt(square_total / entry_count + 1e-06)
        total_out[...] = jnp.broadcast_to(factor, total_out.shape)
        remote(seven, seven, sq_send, sq_recv, {"fsdp": other}).wait_send()

    def tell():
        return remote(total_out, total_out, fa_send, fa_recv, {"rep": jnp.where(is_edge, near, edge)})

    on_middle(lambda: tell().start())
    with jax.named_scope("told"):
        on_edge(lambda: tell().wait_recv())
    factor_ref[...] = total_out[...]

    @on_middle
    def _():
        tell().wait_send()
        shares_sent()
        grads_sent(4, gz_in)
        grads_sent(6, gz_out)
        all_sent(2, columns, z_in)
        all_sent(3, columns, z_out)
        all_sent(3, columns, x_send)
        all_sent(1, extra_columns, ze_send)


def by_kernel(n_rep, n_tp, entry_count, gate_pre, up_pre, out_grad):
    rows, columns = gate_pre.shape
    tokens = rows * n_rep * 2
    half = out_grad.shape[1] // 2
    quarter = half // n_tp
    count = chunking(columns)[1]
    dma = pltpu.SemaphoreType.DMA
    block, whole = dma((n_rep, 2)), dma((n_rep,))
    return pl.pallas_call(
        functools.partial(gather_multiply, entry_count),
        out_shape=(
            pltpu.VMEM((half, columns), jnp.bfloat16),
            pltpu.VMEM((8, LANES), jnp.float32),
        ),
        in_specs=[pl.BlockSpec(memory_space=pl.ANY)] * 3,
        out_specs=(pl.BlockSpec(memory_space=pltpu.VMEM), pl.BlockSpec(memory_space=pltpu.VMEM)),
        scratch_shapes=[
            pltpu.VMEM((tokens, columns), jnp.bfloat16),
            pltpu.VMEM((tokens, half), jnp.bfloat16),
            pltpu.VMEM((half, tokens), jnp.bfloat16),
            pltpu.VMEM((rows, columns), jnp.bfloat16),
            pltpu.VMEM((rows, columns), jnp.bfloat16),
            pltpu.VMEM((rows, quarter), jnp.bfloat16),
            pltpu.VMEM((2 * n_tp, 8, LANES), jnp.float32),
            pltpu.VMEM((8, LANES), jnp.float32),
            pltpu.VMEM((half, 2 * WIDTH), jnp.float32),
            pltpu.VMEM((half, 2 * WIDTH), jnp.float32),
            dma((4,)), dma, dma, block, dma, dma, dma, block,
            dma, whole, dma, whole,
            dma((3, count)), dma, dma, dma, dma, dma, dma, dma((n_rep, count)),
            dma, dma, dma, dma,
        ],
        compiler_params=pltpu.CompilerParams(
            collective_id=0, has_side_effects=True, vmem_limit_bytes=VMEM_LIMIT * 3 // 4
        ),
    )(gate_pre, up_pre, out_grad)


def scale(summed, factors):
    half, columns = summed.shape
    rows = 128

    def body(summed_ref, factor_ref, out_ref, ready, sems):
        steps = half // rows
        depth = ready.shape[0]

        def leave(m):
            slot = lax.rem(m, depth)
            spot = pl.ds(pl.multiple_of(m * rows, rows), rows)
            return pltpu.make_async_copy(ready.at[slot], out_ref.at[spot, :], sems.at[slot])

        @pl.loop(0, steps)
        def _(m):
            slot = lax.rem(m, depth)
            spot = pl.ds(pl.multiple_of(m * rows, rows), rows)

            @pl.when(m >= depth)
            def _():
                leave(m - depth).wait()
            for at in range(0, columns, LANES):
                cols = pl.ds(at, LANES)
                scaled = summed_ref[spot, cols].astype(jnp.float32) * factor_ref[0:1, :]
                ready[slot, :, cols] = scaled.astype(ready.dtype)
            leave(m).start()

        @pl.loop(max(steps - depth, 0), steps)
        def _(m):
            leave(m).wait()

    return pl.pallas_call(
        body,
        out_shape=jax.ShapeDtypeStruct((half, columns), jnp.bfloat16),
        in_specs=[pl.BlockSpec(memory_space=pltpu.VMEM)] * 2,
        out_specs=pl.BlockSpec(memory_space=pl.ANY),
        scratch_shapes=[pltpu.VMEM((4, rows, columns), jnp.bfloat16), pltpu.SemaphoreType.DMA((4,))],
        compiler_params=pltpu.CompilerParams(vmem_limit_bytes=16 * 1024 * 1024),
    )(summed, factors)


def by_xla(gate_pre, up_pre, out_grad):
    hidden = (jax.nn.silu(gate_pre.astype(jnp.float32)) * up_pre.astype(jnp.float32)).astype(
        jnp.bfloat16
    )
    spread = lax.all_to_all(out_grad, "fsdp", split_axis=1, concat_axis=0, tiled=True)
    grad_rows = lax.all_gather(spread, "rep", axis=0, tiled=True)
    hidden_rows = lax.all_gather(hidden, ("rep", "fsdp"), axis=0, tiled=True)
    summed = lax.dot_general(
        grad_rows, hidden_rows, (((0,), (0,)), ((), ())), preferred_element_type=jnp.float32
    )
    return summed, jnp.sum(summed * summed)


def kernel_fits(n_rep, n_fsdp, n_tp, rows, columns, features):
    tokens, half = rows * n_rep * n_fsdp, features // n_fsdp
    held_bytes = 2 * (tokens * columns + 2 * tokens * half + half * columns + 2 * rows * columns)
    held_bytes += 16 * half * WIDTH
    aligned = rows % 128 == 0 and columns % LANES == 0 and half % (LANES * n_tp) == 0
    shaped = (n_rep, n_fsdp, n_tp) == (4, 2, 4) and columns >= max(12 * WIDTH, 7 * half // n_tp)
    return shaped and aligned and half % TILE == 0 and held_bytes < VMEM_LIMIT * 3 // 4


def solution(mesh):
    n_rep, n_fsdp, n_tp = (mesh.shape[axis] for axis in ("rep", "fsdp", "tp"))

    def on_device(gate_pre, up_pre, out_grad):
        half, columns = out_grad.shape[1] // n_fsdp, gate_pre.shape[1]
        entry_count = half * n_fsdp * columns * n_tp
        if kernel_fits(n_rep, n_fsdp, n_tp, *gate_pre.shape, out_grad.shape[1]):
            summed, factors = by_kernel(n_rep, n_tp, entry_count, gate_pre, up_pre, out_grad)
            return scale(summed, factors)
        summed, square_sum = by_xla(gate_pre, up_pre, out_grad)
        square_total = lax.psum(square_sum, ("fsdp", "tp"))
        factor = 1.0 / jnp.sqrt(square_total / entry_count + 1e-06)
        return (summed * factor).astype(jnp.bfloat16)

    return jax.shard_map(
        on_device,
        mesh=mesh,
        in_specs=(P(("rep", "fsdp"), "tp"), P(("rep", "fsdp"), "tp"), P(("rep", "fsdp"), None)),
        out_specs=P("fsdp", "tp"),
        check_vma=False,
    )
```

```python
import functools

import jax
import jax.numpy as jnp
from jax import lax
from jax.experimental import pallas as pl
from jax.experimental.pallas import tpu as pltpu
from jax.sharding import PartitionSpec as P

MESH = pl.DeviceIdType.MESH
LANES = 128
VMEM_LIMIT = 60 * 1024 * 1024
WIDTH = 256
TILE = 1024
LAG = 4
EDGE_LAG = 2
AHEAD = 4
FILL = 3
EXTRA = (8,)


class Chunk:
    def __init__(self, index, start, size):
        self.index, self.start, self.size = index, start, size

    @property
    def cols(self):
        start = self.start
        return pl.ds(start if isinstance(start, int) else pl.multiple_of(start, LANES), self.size)


def chunking(columns):
    full, rest = columns // WIDTH, columns % WIDTH

    def chunk(index):
        if isinstance(index, int) and index == full:
            return Chunk(index, full * WIDTH, rest)
        return Chunk(index, index * WIDTH, WIDTH)

    return full, full + (1 if rest else 0), chunk


def gather_multiply(
    entry_count, gate_ref, up_ref, grad_ref, out_ref, factor_ref,
    held, grads, turned, gate_in, up_in, across_in, sums, total_out,
    middle_part, end_part,
    local_sem, gx_send, gx_recv, gz_recv, gz_out, gz_in, gy_send, gy_recv,
    gs_send, gs_recv, gf_send, gf_recv,
    z_recv, z_out, z_in, zo_send, ze_send, x_send, xn_send, x_recv,
    sq_send, sq_recv, fa_send, fa_recv,
):
    rep = lax.axis_index("rep")
    fsdp = lax.axis_index("fsdp")
    tp = lax.axis_index("tp")
    rows, columns = gate_ref.shape
    half = grads.shape[1]
    n_tp = 4
    quarter = half // n_tp
    full, count, chunk = chunking(columns)
    extras = (*EXTRA, count - 1)
    extra_columns = len(EXTRA) * WIDTH + chunk(count - 1).size
    other = 1 - fsdp
    side = rep // 2
    edge, near, far, far_edge = 3 * side, 1 + side, 2 - side, 3 - 3 * side
    is_edge = rep == edge
    inner = jnp.where(is_edge, near, far)
    sibling = tp + 1 - 2 * lax.rem(tp, 2)
    opposite = lax.rem(tp + 2, n_tp)
    past = lax.rem(sibling + 2, n_tp)

    def rows_of(r, s):
        return pl.ds(pl.multiple_of((r * 2 + s) * rows, rows), rows)

    def quarter_of(t):
        return pl.ds(pl.multiple_of(t * quarter, LANES), quarter)

    def remote(src, dst, send, recv, device):
        return pltpu.make_async_remote_copy(
            src_ref=src, dst_ref=dst, send_sem=send, recv_sem=recv,
            device_id=device, device_id_type=MESH,
        )

    loads = [
        pltpu.make_async_copy(gate_ref, gate_in, local_sem.at[0]),
        pltpu.make_async_copy(up_ref, up_in, local_sem.at[1]),
        pltpu.make_async_copy(
            grad_ref.at[:, pl.ds(pl.multiple_of(fsdp * half, LANES), half)],
            grads.at[rows_of(rep, fsdp), :], local_sem.at[2],
        ),
        pltpu.make_async_copy(
            grad_ref.at[:, pl.ds(pl.multiple_of(other * half + tp * quarter, LANES), quarter)],
            across_in, local_sem.at[3],
        ),
    ]
    for load in loads:
        load.start()

    barrier = pltpu.get_barrier_semaphore()
    for peer in ({"fsdp": other}, {"tp": sibling}, {"tp": opposite}):
        pl.semaphore_signal(barrier, inc=1, device_id=peer, device_id_type=MESH)
    pl.semaphore_signal(barrier, inc=1, device_id={"rep": inner}, device_id_type=MESH)

    @pl.when(jnp.logical_not(is_edge))
    def _():
        pl.semaphore_signal(barrier, inc=1, device_id={"rep": edge}, device_id_type=MESH)

    with jax.named_scope("load"):
        for load in loads:
            load.wait()

    @pl.loop(0, columns // LANES)
    def _(at):
        cols = pl.ds(pl.multiple_of(at * LANES, LANES), LANES)
        gate = gate_in[:, cols].astype(jnp.float32)
        held[rows_of(rep, fsdp), cols] = (
            jax.nn.silu(gate) * up_in[:, cols].astype(jnp.float32)
        ).astype(held.dtype)

    with jax.named_scope("barrier"):
        pl.semaphore_wait(barrier, 4 + jnp.where(is_edge, 0, 1))

    def grad_across():
        return remote(across_in, grads.at[rows_of(rep, fsdp), quarter_of(tp)], gx_send, gx_recv, {"fsdp": other})

    def grad_spot(r, s, t):
        return grads.at[rows_of(r, s), quarter_of(t)]

    def grad_hop(r, s, inward):
        spot = grad_spot(r, s, tp)
        to = inner if inward else edge
        return remote(spot, spot, (gz_in if inward else gz_out), gz_recv.at[r, s], {"rep": to})

    def grad_got(r, s):
        spot = grad_spot(r, s, tp)
        return remote(spot, spot, gz_in, gz_recv.at[r, s], {"rep": inner})

    def over_y(r, s, t):
        spot = grad_spot(r, s, t)
        return remote(spot, spot, gy_send, gy_recv.at[r, s], {"tp": opposite})

    def to_sibling(r, s, t):
        spot = grad_spot(r, s, t)
        return remote(spot, spot, gs_send, gs_recv.at[r], {"tp": sibling})

    def pass_sibling(r, s, t):
        spot = grad_spot(r, s, t)
        return remote(spot, spot, gf_send, gf_recv.at[r], {"tp": sibling})

    def hop(r, ch, inward, slot):
        spot = held.at[rows_of(r, fsdp), ch.cols]
        to = inner if inward else edge
        return remote(spot, spot, z_in if inward else z_out, z_recv.at[slot, ch.index], {"rep": to})

    def hop_got(slot, ch):
        spot = held.at[pl.ds(0, rows), ch.cols]
        return remote(spot, spot, z_in, z_recv.at[slot, ch.index], {"rep": inner})

    def hop_other(ch):
        spot = held.at[rows_of(edge, other), ch.cols]
        return remote(spot, spot, zo_send, x_recv.at[edge, ch.index], {"rep": inner})

    def cross(r, ch, send=None):
        spot = held.at[rows_of(r, fsdp), ch.cols]
        return remote(spot, spot, x_send if send is None else send, x_recv.at[r, ch.index], {"fsdp": other})

    def crossed(r, ch):
        spot = held.at[rows_of(r, other), ch.cols]
        return remote(spot, spot, x_send, x_recv.at[r, ch.index], {"fsdp": other})

    def hop_extra(ch):
        spot = held.at[rows_of(near, other), ch.cols]
        return remote(spot, spot, ze_send, x_recv.at[near, ch.index], {"rep": jnp.where(is_edge, near, edge)})

    def all_sent(blocks, width, send):
        spot = held.at[pl.ds(0, blocks * rows), pl.ds(0, width)]
        remote(spot, spot, send, gx_recv, {"fsdp": other}).wait_send()

    def among_extra(index):
        return functools.reduce(jnp.logical_or, [index == at for at in EXTRA])

    def when_extra(ch, act, otherwise):
        if isinstance(ch.index, int):
            act() if ch.index in extras else otherwise()
            return
        pl.when(among_extra(ch.index))(act)
        pl.when(jnp.logical_not(among_extra(ch.index)))(otherwise)

    def on_edge(act):
        pl.when(is_edge)(act)

    def on_middle(act):
        pl.when(jnp.logical_not(is_edge))(act)

    def chunks_from(low, high, act):
        if low < min(high, full):
            @pl.loop(low, min(high, full))
            def _(index):
                act(chunk(index))
        if full < count == high:
            act(chunk(full))

    grad_across().start()
    grad_hop(rep, fsdp, True).start()
    on_middle(lambda: grad_hop(rep, fsdp, False).start())

    early = 2

    def own_inward(ch):
        hop(rep, ch, True, jnp.where(is_edge, 0, 1)).start()

    chunks_from(0, early, own_inward)
    on_middle(lambda: chunks_from(0, early, lambda ch: hop(rep, ch, False, 0).start()))

    def own_across(low, high):
        for index in range(low, min(high, count)):
            cross(rep, chunk(index)).start()

    own_across(0, 4)

    def share(r, s):
        over_y(r, s, tp).start()
        to_sibling(r, s, tp).start()

    def pass_on(r, s):
        over_y(r, s, opposite).wait_recv()
        pass_sibling(r, s, opposite).start()

    def settle(r, pairs):
        spots = grads.at[pl.ds(0, pairs * rows), pl.ds(0, quarter)]
        remote(spots, spots, gs_send, gs_recv.at[r], {"tp": sibling}).wait_recv()
        remote(spots, spots, gf_send, gf_recv.at[r], {"tp": sibling}).wait_recv()

    tile = 256

    def turn(r):
        spot = pl.ds(pl.multiple_of(r * 2 * rows, 2 * rows), 2 * rows)

        @pl.loop(0, half // tile)
        def _(m):
            part = pl.ds(pl.multiple_of(m * tile, tile), tile)
            turned[part, spot] = grads[spot, part].T

    def take_own():
        grad_across().wait_recv()
        grad_hop(rep, other, True).start()
        on_middle(lambda: grad_hop(rep, other, False).start())
        share(rep, other)

    def perform(plan, acts):
        for at, (name, *args) in enumerate(plan):
            with jax.named_scope(f"{name}{at}"):
                acts[name](*args)

    def grads_sent(blocks, send):
        all_sent(1, blocks * quarter, send)

    def shares_sent():
        grad_across().wait_send()
        for send in (gy_send, gs_send, gf_send):
            grads_sent(7, send)

    def clear():
        sums[fsdp * n_tp + tp] = jnp.zeros(sums.shape[1:], sums.dtype)

    def leave(product, spot, ch, squared):
        out_ref[spot, ch.cols] = product.astype(out_ref.dtype)
        if squared:
            squares = jnp.sum((product * product).reshape(TILE // 8, 8, ch.size), axis=0)
            total = squares[:, :LANES]
            for at in range(LANES, ch.size, LANES):
                total = total + squares[:, at:at + LANES]
            sums[fsdp * n_tp + tp] += total

    def tile_of(m):
        return pl.ds(pl.multiple_of(m * TILE, TILE), TILE)

    def multiply_tile(ch, m, squared):
        spot = tile_of(m)
        product = jnp.dot(turned[spot, :], held[:, ch.cols], preferred_element_type=jnp.float32)
        leave(product, spot, ch, squared)

    pair = 2 * rows
    ends = {"first": pl.multiple_of(edge * pair, pair), "late": pl.multiple_of(far_edge * pair, pair)}

    def part(spot, ch, start, size):
        tokens = pl.ds(start, size)
        return jnp.dot(turned[spot, tokens], held[tokens, ch.cols], preferred_element_type=jnp.float32)

    def kept(ch):
        return pl.ds((ch.index - (count - 2)) * WIDTH, ch.size)

    def begin(ch):
        @pl.loop(0, tiles)
        def _(m):
            spot = tile_of(m)
            middle_part[spot, kept(ch)] = part(spot, ch, pair, 2 * pair)

    def begin_end(ch):
        @pl.loop(0, tiles)
        def _(m):
            spot = tile_of(m)
            end_part[spot, kept(ch)] = part(spot, ch, ends["first"], pair)

    def complete(ch, squared):
        @pl.loop(0, tiles)
        def _(m):
            spot = tile_of(m)
            both = end_part[spot, kept(ch)] + part(spot, ch, ends["late"], pair)
            leave(middle_part[spot, kept(ch)] + both, spot, ch, squared)

    tiles = half // TILE

    def finish(ch, arrived, squared):
        with jax.named_scope("arrived_last"):
            arrived(ch)
        with jax.named_scope("multiply_last"):
            pl.loop(0, tiles)(lambda m: multiply_tile(ch, m, squared))

    def sweep(events, arrived_but_last, between, ended, lag, squared):
        def arrived(ch):
            arrived_but_last(ch)
            crossed(far_edge, ch).wait_recv()

        places = [at * tiles // len(events) for at in range(len(events))]

        def step(index):
            ch, lagging = chunk(index), chunk(index - lag)
            plan = [(place, event, ch) for place, event in zip(places, events)]
            plan.insert(sum(place == 0 for place in places), (0, arrived, lagging))

            @pl.loop(0, tiles)
            def _(m):
                for at, (place, event, subject) in enumerate(plan):
                    def run():
                        with jax.named_scope(f"event{at}"):
                            event(subject)
                    pl.when(m == place)(run)
                with jax.named_scope("multiply"):
                    multiply_tile(lagging, m, squared)

        pl.loop(LAG, count - 2)(step)
        between()
        ahead, far_pull, last_pull = events
        last_two = chunk(count - 2), chunk(count - 1)
        for index, pull in ((count - 2, far_pull), (count - 1, last_pull)):
            with jax.named_scope("pull_last"):
                ahead(chunk(index))
                for ch in last_two:
                    pull(ch)
            finish(chunk(index - lag), arrived, squared)
        ended()
        chunks_from(count - lag, count - 2, lambda ch: finish(ch, arrived, squared))
        for ch in last_two:
            with jax.named_scope("begin"):
                arrived_but_last(ch)
                begin(ch)
                if squared:
                    begin_end(ch)
        for ch in last_two:
            with jax.named_scope("late"):
                crossed(far_edge, ch).wait_recv()
                complete(ch, squared)

    @on_edge
    def _():
        places = {"near": near, "far": far, "last": far_edge}
        sides = {"own": fsdp, "other": other}

        def take(name, s):
            grad_got(places[name], sides[s]).wait_recv()
            share(places[name], sides[s])

        def land(name, s, whole):
            r = rep if name == "rep" else places[name]
            pass_on(r, sides[s])
            if whole:
                settle(r, 1 if name == "rep" else 2)
                turn(r)

        def relay(*indices):
            for index in indices:
                if index + early < count:
                    own_inward(chunk(index + early))
                if index < count:
                    crossed(edge, chunk(index)).wait_recv()
                    hop_other(chunk(index)).start()

        def pull(slot, r):
            def event(ch):
                hop_got(slot, ch).wait_recv()
                cross(r, ch).start()
            return event

        def pull_near(ch):
            hop_got(0, ch).wait_recv()
            when_extra(ch, lambda: None, lambda: cross(near, ch, xn_send).start())

        pulls = [pull(1, far), pull(2, far_edge)]

        def near_at(*indices):
            for index in indices:
                pull_near(chunk(index))

        def near_ahead(ch):
            index = ch.index + FILL
            if isinstance(index, int):
                if index < count:
                    near_at(index)
                return
            pl.when(index < full)(lambda: near_at(index))
            if full < count:
                pl.when(index == full)(lambda: near_at(full))

        def early_events(*indices):
            for index in indices:
                if index >= early:
                    near_at(index + FILL)
                for event in pulls:
                    event(chunk(index))

        def arrived(ch):
            crossed(near, ch).wait_recv()
            crossed(far, ch).wait_recv()

        def compute(index):
            def whole(ch):
                arrived(ch)
                crossed(far_edge, ch).wait_recv()
            finish(chunk(index), whole, False)

        def batch(k):
            return range(k * count // 8, (k + 1) * count // 8)

        perform(
            [
                ("own",), ("across", 4, 9), ("take", "near", "own"), ("relay", *batch(0)),
                ("near", *range(early)), ("take", "near", "other"), ("across", 9, 12),
                ("land", "rep", "other", True), ("relay", *batch(1)),
                ("take", "far", "own"), ("across", 12, count), ("near", early), ("land", "near", "own", False),
                ("relay", *batch(2)), ("take", "far", "other"), ("near", early + 1),
                ("land", "near", "other", True), ("relay", *batch(3)), ("take", "last", "own"),
                ("near", early + 2), ("land", "far", "own", False), ("relay", *batch(4)),
                ("take", "last", "other"), ("land", "far", "other", True), ("relay", *batch(5)),
                ("early", 0), ("relay", *batch(6)), ("early", 1), ("land", "last", "own", False),
                ("relay", *batch(7)), ("early", 2), ("land", "last", "other", True),
                ("compute", 0), ("early", 3), ("compute", 1),
            ],
            {"own": take_own, "take": take, "land": land, "relay": relay, "early": early_events, "near": near_at,
             "compute": compute, "across": own_across},
        )

        def between():
            shares_sent()
            grads_sent(2, gz_in)
            all_sent(1, columns, z_in)
            all_sent(1, columns, zo_send)
            for index in (count - 2, count - 1):
                begin_end(chunk(index))

        sweep([near_ahead, *pulls], arrived, between, lambda: None, EDGE_LAG, False)
        all_sent(1, columns - extra_columns, xn_send)
        all_sent(3, columns, x_send)

    @on_middle
    def _():
        places = {"edge": edge, "far": far, "last": far_edge}
        sides = {"own": fsdp, "other": other}

        def take(name, s):
            r, s = places[name], sides[s]
            grad_got(r, s).wait_recv()
            grad_hop(r, s, name == "edge").start()
            share(r, s)

        def land(name, s, whole=True):
            r = rep if name == "rep" else places[name]
            pass_on(r, sides[s])
            if whole:
                settle(r, 1 if name == "rep" else 2)
                turn(r)

        def inward(*indices):
            for index in indices:
                ch = chunk(index)
                if not isinstance(index, int) or index >= early:
                    own_inward(ch)
                hop_got(0, ch).wait_recv()
                hop(edge, ch, True, 2).start()

        def fill(*indices):
            for index in indices:
                hop(rep, chunk(index), False, 0).start()

        def outer(ch):
            if isinstance(ch.index, int):
                if ch.index + FILL < count:
                    fill(ch.index + FILL)
            else:
                pl.when(ch.index + FILL < full)(lambda: fill(ch.index + FILL))
                if full < count:
                    pl.when(ch.index + FILL == full)(lambda: fill(full))
            follow(ch.index + AHEAD)
            if not isinstance(ch.index, int):
                pl.when(among_extra(ch.index))(lambda: send_extra(ch))

        def send_extra(ch):
            crossed(rep, ch).wait_recv()
            hop_extra(ch).start()

        def follow(index):
            if isinstance(index, int):
                if index < count:
                    inward(index)
                return
            pl.when(index < full)(lambda: inward(index))
            if full < count:
                pl.when(index == full)(lambda: inward(full))

        def pull(slot, r):
            def event(ch):
                hop_got(slot, ch).wait_recv()
                hop(r, ch, False, slot).start()
                cross(r, ch).start()
            return event

        pulls = [pull(1, far), pull(2, far_edge)]

        def early_events(*indices):
            for index in indices:
                if index >= early:
                    fill(index + FILL)
                for event in pulls:
                    event(chunk(index))

        perform(
            [
                ("own",), ("take", "far", "own"), ("across", 4, 9), ("fill", early),
                ("take", "edge", "own"), ("take", "edge", "other"), ("across", 9, 12),
                ("inward", *range(early)), ("take", "far", "other"),
                ("fill", early + 1), ("land", "rep", "other"), ("take", "last", "own"),
                ("across", 12, count),
                ("fill", early + 2), ("land", "far", "own", False),
                ("inward", *range(early, LAG)), ("take", "last", "other"), ("land", "edge", "own", False),
                ("early", 0, 1), ("inward", *range(LAG, LAG + 2)), ("land", "edge", "other"),
                ("land", "far", "other"), ("early", 2), ("inward", LAG + 2), ("land", "last", "own", False),
                ("early", 3), ("inward", LAG + 3), ("land", "last", "other"),
            ],
            {"own": take_own, "take": take, "land": land, "inward": inward, "early": early_events, "fill": fill,
             "across": own_across},
        )

        def arrived(ch):
            hop_other(ch).wait_recv()
            when_extra(ch, lambda: None, lambda: crossed(rep, ch).wait_recv())
            crossed(far, ch).wait_recv()

        clear()

        def ended():
            send_extra(chunk(count - 1))

        sweep([outer, *pulls], arrived, lambda: None, ended, LAG, True)

        mine = fsdp * n_tp + tp
        peers = [(a, k) for a in range(2) for k in range(n_tp) if a or k]

        def exchange(at):
            a, k = peers[at]
            to_side = other if a else fsdp
            to_tp = lax.rem(tp + k, n_tp)
            spot = sums.at[mine]
            return remote(spot, spot, sq_send, sq_recv, {"fsdp": to_side, "tp": to_tp})

        for at in range(len(peers)):
            exchange(at).start()
        with jax.named_scope("exchange"):
            seven = sums.at[pl.ds(0, len(peers))]
            remote(seven, seven, sq_send, sq_recv, {"fsdp": other}).wait_recv()
        square_total = jnp.sum(jnp.sum(sums[...], axis=0), keepdims=True)
        factor = 1.0 / jnp.sqrt(square_total / entry_count + 1e-06)
        total_out[...] = jnp.broadcast_to(factor, total_out.shape)
        remote(seven, seven, sq_send, sq_recv, {"fsdp": other}).wait_send()

    def tell():
        return remote(total_out, total_out, fa_send, fa_recv, {"rep": jnp.where(is_edge, near, edge)})

    on_middle(lambda: tell().start())
    with jax.named_scope("told"):
        on_edge(lambda: tell().wait_recv())
    factor_ref[...] = total_out[...]

    @on_middle
    def _():
        tell().wait_send()
        shares_sent()
        grads_sent(4, gz_in)
        grads_sent(6, gz_out)
        all_sent(2, columns, z_in)
        all_sent(3, columns, z_out)
        all_sent(3, columns, x_send)
        all_sent(1, extra_columns, ze_send)


def by_kernel(n_rep, n_tp, entry_count, gate_pre, up_pre, out_grad):
    rows, columns = gate_pre.shape
    tokens = rows * n_rep * 2
    half = out_grad.shape[1] // 2
    quarter = half // n_tp
    count = chunking(columns)[1]
    dma = pltpu.SemaphoreType.DMA
    block, whole = dma((n_rep, 2)), dma((n_rep,))
    return pl.pallas_call(
        functools.partial(gather_multiply, entry_count),
        out_shape=(
            pltpu.VMEM((half, columns), jnp.bfloat16),
            pltpu.VMEM((8, LANES), jnp.float32),
        ),
        in_specs=[pl.BlockSpec(memory_space=pl.ANY)] * 3,
        out_specs=(pl.BlockSpec(memory_space=pltpu.VMEM), pl.BlockSpec(memory_space=pltpu.VMEM)),
        scratch_shapes=[
            pltpu.VMEM((tokens, columns), jnp.bfloat16),
            pltpu.VMEM((tokens, half), jnp.bfloat16),
            pltpu.VMEM((half, tokens), jnp.bfloat16),
            pltpu.VMEM((rows, columns), jnp.bfloat16),
            pltpu.VMEM((rows, columns), jnp.bfloat16),
            pltpu.VMEM((rows, quarter), jnp.bfloat16),
            pltpu.VMEM((2 * n_tp, 8, LANES), jnp.float32),
            pltpu.VMEM((8, LANES), jnp.float32),
            pltpu.VMEM((half, 2 * WIDTH), jnp.float32),
            pltpu.VMEM((half, 2 * WIDTH), jnp.float32),
            dma((4,)), dma, dma, block, dma, dma, dma, block,
            dma, whole, dma, whole,
            dma((3, count)), dma, dma, dma, dma, dma, dma, dma((n_rep, count)),
            dma, dma, dma, dma,
        ],
        compiler_params=pltpu.CompilerParams(
            collective_id=0, has_side_effects=True, vmem_limit_bytes=VMEM_LIMIT * 3 // 4
        ),
    )(gate_pre, up_pre, out_grad)


def scale(summed, factors):
    half, columns = summed.shape
    rows = 128

    def body(summed_ref, factor_ref, out_ref, ready, sems):
        steps = half // rows
        depth = ready.shape[0]

        def leave(m):
            slot = lax.rem(m, depth)
            spot = pl.ds(pl.multiple_of(m * rows, rows), rows)
            return pltpu.make_async_copy(ready.at[slot], out_ref.at[spot, :], sems.at[slot])

        @pl.loop(0, steps)
        def _(m):
            slot = lax.rem(m, depth)
            spot = pl.ds(pl.multiple_of(m * rows, rows), rows)

            @pl.when(m >= depth)
            def _():
                leave(m - depth).wait()
            for at in range(0, columns, LANES):
                cols = pl.ds(at, LANES)
                scaled = summed_ref[spot, cols].astype(jnp.float32) * factor_ref[0:1, :]
                ready[slot, :, cols] = scaled.astype(ready.dtype)
            leave(m).start()

        @pl.loop(max(steps - depth, 0), steps)
        def _(m):
            leave(m).wait()

    return pl.pallas_call(
        body,
        out_shape=jax.ShapeDtypeStruct((half, columns), jnp.bfloat16),
        in_specs=[pl.BlockSpec(memory_space=pltpu.VMEM)] * 2,
        out_specs=pl.BlockSpec(memory_space=pl.ANY),
        scratch_shapes=[pltpu.VMEM((4, rows, columns), jnp.bfloat16), pltpu.SemaphoreType.DMA((4,))],
        compiler_params=pltpu.CompilerParams(vmem_limit_bytes=16 * 1024 * 1024),
    )(summed, factors)


def by_xla(gate_pre, up_pre, out_grad):
    hidden = (jax.nn.silu(gate_pre.astype(jnp.float32)) * up_pre.astype(jnp.float32)).astype(
        jnp.bfloat16
    )
    spread = lax.all_to_all(out_grad, "fsdp", split_axis=1, concat_axis=0, tiled=True)
    grad_rows = lax.all_gather(spread, "rep", axis=0, tiled=True)
    hidden_rows = lax.all_gather(hidden, ("rep", "fsdp"), axis=0, tiled=True)
    summed = lax.dot_general(
        grad_rows, hidden_rows, (((0,), (0,)), ((), ())), preferred_element_type=jnp.float32
    )
    return summed, jnp.sum(summed * summed)


def kernel_fits(n_rep, n_fsdp, n_tp, rows, columns, features):
    tokens, half = rows * n_rep * n_fsdp, features // n_fsdp
    held_bytes = 2 * (tokens * columns + 2 * tokens * half + half * columns + 2 * rows * columns)
    held_bytes += 16 * half * WIDTH
    aligned = rows % 128 == 0 and columns % LANES == 0 and half % (LANES * n_tp) == 0
    shaped = (n_rep, n_fsdp, n_tp) == (4, 2, 4) and columns >= max(12 * WIDTH, 7 * half // n_tp)
    return shaped and aligned and half % TILE == 0 and held_bytes < VMEM_LIMIT * 3 // 4


def solution(mesh):
    n_rep, n_fsdp, n_tp = (mesh.shape[axis] for axis in ("rep", "fsdp", "tp"))

    def on_device(gate_pre, up_pre, out_grad):
        half, columns = out_grad.shape[1] // n_fsdp, gate_pre.shape[1]
        entry_count = half * n_fsdp * columns * n_tp
        if kernel_fits(n_rep, n_fsdp, n_tp, *gate_pre.shape, out_grad.shape[1]):
            summed, factors = by_kernel(n_rep, n_tp, entry_count, gate_pre, up_pre, out_grad)
            return scale(summed, factors)
        summed, square_sum = by_xla(gate_pre, up_pre, out_grad)
        square_total = lax.psum(square_sum, ("fsdp", "tp"))
        factor = 1.0 / jnp.sqrt(square_total / entry_count + 1e-06)
        return (summed * factor).astype(jnp.bfloat16)

    return jax.shard_map(
        on_device,
        mesh=mesh,
        in_specs=(P(("rep", "fsdp"), "tp"), P(("rep", "fsdp"), "tp"), P(("rep", "fsdp"), None)),
        out_specs=P("fsdp", "tp"),
        check_vma=False,
    )
```

```python
import functools

import jax
import jax.numpy as jnp
from jax import lax
from jax.experimental import pallas as pl
from jax.experimental.pallas import tpu as pltpu
from jax.sharding import PartitionSpec as P

MESH = pl.DeviceIdType.MESH
LANES = 128
VMEM_LIMIT = 60 * 1024 * 1024
WIDTH = 256
TILE = 1024
LAG = 4
EDGE_LAG = 2
AHEAD = 4
FILL = 3
EXTRA = (5, 9)


class Chunk:
    def __init__(self, index, start, size):
        self.index, self.start, self.size = index, start, size

    @property
    def cols(self):
        start = self.start
        return pl.ds(start if isinstance(start, int) else pl.multiple_of(start, LANES), self.size)


def chunking(columns):
    full, rest = columns // WIDTH, columns % WIDTH

    def chunk(index):
        if isinstance(index, int) and index == full:
            return Chunk(index, full * WIDTH, rest)
        return Chunk(index, index * WIDTH, WIDTH)

    return full, full + (1 if rest else 0), chunk


def gather_multiply(
    entry_count, gate_ref, up_ref, grad_ref, out_ref, factor_ref,
    held, grads, turned, gate_in, up_in, across_in, sums, total_out,
    middle_part, end_part,
    local_sem, gx_send, gx_recv, gz_recv, gz_out, gz_in, gy_send, gy_recv,
    gs_send, gs_recv, gf_send, gf_recv,
    z_recv, z_out, z_in, zo_send, ze_send, x_send, xn_send, x_recv,
    sq_send, sq_recv, fa_send, fa_recv,
):
    rep = lax.axis_index("rep")
    fsdp = lax.axis_index("fsdp")
    tp = lax.axis_index("tp")
    rows, columns = gate_ref.shape
    half = grads.shape[1]
    n_tp = 4
    quarter = half // n_tp
    full, count, chunk = chunking(columns)
    extras = (*EXTRA, count - 1)
    extra_columns = len(EXTRA) * WIDTH + chunk(count - 1).size
    other = 1 - fsdp
    side = rep // 2
    edge, near, far, far_edge = 3 * side, 1 + side, 2 - side, 3 - 3 * side
    is_edge = rep == edge
    inner = jnp.where(is_edge, near, far)
    sibling = tp + 1 - 2 * lax.rem(tp, 2)
    opposite = lax.rem(tp + 2, n_tp)
    past = lax.rem(sibling + 2, n_tp)

    def rows_of(r, s):
        return pl.ds(pl.multiple_of((r * 2 + s) * rows, rows), rows)

    def quarter_of(t):
        return pl.ds(pl.multiple_of(t * quarter, LANES), quarter)

    def remote(src, dst, send, recv, device):
        return pltpu.make_async_remote_copy(
            src_ref=src, dst_ref=dst, send_sem=send, recv_sem=recv,
            device_id=device, device_id_type=MESH,
        )

    loads = [
        pltpu.make_async_copy(
            grad_ref.at[:, pl.ds(pl.multiple_of(other * half + tp * quarter, LANES), quarter)],
            across_in, local_sem.at[0],
        ),
        pltpu.make_async_copy(
            grad_ref.at[:, pl.ds(pl.multiple_of(fsdp * half, LANES), half)],
            grads.at[rows_of(rep, fsdp), :], local_sem.at[1],
        ),
        pltpu.make_async_copy(gate_ref, gate_in, local_sem.at[2]),
        pltpu.make_async_copy(up_ref, up_in, local_sem.at[3]),
    ]
    for load in loads:
        load.start()

    barrier = pltpu.get_barrier_semaphore()
    for peer in ({"fsdp": other}, {"tp": sibling}, {"tp": opposite}):
        pl.semaphore_signal(barrier, inc=1, device_id=peer, device_id_type=MESH)
    pl.semaphore_signal(barrier, inc=1, device_id={"rep": inner}, device_id_type=MESH)

    @pl.when(jnp.logical_not(is_edge))
    def _():
        pl.semaphore_signal(barrier, inc=1, device_id={"rep": edge}, device_id_type=MESH)

    with jax.named_scope("barrier"):
        pl.semaphore_wait(barrier, 4 + jnp.where(is_edge, 0, 1))

    def grad_across():
        return remote(across_in, grads.at[rows_of(rep, fsdp), quarter_of(tp)], gx_send, gx_recv, {"fsdp": other})

    def grad_spot(r, s, t):
        return grads.at[rows_of(r, s), quarter_of(t)]

    def grad_hop(r, s, inward):
        spot = grad_spot(r, s, tp)
        to = inner if inward else edge
        return remote(spot, spot, (gz_in if inward else gz_out), gz_recv.at[r, s], {"rep": to})

    def grad_got(r, s):
        spot = grad_spot(r, s, tp)
        return remote(spot, spot, gz_in, gz_recv.at[r, s], {"rep": inner})

    def over_y(r, s, t):
        spot = grad_spot(r, s, t)
        return remote(spot, spot, gy_send, gy_recv.at[r, s], {"tp": opposite})

    def to_sibling(r, s, t):
        spot = grad_spot(r, s, t)
        return remote(spot, spot, gs_send, gs_recv.at[r], {"tp": sibling})

    def pass_sibling(r, s, t):
        spot = grad_spot(r, s, t)
        return remote(spot, spot, gf_send, gf_recv.at[r], {"tp": sibling})

    def hop(r, ch, inward, slot):
        spot = held.at[rows_of(r, fsdp), ch.cols]
        to = inner if inward else edge
        return remote(spot, spot, z_in if inward else z_out, z_recv.at[slot, ch.index], {"rep": to})

    def hop_got(slot, ch):
        spot = held.at[pl.ds(0, rows), ch.cols]
        return remote(spot, spot, z_in, z_recv.at[slot, ch.index], {"rep": inner})

    def hop_other(ch):
        spot = held.at[rows_of(edge, other), ch.cols]
        return remote(spot, spot, zo_send, x_recv.at[edge, ch.index], {"rep": inner})

    def cross(r, ch, send=None):
        spot = held.at[rows_of(r, fsdp), ch.cols]
        return remote(spot, spot, x_send if send is None else send, x_recv.at[r, ch.index], {"fsdp": other})

    def crossed(r, ch):
        spot = held.at[rows_of(r, other), ch.cols]
        return remote(spot, spot, x_send, x_recv.at[r, ch.index], {"fsdp": other})

    def hop_extra(ch):
        spot = held.at[rows_of(near, other), ch.cols]
        return remote(spot, spot, ze_send, x_recv.at[near, ch.index], {"rep": jnp.where(is_edge, near, edge)})

    def all_sent(blocks, width, send):
        spot = held.at[pl.ds(0, blocks * rows), pl.ds(0, width)]
        remote(spot, spot, send, gx_recv, {"fsdp": other}).wait_send()

    def among_extra(index):
        return functools.reduce(jnp.logical_or, [index == at for at in EXTRA])

    def when_extra(ch, act, otherwise):
        if isinstance(ch.index, int):
            act() if ch.index in extras else otherwise()
            return
        pl.when(among_extra(ch.index))(act)
        pl.when(jnp.logical_not(among_extra(ch.index)))(otherwise)

    def on_edge(act):
        pl.when(is_edge)(act)

    def on_middle(act):
        pl.when(jnp.logical_not(is_edge))(act)

    def chunks_from(low, high, act):
        if low < min(high, full):
            @pl.loop(low, min(high, full))
            def _(index):
                act(chunk(index))
        if full < count == high:
            act(chunk(full))

    loads[0].wait()
    grad_across().start()
    loads[1].wait()
    grad_hop(rep, fsdp, True).start()
    on_middle(lambda: grad_hop(rep, fsdp, False).start())

    with jax.named_scope("load"):
        loads[2].wait()
        loads[3].wait()

    @pl.loop(0, columns // LANES)
    def _(at):
        cols = pl.ds(pl.multiple_of(at * LANES, LANES), LANES)
        gate = gate_in[:, cols].astype(jnp.float32)
        held[rows_of(rep, fsdp), cols] = (
            jax.nn.silu(gate) * up_in[:, cols].astype(jnp.float32)
        ).astype(held.dtype)

    early = 2

    def own_inward(ch):
        hop(rep, ch, True, jnp.where(is_edge, 0, 1)).start()

    chunks_from(0, early, own_inward)
    on_middle(lambda: chunks_from(0, early, lambda ch: hop(rep, ch, False, 0).start()))

    def own_across(low, high):
        for index in range(low, min(high, count)):
            cross(rep, chunk(index)).start()

    own_across(0, 4)

    def share(r, s):
        over_y(r, s, tp).start()
        to_sibling(r, s, tp).start()

    def pass_on(r, s):
        over_y(r, s, opposite).wait_recv()
        pass_sibling(r, s, opposite).start()

    def settle(r, pairs):
        spots = grads.at[pl.ds(0, pairs * rows), pl.ds(0, quarter)]
        remote(spots, spots, gs_send, gs_recv.at[r], {"tp": sibling}).wait_recv()
        remote(spots, spots, gf_send, gf_recv.at[r], {"tp": sibling}).wait_recv()

    tile = 256

    def turn(r):
        spot = pl.ds(pl.multiple_of(r * 2 * rows, 2 * rows), 2 * rows)

        @pl.loop(0, half // tile)
        def _(m):
            part = pl.ds(pl.multiple_of(m * tile, tile), tile)
            turned[part, spot] = grads[spot, part].T

    def take_own():
        grad_across().wait_recv()
        grad_hop(rep, other, True).start()
        on_middle(lambda: grad_hop(rep, other, False).start())
        share(rep, other)

    def perform(plan, acts):
        for at, (name, *args) in enumerate(plan):
            with jax.named_scope(f"{name}{at}"):
                acts[name](*args)

    def grads_sent(blocks, send):
        all_sent(1, blocks * quarter, send)

    def shares_sent():
        grad_across().wait_send()
        for send in (gy_send, gs_send, gf_send):
            grads_sent(7, send)

    def clear():
        sums[fsdp * n_tp + tp] = jnp.zeros(sums.shape[1:], sums.dtype)

    def leave(product, spot, ch, squared):
        out_ref[spot, ch.cols] = product.astype(out_ref.dtype)
        if squared:
            squares = jnp.sum((product * product).reshape(TILE // 8, 8, ch.size), axis=0)
            total = squares[:, :LANES]
            for at in range(LANES, ch.size, LANES):
                total = total + squares[:, at:at + LANES]
            sums[fsdp * n_tp + tp] += total

    def tile_of(m):
        return pl.ds(pl.multiple_of(m * TILE, TILE), TILE)

    def multiply_tile(ch, m, squared):
        spot = tile_of(m)
        product = jnp.dot(turned[spot, :], held[:, ch.cols], preferred_element_type=jnp.float32)
        leave(product, spot, ch, squared)

    pair = 2 * rows
    ends = {"first": pl.multiple_of(edge * pair, pair), "late": pl.multiple_of(far_edge * pair, pair)}

    def part(spot, ch, start, size):
        tokens = pl.ds(start, size)
        return jnp.dot(turned[spot, tokens], held[tokens, ch.cols], preferred_element_type=jnp.float32)

    def kept(ch):
        return pl.ds((ch.index - (count - 2)) * WIDTH, ch.size)

    def begin(ch):
        @pl.loop(0, tiles)
        def _(m):
            spot = tile_of(m)
            middle_part[spot, kept(ch)] = part(spot, ch, pair, 2 * pair)

    def begin_end(ch):
        @pl.loop(0, tiles)
        def _(m):
            spot = tile_of(m)
            end_part[spot, kept(ch)] = part(spot, ch, ends["first"], pair)

    def complete(ch, squared):
        @pl.loop(0, tiles)
        def _(m):
            spot = tile_of(m)
            both = end_part[spot, kept(ch)] + part(spot, ch, ends["late"], pair)
            leave(middle_part[spot, kept(ch)] + both, spot, ch, squared)

    tiles = half // TILE

    def finish(ch, arrived, squared):
        with jax.named_scope("arrived_last"):
            arrived(ch)
        with jax.named_scope("multiply_last"):
            pl.loop(0, tiles)(lambda m: multiply_tile(ch, m, squared))

    def sweep(events, arrived_but_last, between, ended, lag, squared):
        def arrived(ch):
            arrived_but_last(ch)
            crossed(far_edge, ch).wait_recv()

        places = [at * tiles // len(events) for at in range(len(events))]

        def step(index):
            ch, lagging = chunk(index), chunk(index - lag)
            plan = [(place, event, ch) for place, event in zip(places, events)]
            plan.insert(sum(place == 0 for place in places), (0, arrived, lagging))

            @pl.loop(0, tiles)
            def _(m):
                for at, (place, event, subject) in enumerate(plan):
                    def run():
                        with jax.named_scope(f"event{at}"):
                            event(subject)
                    pl.when(m == place)(run)
                with jax.named_scope("multiply"):
                    multiply_tile(lagging, m, squared)

        pl.loop(LAG, count - 2)(step)
        between()
        ahead, far_pull, last_pull = events
        last_two = chunk(count - 2), chunk(count - 1)
        for index, pull in ((count - 2, far_pull), (count - 1, last_pull)):
            with jax.named_scope("pull_last"):
                ahead(chunk(index))
                for ch in last_two:
                    pull(ch)
            finish(chunk(index - lag), arrived, squared)
        ended()
        chunks_from(count - lag, count - 2, lambda ch: finish(ch, arrived, squared))
        for ch in last_two:
            with jax.named_scope("begin"):
                arrived_but_last(ch)
                begin(ch)
                if squared:
                    begin_end(ch)
        for ch in last_two:
            with jax.named_scope("late"):
                crossed(far_edge, ch).wait_recv()
                complete(ch, squared)

    @on_edge
    def _():
        places = {"near": near, "far": far, "last": far_edge}
        sides = {"own": fsdp, "other": other}

        def take(name, s):
            grad_got(places[name], sides[s]).wait_recv()
            share(places[name], sides[s])

        def land(name, s, whole):
            r = rep if name == "rep" else places[name]
            pass_on(r, sides[s])
            if whole:
                settle(r, 1 if name == "rep" else 2)
                turn(r)

        def relay(*indices):
            for index in indices:
                if index + early < count:
                    own_inward(chunk(index + early))
                if index < count:
                    crossed(edge, chunk(index)).wait_recv()
                    hop_other(chunk(index)).start()

        def pull(slot, r):
            def event(ch):
                hop_got(slot, ch).wait_recv()
                cross(r, ch).start()
            return event

        def pull_near(ch):
            hop_got(0, ch).wait_recv()
            when_extra(ch, lambda: None, lambda: cross(near, ch, xn_send).start())

        pulls = [pull(1, far), pull(2, far_edge)]

        def near_at(*indices):
            for index in indices:
                pull_near(chunk(index))

        def near_ahead(ch):
            index = ch.index + FILL
            if isinstance(index, int):
                if index < count:
                    near_at(index)
                return
            pl.when(index < full)(lambda: near_at(index))
            if full < count:
                pl.when(index == full)(lambda: near_at(full))

        def early_events(*indices):
            for index in indices:
                if index >= early:
                    near_at(index + FILL)
                for event in pulls:
                    event(chunk(index))

        def arrived(ch):
            crossed(near, ch).wait_recv()
            crossed(far, ch).wait_recv()

        def compute(index):
            def whole(ch):
                arrived(ch)
                crossed(far_edge, ch).wait_recv()
            finish(chunk(index), whole, False)

        def batch(k):
            return range(k * count // 8, (k + 1) * count // 8)

        perform(
            [
                ("own",), ("across", 4, 9), ("take", "near", "own"), ("relay", *batch(0)),
                ("near", *range(early)), ("take", "near", "other"), ("across", 9, 12),
                ("land", "rep", "other", True), ("relay", *batch(1)),
                ("take", "far", "own"), ("across", 12, count), ("near", early), ("land", "near", "own", False),
                ("relay", *batch(2)), ("take", "far", "other"), ("near", early + 1),
                ("land", "near", "other", True), ("relay", *batch(3)), ("take", "last", "own"),
                ("near", early + 2), ("land", "far", "own", False), ("relay", *batch(4)),
                ("take", "last", "other"), ("land", "far", "other", True), ("relay", *batch(5)),
                ("early", 0), ("relay", *batch(6)), ("early", 1), ("land", "last", "own", False),
                ("relay", *batch(7)), ("early", 2), ("land", "last", "other", True),
                ("compute", 0), ("early", 3), ("compute", 1),
            ],
            {"own": take_own, "take": take, "land": land, "relay": relay, "early": early_events, "near": near_at,
             "compute": compute, "across": own_across},
        )

        def between():
            shares_sent()
            grads_sent(2, gz_in)
            all_sent(1, columns, z_in)
            all_sent(1, columns, zo_send)
            for index in (count - 2, count - 1):
                begin_end(chunk(index))

        sweep([near_ahead, *pulls], arrived, between, lambda: None, EDGE_LAG, False)
        all_sent(1, columns - extra_columns, xn_send)
        all_sent(3, columns, x_send)

    @on_middle
    def _():
        places = {"edge": edge, "far": far, "last": far_edge}
        sides = {"own": fsdp, "other": other}

        def take(name, s):
            r, s = places[name], sides[s]
            grad_got(r, s).wait_recv()
            grad_hop(r, s, name == "edge").start()
            share(r, s)

        def land(name, s, whole=True):
            r = rep if name == "rep" else places[name]
            pass_on(r, sides[s])
            if whole:
                settle(r, 1 if name == "rep" else 2)
                turn(r)

        def inward(*indices):
            for index in indices:
                ch = chunk(index)
                if not isinstance(index, int) or index >= early:
                    own_inward(ch)
                hop_got(0, ch).wait_recv()
                hop(edge, ch, True, 2).start()

        def fill(*indices):
            for index in indices:
                hop(rep, chunk(index), False, 0).start()

        def outer(ch):
            if isinstance(ch.index, int):
                if ch.index + FILL < count:
                    fill(ch.index + FILL)
            else:
                pl.when(ch.index + FILL < full)(lambda: fill(ch.index + FILL))
                if full < count:
                    pl.when(ch.index + FILL == full)(lambda: fill(full))
            follow(ch.index + AHEAD)
            if not isinstance(ch.index, int):
                pl.when(among_extra(ch.index))(lambda: send_extra(ch))

        def send_extra(ch):
            crossed(rep, ch).wait_recv()
            hop_extra(ch).start()

        def follow(index):
            if isinstance(index, int):
                if index < count:
                    inward(index)
                return
            pl.when(index < full)(lambda: inward(index))
            if full < count:
                pl.when(index == full)(lambda: inward(full))

        def pull(slot, r):
            def event(ch):
                hop_got(slot, ch).wait_recv()
                hop(r, ch, False, slot).start()
                cross(r, ch).start()
            return event

        pulls = [pull(1, far), pull(2, far_edge)]

        def early_events(*indices):
            for index in indices:
                if index >= early:
                    fill(index + FILL)
                for event in pulls:
                    event(chunk(index))

        perform(
            [
                ("own",), ("take", "far", "own"), ("across", 4, 9), ("fill", early),
                ("take", "edge", "own"), ("take", "edge", "other"), ("across", 9, 12),
                ("inward", *range(early)), ("take", "far", "other"),
                ("fill", early + 1), ("land", "rep", "other"), ("take", "last", "own"),
                ("across", 12, count),
                ("fill", early + 2), ("land", "far", "own", False),
                ("inward", *range(early, LAG)), ("take", "last", "other"), ("land", "edge", "own", False),
                ("early", 0, 1), ("inward", *range(LAG, LAG + 2)), ("land", "edge", "other"),
                ("land", "far", "other"), ("early", 2), ("inward", LAG + 2), ("land", "last", "own", False),
                ("early", 3), ("inward", LAG + 3), ("land", "last", "other"),
            ],
            {"own": take_own, "take": take, "land": land, "inward": inward, "early": early_events, "fill": fill,
             "across": own_across},
        )

        def arrived(ch):
            hop_other(ch).wait_recv()
            when_extra(ch, lambda: None, lambda: crossed(rep, ch).wait_recv())
            crossed(far, ch).wait_recv()

        clear()

        def ended():
            send_extra(chunk(count - 1))

        sweep([outer, *pulls], arrived, lambda: None, ended, LAG, True)

        mine = fsdp * n_tp + tp
        peers = [(a, k) for a in range(2) for k in range(n_tp) if a or k]

        def exchange(at):
            a, k = peers[at]
            to_side = other if a else fsdp
            to_tp = lax.rem(tp + k, n_tp)
            spot = sums.at[mine]
            return remote(spot, spot, sq_send, sq_recv, {"fsdp": to_side, "tp": to_tp})

        for at in range(len(peers)):
            exchange(at).start()
        with jax.named_scope("exchange"):
            seven = sums.at[pl.ds(0, len(peers))]
            remote(seven, seven, sq_send, sq_recv, {"fsdp": other}).wait_recv()
        square_total = jnp.sum(jnp.sum(sums[...], axis=0), keepdims=True)
        factor = 1.0 / jnp.sqrt(square_total / entry_count + 1e-06)
        total_out[...] = jnp.broadcast_to(factor, total_out.shape)
        remote(seven, seven, sq_send, sq_recv, {"fsdp": other}).wait_send()

    def tell():
        return remote(total_out, total_out, fa_send, fa_recv, {"rep": jnp.where(is_edge, near, edge)})

    on_middle(lambda: tell().start())
    with jax.named_scope("told"):
        on_edge(lambda: tell().wait_recv())
    factor_ref[...] = total_out[...]

    @on_middle
    def _():
        tell().wait_send()
        shares_sent()
        grads_sent(4, gz_in)
        grads_sent(6, gz_out)
        all_sent(2, columns, z_in)
        all_sent(3, columns, z_out)
        all_sent(3, columns, x_send)
        all_sent(1, extra_columns, ze_send)


def by_kernel(n_rep, n_tp, entry_count, gate_pre, up_pre, out_grad):
    rows, columns = gate_pre.shape
    tokens = rows * n_rep * 2
    half = out_grad.shape[1] // 2
    quarter = half // n_tp
    count = chunking(columns)[1]
    dma = pltpu.SemaphoreType.DMA
    block, whole = dma((n_rep, 2)), dma((n_rep,))
    return pl.pallas_call(
        functools.partial(gather_multiply, entry_count),
        out_shape=(
            pltpu.VMEM((half, columns), jnp.bfloat16),
            pltpu.VMEM((8, LANES), jnp.float32),
        ),
        in_specs=[pl.BlockSpec(memory_space=pl.ANY)] * 3,
        out_specs=(pl.BlockSpec(memory_space=pltpu.VMEM), pl.BlockSpec(memory_space=pltpu.VMEM)),
        scratch_shapes=[
            pltpu.VMEM((tokens, columns), jnp.bfloat16),
            pltpu.VMEM((tokens, half), jnp.bfloat16),
            pltpu.VMEM((half, tokens), jnp.bfloat16),
            pltpu.VMEM((rows, columns), jnp.bfloat16),
            pltpu.VMEM((rows, columns), jnp.bfloat16),
            pltpu.VMEM((rows, quarter), jnp.bfloat16),
            pltpu.VMEM((2 * n_tp, 8, LANES), jnp.float32),
            pltpu.VMEM((8, LANES), jnp.float32),
            pltpu.VMEM((half, 2 * WIDTH), jnp.float32),
            pltpu.VMEM((half, 2 * WIDTH), jnp.float32),
            dma((4,)), dma, dma, block, dma, dma, dma, block,
            dma, whole, dma, whole,
            dma((3, count)), dma, dma, dma, dma, dma, dma, dma((n_rep, count)),
            dma, dma, dma, dma,
        ],
        compiler_params=pltpu.CompilerParams(
            collective_id=0, has_side_effects=True, vmem_limit_bytes=VMEM_LIMIT * 3 // 4
        ),
    )(gate_pre, up_pre, out_grad)


def scale(summed, factors):
    half, columns = summed.shape
    rows = 128

    def body(summed_ref, factor_ref, out_ref, ready, sems):
        steps = half // rows
        depth = ready.shape[0]

        def leave(m):
            slot = lax.rem(m, depth)
            spot = pl.ds(pl.multiple_of(m * rows, rows), rows)
            return pltpu.make_async_copy(ready.at[slot], out_ref.at[spot, :], sems.at[slot])

        @pl.loop(0, steps)
        def _(m):
            slot = lax.rem(m, depth)
            spot = pl.ds(pl.multiple_of(m * rows, rows), rows)

            @pl.when(m >= depth)
            def _():
                leave(m - depth).wait()
            for at in range(0, columns, LANES):
                cols = pl.ds(at, LANES)
                scaled = summed_ref[spot, cols].astype(jnp.float32) * factor_ref[0:1, :]
                ready[slot, :, cols] = scaled.astype(ready.dtype)
            leave(m).start()

        @pl.loop(max(steps - depth, 0), steps)
        def _(m):
            leave(m).wait()

    return pl.pallas_call(
        body,
        out_shape=jax.ShapeDtypeStruct((half, columns), jnp.bfloat16),
        in_specs=[pl.BlockSpec(memory_space=pltpu.VMEM)] * 2,
        out_specs=pl.BlockSpec(memory_space=pl.ANY),
        scratch_shapes=[pltpu.VMEM((4, rows, columns), jnp.bfloat16), pltpu.SemaphoreType.DMA((4,))],
        compiler_params=pltpu.CompilerParams(vmem_limit_bytes=16 * 1024 * 1024),
    )(summed, factors)


def by_xla(gate_pre, up_pre, out_grad):
    hidden = (jax.nn.silu(gate_pre.astype(jnp.float32)) * up_pre.astype(jnp.float32)).astype(
        jnp.bfloat16
    )
    spread = lax.all_to_all(out_grad, "fsdp", split_axis=1, concat_axis=0, tiled=True)
    grad_rows = lax.all_gather(spread, "rep", axis=0, tiled=True)
    hidden_rows = lax.all_gather(hidden, ("rep", "fsdp"), axis=0, tiled=True)
    summed = lax.dot_general(
        grad_rows, hidden_rows, (((0,), (0,)), ((), ())), preferred_element_type=jnp.float32
    )
    return summed, jnp.sum(summed * summed)


def kernel_fits(n_rep, n_fsdp, n_tp, rows, columns, features):
    tokens, half = rows * n_rep * n_fsdp, features // n_fsdp
    held_bytes = 2 * (tokens * columns + 2 * tokens * half + half * columns + 2 * rows * columns)
    held_bytes += 16 * half * WIDTH
    aligned = rows % 128 == 0 and columns % LANES == 0 and half % (LANES * n_tp) == 0
    shaped = (n_rep, n_fsdp, n_tp) == (4, 2, 4) and columns >= max(12 * WIDTH, 7 * half // n_tp)
    return shaped and aligned and half % TILE == 0 and held_bytes < VMEM_LIMIT * 3 // 4


def solution(mesh):
    n_rep, n_fsdp, n_tp = (mesh.shape[axis] for axis in ("rep", "fsdp", "tp"))

    def on_device(gate_pre, up_pre, out_grad):
        half, columns = out_grad.shape[1] // n_fsdp, gate_pre.shape[1]
        entry_count = half * n_fsdp * columns * n_tp
        if kernel_fits(n_rep, n_fsdp, n_tp, *gate_pre.shape, out_grad.shape[1]):
            summed, factors = by_kernel(n_rep, n_tp, entry_count, gate_pre, up_pre, out_grad)
            return scale(summed, factors)
        summed, square_sum = by_xla(gate_pre, up_pre, out_grad)
        square_total = lax.psum(square_sum, ("fsdp", "tp"))
        factor = 1.0 / jnp.sqrt(square_total / entry_count + 1e-06)
        return (summed * factor).astype(jnp.bfloat16)

    return jax.shard_map(
        on_device,
        mesh=mesh,
        in_specs=(P(("rep", "fsdp"), "tp"), P(("rep", "fsdp"), "tp"), P(("rep", "fsdp"), None)),
        out_specs=P("fsdp", "tp"),
        check_vma=False,
    )
```

```python
import functools

import jax
import jax.numpy as jnp
from jax import lax
from jax.experimental import pallas as pl
from jax.experimental.pallas import tpu as pltpu
from jax.sharding import PartitionSpec as P

MESH = pl.DeviceIdType.MESH
LANES = 128
VMEM_LIMIT = 60 * 1024 * 1024
WIDTH = 256
TILE = 1024
LAG = 4
EDGE_LAG = 2
AHEAD = 4
FILL = 3
EXTRA = (5, 9)


class Chunk:
    def __init__(self, index, start, size):
        self.index, self.start, self.size = index, start, size

    @property
    def cols(self):
        start = self.start
        return pl.ds(start if isinstance(start, int) else pl.multiple_of(start, LANES), self.size)


def chunking(columns):
    full, rest = columns // WIDTH, columns % WIDTH

    def chunk(index):
        if isinstance(index, int) and index == full:
            return Chunk(index, full * WIDTH, rest)
        return Chunk(index, index * WIDTH, WIDTH)

    return full, full + (1 if rest else 0), chunk


def gather_multiply(
    entry_count, gate_ref, up_ref, grad_ref, out_ref, factor_ref,
    held, grads, turned, gate_in, up_in, across_in, sums, total_out,
    middle_part, end_part,
    local_sem, gx_send, gx_recv, gz_recv, gz_out, gz_in, gy_send, gy_recv,
    gs_send, gs_recv, gf_send, gf_recv,
    z_recv, z_out, z_in, zo_send, ze_send, x_send, xn_send, x_recv,
    sq_send, sq_recv, fa_send, fa_recv,
):
    rep = lax.axis_index("rep")
    fsdp = lax.axis_index("fsdp")
    tp = lax.axis_index("tp")
    rows, columns = gate_ref.shape
    half = grads.shape[1]
    n_tp = 4
    quarter = half // n_tp
    full, count, chunk = chunking(columns)
    extras = (*EXTRA, count - 1)
    extra_columns = len(EXTRA) * WIDTH + chunk(count - 1).size
    other = 1 - fsdp
    side = rep // 2
    edge, near, far, far_edge = 3 * side, 1 + side, 2 - side, 3 - 3 * side
    is_edge = rep == edge
    inner = jnp.where(is_edge, near, far)
    sibling = tp + 1 - 2 * lax.rem(tp, 2)
    opposite = lax.rem(tp + 2, n_tp)
    past = lax.rem(sibling + 2, n_tp)

    def rows_of(r, s):
        return pl.ds(pl.multiple_of((r * 2 + s) * rows, rows), rows)

    def quarter_of(t):
        return pl.ds(pl.multiple_of(t * quarter, LANES), quarter)

    def remote(src, dst, send, recv, device):
        return pltpu.make_async_remote_copy(
            src_ref=src, dst_ref=dst, send_sem=send, recv_sem=recv,
            device_id=device, device_id_type=MESH,
        )

    loads = [
        pltpu.make_async_copy(
            grad_ref.at[:, pl.ds(pl.multiple_of(other * half + tp * quarter, LANES), quarter)],
            across_in, local_sem.at[0],
        ),
        pltpu.make_async_copy(
            grad_ref.at[:, pl.ds(pl.multiple_of(fsdp * half, LANES), half)],
            grads.at[rows_of(rep, fsdp), :], local_sem.at[1],
        ),
        pltpu.make_async_copy(gate_ref, gate_in, local_sem.at[2]),
        pltpu.make_async_copy(up_ref, up_in, local_sem.at[3]),
    ]
    for load in loads:
        load.start()

    barrier = pltpu.get_barrier_semaphore()
    for peer in ({"fsdp": other}, {"tp": sibling}, {"tp": opposite}):
        pl.semaphore_signal(barrier, inc=1, device_id=peer, device_id_type=MESH)
    pl.semaphore_signal(barrier, inc=1, device_id={"rep": inner}, device_id_type=MESH)

    @pl.when(jnp.logical_not(is_edge))
    def _():
        pl.semaphore_signal(barrier, inc=1, device_id={"rep": edge}, device_id_type=MESH)

    with jax.named_scope("barrier"):
        pl.semaphore_wait(barrier, 4 + jnp.where(is_edge, 0, 1))

    def grad_across():
        return remote(across_in, grads.at[rows_of(rep, fsdp), quarter_of(tp)], gx_send, gx_recv, {"fsdp": other})

    def grad_spot(r, s, t):
        return grads.at[rows_of(r, s), quarter_of(t)]

    def grad_hop(r, s, inward):
        spot = grad_spot(r, s, tp)
        to = inner if inward else edge
        return remote(spot, spot, (gz_in if inward else gz_out), gz_recv.at[r, s], {"rep": to})

    def grad_got(r, s):
        spot = grad_spot(r, s, tp)
        return remote(spot, spot, gz_in, gz_recv.at[r, s], {"rep": inner})

    def over_y(r, s, t):
        spot = grad_spot(r, s, t)
        return remote(spot, spot, gy_send, gy_recv.at[r, s], {"tp": opposite})

    def to_sibling(r, s, t):
        spot = grad_spot(r, s, t)
        return remote(spot, spot, gs_send, gs_recv.at[r], {"tp": sibling})

    def pass_sibling(r, s, t):
        spot = grad_spot(r, s, t)
        return remote(spot, spot, gf_send, gf_recv.at[r], {"tp": sibling})

    def hop(r, ch, inward, slot):
        spot = held.at[rows_of(r, fsdp), ch.cols]
        to = inner if inward else edge
        return remote(spot, spot, z_in if inward else z_out, z_recv.at[slot, ch.index], {"rep": to})

    def hop_got(slot, ch):
        spot = held.at[pl.ds(0, rows), ch.cols]
        return remote(spot, spot, z_in, z_recv.at[slot, ch.index], {"rep": inner})

    def hop_other(ch):
        spot = held.at[rows_of(edge, other), ch.cols]
        return remote(spot, spot, zo_send, x_recv.at[edge, ch.index], {"rep": inner})

    def cross(r, ch, send=None):
        spot = held.at[rows_of(r, fsdp), ch.cols]
        return remote(spot, spot, x_send if send is None else send, x_recv.at[r, ch.index], {"fsdp": other})

    def crossed(r, ch):
        spot = held.at[rows_of(r, other), ch.cols]
        return remote(spot, spot, x_send, x_recv.at[r, ch.index], {"fsdp": other})

    def hop_extra(ch):
        spot = held.at[rows_of(near, other), ch.cols]
        return remote(spot, spot, ze_send, x_recv.at[near, ch.index], {"rep": jnp.where(is_edge, near, edge)})

    def all_sent(blocks, width, send):
        spot = held.at[pl.ds(0, blocks * rows), pl.ds(0, width)]
        remote(spot, spot, send, gx_recv, {"fsdp": other}).wait_send()

    def among_extra(index):
        return functools.reduce(jnp.logical_or, [index == at for at in EXTRA])

    def when_extra(ch, act, otherwise):
        if isinstance(ch.index, int):
            act() if ch.index in extras else otherwise()
            return
        pl.when(among_extra(ch.index))(act)
        pl.when(jnp.logical_not(among_extra(ch.index)))(otherwise)

    def on_edge(act):
        pl.when(is_edge)(act)

    def on_middle(act):
        pl.when(jnp.logical_not(is_edge))(act)

    def chunks_from(low, high, act):
        if low < min(high, full):
            @pl.loop(low, min(high, full))
            def _(index):
                act(chunk(index))
        if full < count == high:
            act(chunk(full))

    loads[0].wait()
    grad_across().start()
    loads[1].wait()
    grad_hop(rep, fsdp, True).start()
    on_middle(lambda: grad_hop(rep, fsdp, False).start())

    with jax.named_scope("load"):
        loads[2].wait()
        loads[3].wait()

    @pl.loop(0, columns // LANES)
    def _(at):
        cols = pl.ds(pl.multiple_of(at * LANES, LANES), LANES)
        gate = gate_in[:, cols].astype(jnp.float32)
        held[rows_of(rep, fsdp), cols] = (
            jax.nn.silu(gate) * up_in[:, cols].astype(jnp.float32)
        ).astype(held.dtype)

    early = 2

    def own_inward(ch):
        hop(rep, ch, True, jnp.where(is_edge, 0, 1)).start()

    chunks_from(0, early, own_inward)
    on_middle(lambda: chunks_from(0, early, lambda ch: hop(rep, ch, False, 0).start()))

    def own_across(low, high):
        for index in range(low, min(high, count)):
            cross(rep, chunk(index)).start()

    own_across(0, 4)

    def share(r, s):
        over_y(r, s, tp).start()
        to_sibling(r, s, tp).start()

    def pass_on(r, s):
        over_y(r, s, opposite).wait_recv()
        pass_sibling(r, s, opposite).start()

    def settle(r, pairs):
        spots = grads.at[pl.ds(0, pairs * rows), pl.ds(0, quarter)]
        remote(spots, spots, gs_send, gs_recv.at[r], {"tp": sibling}).wait_recv()
        remote(spots, spots, gf_send, gf_recv.at[r], {"tp": sibling}).wait_recv()

    tile = 256

    def turn(r):
        spot = pl.ds(pl.multiple_of(r * 2 * rows, 2 * rows), 2 * rows)

        @pl.loop(0, half // tile)
        def _(m):
            part = pl.ds(pl.multiple_of(m * tile, tile), tile)
            turned[part, spot] = grads[spot, part].T

    def take_own():
        grad_across().wait_recv()
        grad_hop(rep, other, True).start()
        on_middle(lambda: grad_hop(rep, other, False).start())
        share(rep, other)

    def perform(plan, acts):
        for at, (name, *args) in enumerate(plan):
            with jax.named_scope(f"{name}{at}"):
                acts[name](*args)

    def grads_sent(blocks, send):
        all_sent(1, blocks * quarter, send)

    def shares_sent():
        grad_across().wait_send()
        for send in (gy_send, gs_send, gf_send):
            grads_sent(7, send)

    def clear():
        sums[fsdp * n_tp + tp] = jnp.zeros(sums.shape[1:], sums.dtype)

    def leave(product, spot, ch, squared):
        out_ref[spot, ch.cols] = product.astype(out_ref.dtype)
        if squared:
            squares = jnp.sum((product * product).reshape(TILE // 8, 8, ch.size), axis=0)
            total = squares[:, :LANES]
            for at in range(LANES, ch.size, LANES):
                total = total + squares[:, at:at + LANES]
            sums[fsdp * n_tp + tp] += total

    def tile_of(m):
        return pl.ds(pl.multiple_of(m * TILE, TILE), TILE)

    def multiply_tile(ch, m, squared):
        spot = tile_of(m)
        product = jnp.dot(turned[spot, :], held[:, ch.cols], preferred_element_type=jnp.float32)
        leave(product, spot, ch, squared)

    pair = 2 * rows
    ends = {"first": pl.multiple_of(edge * pair, pair), "late": pl.multiple_of(far_edge * pair, pair)}

    def part(spot, ch, start, size):
        tokens = pl.ds(start, size)
        return jnp.dot(turned[spot, tokens], held[tokens, ch.cols], preferred_element_type=jnp.float32)

    def kept(ch):
        return pl.ds((ch.index - (count - 3)) * WIDTH, ch.size)

    def begin(ch):
        @pl.loop(0, tiles)
        def _(m):
            spot = tile_of(m)
            middle_part[spot, kept(ch)] = part(spot, ch, pair, 2 * pair)

    def begin_end(ch):
        @pl.loop(0, tiles)
        def _(m):
            spot = tile_of(m)
            end_part[spot, kept(ch)] = part(spot, ch, ends["first"], pair)

    def complete(ch, squared):
        @pl.loop(0, tiles)
        def _(m):
            spot = tile_of(m)
            both = end_part[spot, kept(ch)] + part(spot, ch, ends["late"], pair)
            leave(middle_part[spot, kept(ch)] + both, spot, ch, squared)

    tiles = half // TILE

    def finish(ch, arrived, squared):
        with jax.named_scope("arrived_last"):
            arrived(ch)
        with jax.named_scope("multiply_last"):
            pl.loop(0, tiles)(lambda m: multiply_tile(ch, m, squared))

    def sweep(events, arrived_but_last, between, ended, lag, squared):
        def arrived(ch):
            arrived_but_last(ch)
            crossed(far_edge, ch).wait_recv()

        places = [at * tiles // len(events) for at in range(len(events))]

        def step(index):
            ch, lagging = chunk(index), chunk(index - lag)
            plan = [(place, event, ch) for place, event in zip(places, events)]
            plan.insert(sum(place == 0 for place in places), (0, arrived, lagging))

            @pl.loop(0, tiles)
            def _(m):
                for at, (place, event, subject) in enumerate(plan):
                    def run():
                        with jax.named_scope(f"event{at}"):
                            event(subject)
                    pl.when(m == place)(run)
                with jax.named_scope("multiply"):
                    multiply_tile(lagging, m, squared)

        last_three = [chunk(index) for index in range(count - 3, count)]
        far_pull, last_pull = events[1:]
        pl.loop(LAG, count - 3)(step)
        between()
        with jax.named_scope("far_last"):
            for ch in last_three:
                far_pull(ch)
        remaining = count - 3 - lag
        chunks_from(remaining, remaining + 1, lambda ch: finish(ch, arrived, squared))
        with jax.named_scope("pull_last"):
            last_pull(last_three[0])
        chunks_from(remaining + 1, count - 3, lambda ch: finish(ch, arrived, squared))
        with jax.named_scope("pull_last"):
            for ch in last_three[1:]:
                last_pull(ch)
        ended()
        for ch in last_three:
            with jax.named_scope("begin"):
                arrived_but_last(ch)
                begin(ch)
                if squared:
                    begin_end(ch)
        for ch in last_three:
            with jax.named_scope("late"):
                crossed(far_edge, ch).wait_recv()
                complete(ch, squared)

    @on_edge
    def _():
        places = {"near": near, "far": far, "last": far_edge}
        sides = {"own": fsdp, "other": other}

        def take(name, s):
            grad_got(places[name], sides[s]).wait_recv()
            share(places[name], sides[s])

        def land(name, s, whole):
            r = rep if name == "rep" else places[name]
            pass_on(r, sides[s])
            if whole:
                settle(r, 1 if name == "rep" else 2)
                turn(r)

        def relay(*indices):
            for index in indices:
                if index + early < count:
                    own_inward(chunk(index + early))
                if index < count:
                    crossed(edge, chunk(index)).wait_recv()
                    hop_other(chunk(index)).start()

        def pull(slot, r):
            def event(ch):
                hop_got(slot, ch).wait_recv()
                cross(r, ch).start()
            return event

        def pull_near(ch):
            hop_got(0, ch).wait_recv()
            when_extra(ch, lambda: None, lambda: cross(near, ch, xn_send).start())

        pulls = [pull(1, far), pull(2, far_edge)]

        def near_at(*indices):
            for index in indices:
                pull_near(chunk(index))

        def near_ahead(ch):
            index = ch.index + FILL
            if isinstance(index, int):
                if index < count:
                    near_at(index)
                return
            pl.when(index < full)(lambda: near_at(index))
            if full < count:
                pl.when(index == full)(lambda: near_at(full))

        def early_events(*indices):
            for index in indices:
                if index >= early:
                    near_at(index + FILL)
                for event in pulls:
                    event(chunk(index))

        def arrived(ch):
            crossed(near, ch).wait_recv()
            crossed(far, ch).wait_recv()

        def compute(index):
            def whole(ch):
                arrived(ch)
                crossed(far_edge, ch).wait_recv()
            finish(chunk(index), whole, False)

        def batch(k):
            return range(k * count // 8, (k + 1) * count // 8)

        perform(
            [
                ("own",), ("across", 4, 9), ("take", "near", "own"), ("relay", *batch(0)),
                ("near", *range(early)), ("take", "near", "other"), ("across", 9, 12),
                ("land", "rep", "other", True), ("relay", *batch(1)),
                ("take", "far", "own"), ("across", 12, count), ("near", early), ("land", "near", "own", False),
                ("relay", *batch(2)), ("take", "far", "other"), ("near", early + 1),
                ("land", "near", "other", True), ("relay", *batch(3)), ("take", "last", "own"),
                ("near", early + 2), ("land", "far", "own", False), ("relay", *batch(4)),
                ("take", "last", "other"), ("land", "far", "other", True), ("relay", *batch(5)),
                ("early", 0), ("relay", *batch(6)), ("early", 1), ("land", "last", "own", False),
                ("relay", *batch(7)), ("early", 2), ("land", "last", "other", True),
                ("compute", 0), ("early", 3), ("compute", 1),
            ],
            {"own": take_own, "take": take, "land": land, "relay": relay, "early": early_events, "near": near_at,
             "compute": compute, "across": own_across},
        )

        def between():
            shares_sent()
            grads_sent(2, gz_in)
            all_sent(1, columns, z_in)
            all_sent(1, columns, zo_send)
            for index in range(count - 3, count):
                begin_end(chunk(index))

        sweep([near_ahead, *pulls], arrived, between, lambda: None, EDGE_LAG, False)
        all_sent(1, columns - extra_columns, xn_send)
        all_sent(3, columns, x_send)

    @on_middle
    def _():
        places = {"edge": edge, "far": far, "last": far_edge}
        sides = {"own": fsdp, "other": other}

        def take(name, s):
            r, s = places[name], sides[s]
            grad_got(r, s).wait_recv()
            grad_hop(r, s, name == "edge").start()
            share(r, s)

        def land(name, s, whole=True):
            r = rep if name == "rep" else places[name]
            pass_on(r, sides[s])
            if whole:
                settle(r, 1 if name == "rep" else 2)
                turn(r)

        def inward(*indices):
            for index in indices:
                ch = chunk(index)
                if not isinstance(index, int) or index >= early:
                    own_inward(ch)
                hop_got(0, ch).wait_recv()
                hop(edge, ch, True, 2).start()

        def fill(*indices):
            for index in indices:
                hop(rep, chunk(index), False, 0).start()

        def outer(ch):
            if isinstance(ch.index, int):
                if ch.index + FILL < count:
                    fill(ch.index + FILL)
            else:
                pl.when(ch.index + FILL < full)(lambda: fill(ch.index + FILL))
                if full < count:
                    pl.when(ch.index + FILL == full)(lambda: fill(full))
            follow(ch.index + AHEAD)
            if not isinstance(ch.index, int):
                pl.when(among_extra(ch.index))(lambda: send_extra(ch))

        def send_extra(ch):
            crossed(rep, ch).wait_recv()
            hop_extra(ch).start()

        def follow(index):
            if isinstance(index, int):
                if index < count:
                    inward(index)
                return
            pl.when(index < full)(lambda: inward(index))
            if full < count:
                pl.when(index == full)(lambda: inward(full))

        def pull(slot, r):
            def event(ch):
                hop_got(slot, ch).wait_recv()
                hop(r, ch, False, slot).start()
                cross(r, ch).start()
            return event

        pulls = [pull(1, far), pull(2, far_edge)]

        def early_events(*indices):
            for index in indices:
                if index >= early:
                    fill(index + FILL)
                for event in pulls:
                    event(chunk(index))

        perform(
            [
                ("own",), ("take", "far", "own"), ("across", 4, 9), ("fill", early),
                ("take", "edge", "own"), ("take", "edge", "other"), ("across", 9, 12),
                ("inward", *range(early)), ("take", "far", "other"),
                ("fill", early + 1), ("land", "rep", "other"), ("take", "last", "own"),
                ("across", 12, count),
                ("fill", early + 2), ("land", "far", "own", False),
                ("inward", *range(early, LAG)), ("take", "last", "other"), ("land", "edge", "own", False),
                ("early", 0, 1), ("inward", *range(LAG, LAG + 2)), ("land", "edge", "other"),
                ("land", "far", "other"), ("early", 2), ("inward", LAG + 2), ("land", "last", "own", False),
                ("early", 3), ("inward", LAG + 3), ("land", "last", "other"),
            ],
            {"own": take_own, "take": take, "land": land, "inward": inward, "early": early_events, "fill": fill,
             "across": own_across},
        )

        def arrived(ch):
            hop_other(ch).wait_recv()
            when_extra(ch, lambda: None, lambda: crossed(rep, ch).wait_recv())
            crossed(far, ch).wait_recv()

        clear()

        def ended():
            send_extra(chunk(count - 1))

        sweep([outer, *pulls], arrived, lambda: None, ended, LAG, True)

        mine = fsdp * n_tp + tp
        peers = [(a, k) for a in range(2) for k in range(n_tp) if a or k]

        def exchange(at):
            a, k = peers[at]
            to_side = other if a else fsdp
            to_tp = lax.rem(tp + k, n_tp)
            spot = sums.at[mine]
            return remote(spot, spot, sq_send, sq_recv, {"fsdp": to_side, "tp": to_tp})

        for at in range(len(peers)):
            exchange(at).start()
        with jax.named_scope("exchange"):
            seven = sums.at[pl.ds(0, len(peers))]
            remote(seven, seven, sq_send, sq_recv, {"fsdp": other}).wait_recv()
        square_total = jnp.sum(jnp.sum(sums[...], axis=0), keepdims=True)
        factor = 1.0 / jnp.sqrt(square_total / entry_count + 1e-06)
        total_out[...] = jnp.broadcast_to(factor, total_out.shape)
        remote(seven, seven, sq_send, sq_recv, {"fsdp": other}).wait_send()

    def tell():
        return remote(total_out, total_out, fa_send, fa_recv, {"rep": jnp.where(is_edge, near, edge)})

    on_middle(lambda: tell().start())
    with jax.named_scope("told"):
        on_edge(lambda: tell().wait_recv())
    factor_ref[...] = total_out[...]

    @on_middle
    def _():
        tell().wait_send()
        shares_sent()
        grads_sent(4, gz_in)
        grads_sent(6, gz_out)
        all_sent(2, columns, z_in)
        all_sent(3, columns, z_out)
        all_sent(3, columns, x_send)
        all_sent(1, extra_columns, ze_send)


def by_kernel(n_rep, n_tp, entry_count, gate_pre, up_pre, out_grad):
    rows, columns = gate_pre.shape
    tokens = rows * n_rep * 2
    half = out_grad.shape[1] // 2
    quarter = half // n_tp
    full, count, chunk = chunking(columns)
    kept = 2 * WIDTH + chunk(count - 1).size
    dma = pltpu.SemaphoreType.DMA
    block, whole = dma((n_rep, 2)), dma((n_rep,))
    return pl.pallas_call(
        functools.partial(gather_multiply, entry_count),
        out_shape=(
            pltpu.VMEM((half, columns), jnp.bfloat16),
            pltpu.VMEM((8, LANES), jnp.float32),
        ),
        in_specs=[pl.BlockSpec(memory_space=pl.ANY)] * 3,
        out_specs=(pl.BlockSpec(memory_space=pltpu.VMEM), pl.BlockSpec(memory_space=pltpu.VMEM)),
        scratch_shapes=[
            pltpu.VMEM((tokens, columns), jnp.bfloat16),
            pltpu.VMEM((tokens, half), jnp.bfloat16),
            pltpu.VMEM((half, tokens), jnp.bfloat16),
            pltpu.VMEM((rows, columns), jnp.bfloat16),
            pltpu.VMEM((rows, columns), jnp.bfloat16),
            pltpu.VMEM((rows, quarter), jnp.bfloat16),
            pltpu.VMEM((2 * n_tp, 8, LANES), jnp.float32),
            pltpu.VMEM((8, LANES), jnp.float32),
            pltpu.VMEM((half, kept), jnp.float32),
            pltpu.VMEM((half, kept), jnp.float32),
            dma((4,)), dma, dma, block, dma, dma, dma, block,
            dma, whole, dma, whole,
            dma((3, count)), dma, dma, dma, dma, dma, dma, dma((n_rep, count)),
            dma, dma, dma, dma,
        ],
        compiler_params=pltpu.CompilerParams(
            collective_id=0, has_side_effects=True, vmem_limit_bytes=VMEM_LIMIT * 4 // 5
        ),
    )(gate_pre, up_pre, out_grad)


def scale(summed, factors):
    half, columns = summed.shape
    rows = 128

    def body(summed_ref, factor_ref, out_ref, ready, sems):
        steps = half // rows
        depth = ready.shape[0]

        def leave(m):
            slot = lax.rem(m, depth)
            spot = pl.ds(pl.multiple_of(m * rows, rows), rows)
            return pltpu.make_async_copy(ready.at[slot], out_ref.at[spot, :], sems.at[slot])

        @pl.loop(0, steps)
        def _(m):
            slot = lax.rem(m, depth)
            spot = pl.ds(pl.multiple_of(m * rows, rows), rows)

            @pl.when(m >= depth)
            def _():
                leave(m - depth).wait()
            for at in range(0, columns, LANES):
                cols = pl.ds(at, LANES)
                scaled = summed_ref[spot, cols].astype(jnp.float32) * factor_ref[0:1, :]
                ready[slot, :, cols] = scaled.astype(ready.dtype)
            leave(m).start()

        @pl.loop(max(steps - depth, 0), steps)
        def _(m):
            leave(m).wait()

    return pl.pallas_call(
        body,
        out_shape=jax.ShapeDtypeStruct((half, columns), jnp.bfloat16),
        in_specs=[pl.BlockSpec(memory_space=pltpu.VMEM)] * 2,
        out_specs=pl.BlockSpec(memory_space=pl.ANY),
        scratch_shapes=[pltpu.VMEM((4, rows, columns), jnp.bfloat16), pltpu.SemaphoreType.DMA((4,))],
        compiler_params=pltpu.CompilerParams(vmem_limit_bytes=16 * 1024 * 1024),
    )(summed, factors)


def by_xla(gate_pre, up_pre, out_grad):
    hidden = (jax.nn.silu(gate_pre.astype(jnp.float32)) * up_pre.astype(jnp.float32)).astype(
        jnp.bfloat16
    )
    spread = lax.all_to_all(out_grad, "fsdp", split_axis=1, concat_axis=0, tiled=True)
    grad_rows = lax.all_gather(spread, "rep", axis=0, tiled=True)
    hidden_rows = lax.all_gather(hidden, ("rep", "fsdp"), axis=0, tiled=True)
    summed = lax.dot_general(
        grad_rows, hidden_rows, (((0,), (0,)), ((), ())), preferred_element_type=jnp.float32
    )
    return summed, jnp.sum(summed * summed)


def kernel_fits(n_rep, n_fsdp, n_tp, rows, columns, features):
    tokens, half = rows * n_rep * n_fsdp, features // n_fsdp
    held_bytes = 2 * (tokens * columns + 2 * tokens * half + half * columns + 2 * rows * columns)
    held_bytes += 24 * half * WIDTH
    aligned = rows % 128 == 0 and columns % LANES == 0 and half % (LANES * n_tp) == 0
    shaped = (n_rep, n_fsdp, n_tp) == (4, 2, 4) and columns >= max(12 * WIDTH, 7 * half // n_tp)
    return shaped and aligned and half % TILE == 0 and held_bytes < VMEM_LIMIT * 4 // 5


def solution(mesh):
    n_rep, n_fsdp, n_tp = (mesh.shape[axis] for axis in ("rep", "fsdp", "tp"))

    def on_device(gate_pre, up_pre, out_grad):
        half, columns = out_grad.shape[1] // n_fsdp, gate_pre.shape[1]
        entry_count = half * n_fsdp * columns * n_tp
        if kernel_fits(n_rep, n_fsdp, n_tp, *gate_pre.shape, out_grad.shape[1]):
            summed, factors = by_kernel(n_rep, n_tp, entry_count, gate_pre, up_pre, out_grad)
            return scale(summed, factors)
        summed, square_sum = by_xla(gate_pre, up_pre, out_grad)
        square_total = lax.psum(square_sum, ("fsdp", "tp"))
        factor = 1.0 / jnp.sqrt(square_total / entry_count + 1e-06)
        return (summed * factor).astype(jnp.bfloat16)

    return jax.shard_map(
        on_device,
        mesh=mesh,
        in_specs=(P(("rep", "fsdp"), "tp"), P(("rep", "fsdp"), "tp"), P(("rep", "fsdp"), None)),
        out_specs=P("fsdp", "tp"),
        check_vma=False,
    )
```

```python
import functools

import jax
import jax.numpy as jnp
from jax import lax
from jax.experimental import pallas as pl
from jax.experimental.pallas import tpu as pltpu
from jax.sharding import PartitionSpec as P

MESH = pl.DeviceIdType.MESH
LANES = 128
VMEM_LIMIT = 60 * 1024 * 1024
WIDTH = 256
TILE = 2048
LAG = 4
EDGE_LAG = 2
AHEAD = 4
FILL = 3
EXTRA = (5, 9)


class Chunk:
    def __init__(self, index, start, size):
        self.index, self.start, self.size = index, start, size

    @property
    def cols(self):
        start = self.start
        return pl.ds(start if isinstance(start, int) else pl.multiple_of(start, LANES), self.size)


def chunking(columns):
    full, rest = columns // WIDTH, columns % WIDTH

    def chunk(index):
        if isinstance(index, int) and index == full:
            return Chunk(index, full * WIDTH, rest)
        return Chunk(index, index * WIDTH, WIDTH)

    return full, full + (1 if rest else 0), chunk


def gather_multiply(
    entry_count, gate_ref, up_ref, grad_ref, out_ref, factor_ref,
    held, grads, turned, gate_in, up_in, across_in, sums, total_out,
    middle_part, end_part,
    local_sem, gx_send, gx_recv, gz_recv, gz_out, gz_in, gy_send, gy_recv,
    gs_send, gs_recv, gf_send, gf_recv,
    z_recv, z_out, z_in, zo_send, ze_send, x_send, xn_send, x_recv,
    sq_send, sq_recv, fa_send, fa_recv,
):
    rep = lax.axis_index("rep")
    fsdp = lax.axis_index("fsdp")
    tp = lax.axis_index("tp")
    rows, columns = gate_ref.shape
    half = grads.shape[1]
    n_tp = 4
    quarter = half // n_tp
    full, count, chunk = chunking(columns)
    extras = (*EXTRA, count - 1)
    extra_columns = len(EXTRA) * WIDTH + chunk(count - 1).size
    other = 1 - fsdp
    side = rep // 2
    edge, near, far, far_edge = 3 * side, 1 + side, 2 - side, 3 - 3 * side
    is_edge = rep == edge
    inner = jnp.where(is_edge, near, far)
    sibling = tp + 1 - 2 * lax.rem(tp, 2)
    opposite = lax.rem(tp + 2, n_tp)
    past = lax.rem(sibling + 2, n_tp)

    def rows_of(r, s):
        return pl.ds(pl.multiple_of((r * 2 + s) * rows, rows), rows)

    def quarter_of(t):
        return pl.ds(pl.multiple_of(t * quarter, LANES), quarter)

    def remote(src, dst, send, recv, device):
        return pltpu.make_async_remote_copy(
            src_ref=src, dst_ref=dst, send_sem=send, recv_sem=recv,
            device_id=device, device_id_type=MESH,
        )

    loads = [
        pltpu.make_async_copy(
            grad_ref.at[:, pl.ds(pl.multiple_of(other * half + tp * quarter, LANES), quarter)],
            across_in, local_sem.at[0],
        ),
        pltpu.make_async_copy(
            grad_ref.at[:, pl.ds(pl.multiple_of(fsdp * half, LANES), half)],
            grads.at[rows_of(rep, fsdp), :], local_sem.at[1],
        ),
        pltpu.make_async_copy(gate_ref, gate_in, local_sem.at[2]),
        pltpu.make_async_copy(up_ref, up_in, local_sem.at[3]),
    ]
    for load in loads:
        load.start()

    barrier = pltpu.get_barrier_semaphore()
    for peer in ({"fsdp": other}, {"tp": sibling}, {"tp": opposite}):
        pl.semaphore_signal(barrier, inc=1, device_id=peer, device_id_type=MESH)
    pl.semaphore_signal(barrier, inc=1, device_id={"rep": inner}, device_id_type=MESH)

    @pl.when(jnp.logical_not(is_edge))
    def _():
        pl.semaphore_signal(barrier, inc=1, device_id={"rep": edge}, device_id_type=MESH)

    with jax.named_scope("barrier"):
        pl.semaphore_wait(barrier, 4 + jnp.where(is_edge, 0, 1))

    def grad_across():
        return remote(across_in, grads.at[rows_of(rep, fsdp), quarter_of(tp)], gx_send, gx_recv, {"fsdp": other})

    def grad_spot(r, s, t):
        return grads.at[rows_of(r, s), quarter_of(t)]

    def grad_hop(r, s, inward):
        spot = grad_spot(r, s, tp)
        to = inner if inward else edge
        return remote(spot, spot, (gz_in if inward else gz_out), gz_recv.at[r, s], {"rep": to})

    def grad_got(r, s):
        spot = grad_spot(r, s, tp)
        return remote(spot, spot, gz_in, gz_recv.at[r, s], {"rep": inner})

    def over_y(r, s, t):
        spot = grad_spot(r, s, t)
        return remote(spot, spot, gy_send, gy_recv.at[r, s], {"tp": opposite})

    def to_sibling(r, s, t):
        spot = grad_spot(r, s, t)
        return remote(spot, spot, gs_send, gs_recv.at[r], {"tp": sibling})

    def pass_sibling(r, s, t):
        spot = grad_spot(r, s, t)
        return remote(spot, spot, gf_send, gf_recv.at[r], {"tp": sibling})

    def hop(r, ch, inward, slot):
        spot = held.at[rows_of(r, fsdp), ch.cols]
        to = inner if inward else edge
        return remote(spot, spot, z_in if inward else z_out, z_recv.at[slot, ch.index], {"rep": to})

    def hop_got(slot, ch):
        spot = held.at[pl.ds(0, rows), ch.cols]
        return remote(spot, spot, z_in, z_recv.at[slot, ch.index], {"rep": inner})

    def hop_other(ch):
        spot = held.at[rows_of(edge, other), ch.cols]
        return remote(spot, spot, zo_send, x_recv.at[edge, ch.index], {"rep": inner})

    def cross(r, ch, send=None):
        spot = held.at[rows_of(r, fsdp), ch.cols]
        return remote(spot, spot, x_send if send is None else send, x_recv.at[r, ch.index], {"fsdp": other})

    def crossed(r, ch):
        spot = held.at[rows_of(r, other), ch.cols]
        return remote(spot, spot, x_send, x_recv.at[r, ch.index], {"fsdp": other})

    def hop_extra(ch):
        spot = held.at[rows_of(near, other), ch.cols]
        return remote(spot, spot, ze_send, x_recv.at[near, ch.index], {"rep": jnp.where(is_edge, near, edge)})

    def all_sent(blocks, width, send):
        spot = held.at[pl.ds(0, blocks * rows), pl.ds(0, width)]
        remote(spot, spot, send, gx_recv, {"fsdp": other}).wait_send()

    def among_extra(index):
        return functools.reduce(jnp.logical_or, [index == at for at in EXTRA])

    def when_extra(ch, act, otherwise):
        if isinstance(ch.index, int):
            act() if ch.index in extras else otherwise()
            return
        pl.when(among_extra(ch.index))(act)
        pl.when(jnp.logical_not(among_extra(ch.index)))(otherwise)

    def on_edge(act):
        pl.when(is_edge)(act)

    def on_middle(act):
        pl.when(jnp.logical_not(is_edge))(act)

    def chunks_from(low, high, act):
        if low < min(high, full):
            @pl.loop(low, min(high, full))
            def _(index):
                act(chunk(index))
        if full < count == high:
            act(chunk(full))

    loads[0].wait()
    grad_across().start()
    loads[1].wait()
    grad_hop(rep, fsdp, True).start()
    on_middle(lambda: grad_hop(rep, fsdp, False).start())

    with jax.named_scope("load"):
        loads[2].wait()
        loads[3].wait()

    @pl.loop(0, columns // LANES)
    def _(at):
        cols = pl.ds(pl.multiple_of(at * LANES, LANES), LANES)
        gate = gate_in[:, cols].astype(jnp.float32)
        held[rows_of(rep, fsdp), cols] = (
            jax.nn.silu(gate) * up_in[:, cols].astype(jnp.float32)
        ).astype(held.dtype)

    early = 2

    def own_inward(ch):
        hop(rep, ch, True, jnp.where(is_edge, 0, 1)).start()

    chunks_from(0, early, own_inward)
    on_middle(lambda: chunks_from(0, early, lambda ch: hop(rep, ch, False, 0).start()))

    def own_across(low, high):
        for index in range(low, min(high, count)):
            cross(rep, chunk(index)).start()

    own_across(0, 4)

    def share(r, s):
        over_y(r, s, tp).start()
        to_sibling(r, s, tp).start()

    def pass_on(r, s):
        over_y(r, s, opposite).wait_recv()
        pass_sibling(r, s, opposite).start()

    def settle(r, pairs):
        spots = grads.at[pl.ds(0, pairs * rows), pl.ds(0, quarter)]
        remote(spots, spots, gs_send, gs_recv.at[r], {"tp": sibling}).wait_recv()
        remote(spots, spots, gf_send, gf_recv.at[r], {"tp": sibling}).wait_recv()

    tile = 256

    def turn(r):
        spot = pl.ds(pl.multiple_of(r * 2 * rows, 2 * rows), 2 * rows)

        @pl.loop(0, half // tile)
        def _(m):
            part = pl.ds(pl.multiple_of(m * tile, tile), tile)
            turned[part, spot] = grads[spot, part].T

    def take_own():
        grad_across().wait_recv()
        grad_hop(rep, other, True).start()
        on_middle(lambda: grad_hop(rep, other, False).start())
        share(rep, other)

    def perform(plan, acts):
        for at, (name, *args) in enumerate(plan):
            with jax.named_scope(f"{name}{at}"):
                acts[name](*args)

    def grads_sent(blocks, send):
        all_sent(1, blocks * quarter, send)

    def shares_sent():
        grad_across().wait_send()
        for send in (gy_send, gs_send, gf_send):
            grads_sent(7, send)

    def clear():
        sums[fsdp * n_tp + tp] = jnp.zeros(sums.shape[1:], sums.dtype)

    def leave(product, spot, ch, squared):
        out_ref[spot, ch.cols] = product.astype(out_ref.dtype)
        if squared:
            squares = jnp.sum((product * product).reshape(TILE // 8, 8, ch.size), axis=0)
            total = squares[:, :LANES]
            for at in range(LANES, ch.size, LANES):
                total = total + squares[:, at:at + LANES]
            sums[fsdp * n_tp + tp] += total

    def tile_of(m):
        return pl.ds(pl.multiple_of(m * TILE, TILE), TILE)

    def multiply_tile(ch, m, squared):
        spot = tile_of(m)
        product = jnp.dot(turned[spot, :], held[:, ch.cols], preferred_element_type=jnp.float32)
        leave(product, spot, ch, squared)

    pair = 2 * rows
    ends = {"first": pl.multiple_of(edge * pair, pair), "late": pl.multiple_of(far_edge * pair, pair)}

    def part(spot, ch, start, size):
        tokens = pl.ds(start, size)
        return jnp.dot(turned[spot, tokens], held[tokens, ch.cols], preferred_element_type=jnp.float32)

    def kept(ch):
        return pl.ds((ch.index - (count - 3)) * WIDTH, ch.size)

    def begin(ch):
        @pl.loop(0, tiles)
        def _(m):
            spot = tile_of(m)
            middle_part[spot, kept(ch)] = part(spot, ch, pair, 2 * pair)

    def begin_end(ch):
        @pl.loop(0, tiles)
        def _(m):
            spot = tile_of(m)
            end_part[spot, kept(ch)] = part(spot, ch, ends["first"], pair)

    def complete(ch, squared):
        @pl.loop(0, tiles)
        def _(m):
            spot = tile_of(m)
            both = end_part[spot, kept(ch)] + part(spot, ch, ends["late"], pair)
            leave(middle_part[spot, kept(ch)] + both, spot, ch, squared)

    tiles = half // TILE

    def finish(ch, arrived, squared):
        with jax.named_scope("arrived_last"):
            arrived(ch)
        with jax.named_scope("multiply_last"):
            pl.loop(0, tiles)(lambda m: multiply_tile(ch, m, squared))

    def sweep(events, arrived_but_last, between, ended, lag, squared):
        def arrived(ch):
            arrived_but_last(ch)
            crossed(far_edge, ch).wait_recv()

        places = [at * tiles // len(events) for at in range(len(events))]

        def step(index):
            ch, lagging = chunk(index), chunk(index - lag)
            plan = [(place, event, ch) for place, event in zip(places, events)]
            plan.insert(sum(place == 0 for place in places), (0, arrived, lagging))

            @pl.loop(0, tiles)
            def _(m):
                for at, (place, event, subject) in enumerate(plan):
                    def run():
                        with jax.named_scope(f"event{at}"):
                            event(subject)
                    pl.when(m == place)(run)
                with jax.named_scope("multiply"):
                    multiply_tile(lagging, m, squared)

        last_three = [chunk(index) for index in range(count - 3, count)]
        far_pull, last_pull = events[1:]
        pl.loop(LAG, count - 3)(step)
        between()
        remaining = count - 3 - lag
        with jax.named_scope("far_last"):
            far_pull(last_three[0])
        chunks_from(remaining, remaining + 1, lambda ch: finish(ch, arrived, squared))
        with jax.named_scope("far_last"):
            for ch in last_three[1:]:
                far_pull(ch)
        with jax.named_scope("pull_last"):
            last_pull(last_three[0])
        chunks_from(remaining + 1, count - 3, lambda ch: finish(ch, arrived, squared))
        with jax.named_scope("pull_last"):
            for ch in last_three[1:]:
                last_pull(ch)
        ended()
        for ch in last_three:
            with jax.named_scope("begin"):
                arrived_but_last(ch)
                begin(ch)
                if squared:
                    begin_end(ch)
        for ch in last_three:
            with jax.named_scope("late"):
                crossed(far_edge, ch).wait_recv()
                complete(ch, squared)

    @on_edge
    def _():
        places = {"near": near, "far": far, "last": far_edge}
        sides = {"own": fsdp, "other": other}

        def take(name, s):
            grad_got(places[name], sides[s]).wait_recv()
            share(places[name], sides[s])

        def land(name, s, whole):
            r = rep if name == "rep" else places[name]
            pass_on(r, sides[s])
            if whole:
                settle(r, 1 if name == "rep" else 2)
                turn(r)

        def relay(*indices):
            for index in indices:
                if index + early < count:
                    own_inward(chunk(index + early))
                if index < count:
                    crossed(edge, chunk(index)).wait_recv()
                    hop_other(chunk(index)).start()

        def pull(slot, r):
            def event(ch):
                hop_got(slot, ch).wait_recv()
                cross(r, ch).start()
            return event

        def pull_near(ch):
            hop_got(0, ch).wait_recv()
            when_extra(ch, lambda: None, lambda: cross(near, ch, xn_send).start())

        pulls = [pull(1, far), pull(2, far_edge)]

        def near_at(*indices):
            for index in indices:
                pull_near(chunk(index))

        def near_ahead(ch):
            index = ch.index + FILL
            if isinstance(index, int):
                if index < count:
                    near_at(index)
                return
            pl.when(index < full)(lambda: near_at(index))
            if full < count:
                pl.when(index == full)(lambda: near_at(full))

        def early_events(*indices):
            for index in indices:
                if index >= early:
                    near_at(index + FILL)
                for event in pulls:
                    event(chunk(index))

        def arrived(ch):
            crossed(near, ch).wait_recv()
            crossed(far, ch).wait_recv()

        def compute(index):
            def whole(ch):
                arrived(ch)
                crossed(far_edge, ch).wait_recv()
            finish(chunk(index), whole, False)

        def batch(k):
            return range(k * count // 8, (k + 1) * count // 8)

        perform(
            [
                ("own",), ("across", 4, 9), ("take", "near", "own"), ("relay", *batch(0)),
                ("near", *range(early)), ("take", "near", "other"), ("across", 9, 12),
                ("land", "rep", "other", True), ("relay", *batch(1)),
                ("take", "far", "own"), ("across", 12, count), ("near", early), ("land", "near", "own", False),
                ("relay", *batch(2)), ("take", "far", "other"), ("near", early + 1),
                ("land", "near", "other", True), ("relay", *batch(3)), ("take", "last", "own"),
                ("near", early + 2), ("land", "far", "own", False), ("relay", *batch(4)),
                ("take", "last", "other"), ("land", "far", "other", True), ("relay", *batch(5)),
                ("early", 0), ("relay", *batch(6)), ("early", 1), ("land", "last", "own", False),
                ("relay", *batch(7)), ("early", 2), ("land", "last", "other", True),
                ("compute", 0), ("early", 3), ("compute", 1),
            ],
            {"own": take_own, "take": take, "land": land, "relay": relay, "early": early_events, "near": near_at,
             "compute": compute, "across": own_across},
        )

        def between():
            shares_sent()
            grads_sent(2, gz_in)
            all_sent(1, columns, z_in)
            all_sent(1, columns, zo_send)

        def near_and_part(ch):
            near_ahead(ch)
            for at in range(3):
                pl.when(ch.index == LAG + 2 + at)(lambda: begin_end(chunk(count - 3 + at)))

        sweep([near_and_part, *pulls], arrived, between, lambda: None, EDGE_LAG, False)
        all_sent(1, columns - extra_columns, xn_send)
        all_sent(3, columns, x_send)

    @on_middle
    def _():
        places = {"edge": edge, "far": far, "last": far_edge}
        sides = {"own": fsdp, "other": other}

        def take(name, s):
            r, s = places[name], sides[s]
            grad_got(r, s).wait_recv()
            grad_hop(r, s, name == "edge").start()
            share(r, s)

        def land(name, s, whole=True):
            r = rep if name == "rep" else places[name]
            pass_on(r, sides[s])
            if whole:
                settle(r, 1 if name == "rep" else 2)
                turn(r)

        def inward(*indices):
            for index in indices:
                ch = chunk(index)
                if not isinstance(index, int) or index >= early:
                    own_inward(ch)
                hop_got(0, ch).wait_recv()
                hop(edge, ch, True, 2).start()

        def fill(*indices):
            for index in indices:
                hop(rep, chunk(index), False, 0).start()

        def outer(ch):
            if isinstance(ch.index, int):
                if ch.index + FILL < count:
                    fill(ch.index + FILL)
            else:
                pl.when(ch.index + FILL < full)(lambda: fill(ch.index + FILL))
                if full < count:
                    pl.when(ch.index + FILL == full)(lambda: fill(full))
            follow(ch.index + AHEAD)
            if not isinstance(ch.index, int):
                pl.when(among_extra(ch.index))(lambda: send_extra(ch))

        def send_extra(ch):
            crossed(rep, ch).wait_recv()
            hop_extra(ch).start()

        def follow(index):
            if isinstance(index, int):
                if index < count:
                    inward(index)
                return
            pl.when(index < full)(lambda: inward(index))
            if full < count:
                pl.when(index == full)(lambda: inward(full))

        def pull(slot, r):
            def event(ch):
                hop_got(slot, ch).wait_recv()
                hop(r, ch, False, slot).start()
                cross(r, ch).start()
            return event

        pulls = [pull(1, far), pull(2, far_edge)]

        def early_events(*indices):
            for index in indices:
                if index >= early:
                    fill(index + FILL)
                for event in pulls:
                    event(chunk(index))

        perform(
            [
                ("own",), ("take", "far", "own"), ("across", 4, 9), ("fill", early),
                ("take", "edge", "own"), ("take", "edge", "other"), ("across", 9, 12),
                ("inward", *range(early)), ("take", "far", "other"),
                ("fill", early + 1), ("land", "rep", "other"), ("take", "last", "own"),
                ("across", 12, count),
                ("fill", early + 2), ("land", "far", "own", False),
                ("inward", *range(early, LAG)), ("take", "last", "other"), ("land", "edge", "own", False),
                ("early", 0, 1), ("inward", *range(LAG, LAG + 2)), ("land", "edge", "other"),
                ("land", "far", "other"), ("early", 2), ("inward", LAG + 2), ("land", "last", "own", False),
                ("early", 3), ("inward", LAG + 3), ("land", "last", "other"),
            ],
            {"own": take_own, "take": take, "land": land, "inward": inward, "early": early_events, "fill": fill,
             "across": own_across},
        )

        def arrived(ch):
            hop_other(ch).wait_recv()
            when_extra(ch, lambda: None, lambda: crossed(rep, ch).wait_recv())
            crossed(far, ch).wait_recv()

        clear()

        def ended():
            send_extra(chunk(count - 1))

        sweep([outer, *pulls], arrived, lambda: None, ended, LAG, True)

        mine = fsdp * n_tp + tp
        peers = [(a, k) for a in range(2) for k in range(n_tp) if a or k]

        def exchange(at):
            a, k = peers[at]
            to_side = other if a else fsdp
            to_tp = lax.rem(tp + k, n_tp)
            spot = sums.at[mine]
            return remote(spot, spot, sq_send, sq_recv, {"fsdp": to_side, "tp": to_tp})

        for at in range(len(peers)):
            exchange(at).start()
        with jax.named_scope("exchange"):
            seven = sums.at[pl.ds(0, len(peers))]
            remote(seven, seven, sq_send, sq_recv, {"fsdp": other}).wait_recv()
        square_total = jnp.sum(jnp.sum(sums[...], axis=0), keepdims=True)
        factor = 1.0 / jnp.sqrt(square_total / entry_count + 1e-06)
        total_out[...] = jnp.broadcast_to(factor, total_out.shape)
        remote(seven, seven, sq_send, sq_recv, {"fsdp": other}).wait_send()

    def tell():
        return remote(total_out, total_out, fa_send, fa_recv, {"rep": jnp.where(is_edge, near, edge)})

    on_middle(lambda: tell().start())
    with jax.named_scope("told"):
        on_edge(lambda: tell().wait_recv())
    factor_ref[...] = total_out[...]

    @on_middle
    def _():
        tell().wait_send()
        shares_sent()
        grads_sent(4, gz_in)
        grads_sent(6, gz_out)
        all_sent(2, columns, z_in)
        all_sent(3, columns, z_out)
        all_sent(3, columns, x_send)
        all_sent(1, extra_columns, ze_send)


def by_kernel(n_rep, n_tp, entry_count, gate_pre, up_pre, out_grad):
    rows, columns = gate_pre.shape
    tokens = rows * n_rep * 2
    half = out_grad.shape[1] // 2
    quarter = half // n_tp
    full, count, chunk = chunking(columns)
    kept = 2 * WIDTH + chunk(count - 1).size
    dma = pltpu.SemaphoreType.DMA
    block, whole = dma((n_rep, 2)), dma((n_rep,))
    return pl.pallas_call(
        functools.partial(gather_multiply, entry_count),
        out_shape=(
            pltpu.VMEM((half, columns), jnp.bfloat16),
            pltpu.VMEM((8, LANES), jnp.float32),
        ),
        in_specs=[pl.BlockSpec(memory_space=pl.ANY)] * 3,
        out_specs=(pl.BlockSpec(memory_space=pltpu.VMEM), pl.BlockSpec(memory_space=pltpu.VMEM)),
        scratch_shapes=[
            pltpu.VMEM((tokens, columns), jnp.bfloat16),
            pltpu.VMEM((tokens, half), jnp.bfloat16),
            pltpu.VMEM((half, tokens), jnp.bfloat16),
            pltpu.VMEM((rows, columns), jnp.bfloat16),
            pltpu.VMEM((rows, columns), jnp.bfloat16),
            pltpu.VMEM((rows, quarter), jnp.bfloat16),
            pltpu.VMEM((2 * n_tp, 8, LANES), jnp.float32),
            pltpu.VMEM((8, LANES), jnp.float32),
            pltpu.VMEM((half, kept), jnp.float32),
            pltpu.VMEM((half, kept), jnp.float32),
            dma((4,)), dma, dma, block, dma, dma, dma, block,
            dma, whole, dma, whole,
            dma((3, count)), dma, dma, dma, dma, dma, dma, dma((n_rep, count)),
            dma, dma, dma, dma,
        ],
        compiler_params=pltpu.CompilerParams(
            collective_id=0, has_side_effects=True, vmem_limit_bytes=VMEM_LIMIT * 4 // 5
        ),
    )(gate_pre, up_pre, out_grad)


def scale(summed, factors):
    half, columns = summed.shape
    rows = 128

    def body(summed_ref, factor_ref, out_ref, ready, sems):
        steps = half // rows
        depth = ready.shape[0]

        def leave(m):
            slot = lax.rem(m, depth)
            spot = pl.ds(pl.multiple_of(m * rows, rows), rows)
            return pltpu.make_async_copy(ready.at[slot], out_ref.at[spot, :], sems.at[slot])

        @pl.loop(0, steps)
        def _(m):
            slot = lax.rem(m, depth)
            spot = pl.ds(pl.multiple_of(m * rows, rows), rows)

            @pl.when(m >= depth)
            def _():
                leave(m - depth).wait()
            for at in range(0, columns, LANES):
                cols = pl.ds(at, LANES)
                scaled = summed_ref[spot, cols].astype(jnp.float32) * factor_ref[0:1, :]
                ready[slot, :, cols] = scaled.astype(ready.dtype)
            leave(m).start()

        @pl.loop(max(steps - depth, 0), steps)
        def _(m):
            leave(m).wait()

    return pl.pallas_call(
        body,
        out_shape=jax.ShapeDtypeStruct((half, columns), jnp.bfloat16),
        in_specs=[pl.BlockSpec(memory_space=pltpu.VMEM)] * 2,
        out_specs=pl.BlockSpec(memory_space=pl.ANY),
        scratch_shapes=[pltpu.VMEM((4, rows, columns), jnp.bfloat16), pltpu.SemaphoreType.DMA((4,))],
        compiler_params=pltpu.CompilerParams(vmem_limit_bytes=16 * 1024 * 1024),
    )(summed, factors)


def by_xla(gate_pre, up_pre, out_grad):
    hidden = (jax.nn.silu(gate_pre.astype(jnp.float32)) * up_pre.astype(jnp.float32)).astype(
        jnp.bfloat16
    )
    spread = lax.all_to_all(out_grad, "fsdp", split_axis=1, concat_axis=0, tiled=True)
    grad_rows = lax.all_gather(spread, "rep", axis=0, tiled=True)
    hidden_rows = lax.all_gather(hidden, ("rep", "fsdp"), axis=0, tiled=True)
    summed = lax.dot_general(
        grad_rows, hidden_rows, (((0,), (0,)), ((), ())), preferred_element_type=jnp.float32
    )
    return summed, jnp.sum(summed * summed)


def kernel_fits(n_rep, n_fsdp, n_tp, rows, columns, features):
    tokens, half = rows * n_rep * n_fsdp, features // n_fsdp
    held_bytes = 2 * (tokens * columns + 2 * tokens * half + half * columns + 2 * rows * columns)
    held_bytes += 24 * half * WIDTH
    aligned = rows % 128 == 0 and columns % LANES == 0 and half % (LANES * n_tp) == 0
    shaped = (n_rep, n_fsdp, n_tp) == (4, 2, 4) and columns >= max(12 * WIDTH, 7 * half // n_tp)
    return shaped and aligned and half % TILE == 0 and held_bytes < VMEM_LIMIT * 4 // 5


def solution(mesh):
    n_rep, n_fsdp, n_tp = (mesh.shape[axis] for axis in ("rep", "fsdp", "tp"))

    def on_device(gate_pre, up_pre, out_grad):
        half, columns = out_grad.shape[1] // n_fsdp, gate_pre.shape[1]
        entry_count = half * n_fsdp * columns * n_tp
        if kernel_fits(n_rep, n_fsdp, n_tp, *gate_pre.shape, out_grad.shape[1]):
            summed, factors = by_kernel(n_rep, n_tp, entry_count, gate_pre, up_pre, out_grad)
            return scale(summed, factors)
        summed, square_sum = by_xla(gate_pre, up_pre, out_grad)
        square_total = lax.psum(square_sum, ("fsdp", "tp"))
        factor = 1.0 / jnp.sqrt(square_total / entry_count + 1e-06)
        return (summed * factor).astype(jnp.bfloat16)

    return jax.shard_map(
        on_device,
        mesh=mesh,
        in_specs=(P(("rep", "fsdp"), "tp"), P(("rep", "fsdp"), "tp"), P(("rep", "fsdp"), None)),
        out_specs=P("fsdp", "tp"),
        check_vma=False,
    )
```

```python
import functools

import jax
import jax.numpy as jnp
from jax import lax
from jax.experimental import pallas as pl
from jax.experimental.pallas import tpu as pltpu
from jax.sharding import PartitionSpec as P

MESH = pl.DeviceIdType.MESH
LANES = 128
VMEM_LIMIT = 60 * 1024 * 1024
WIDTH = 256
TILE = 1024
LAG = 4
EDGE_LAG = 2
AHEAD = 4
FILL = 3
EXTRA = (5, 9)


class Chunk:
    def __init__(self, index, start, size):
        self.index, self.start, self.size = index, start, size

    @property
    def cols(self):
        start = self.start
        return pl.ds(start if isinstance(start, int) else pl.multiple_of(start, LANES), self.size)


def chunking(columns):
    full, rest = columns // WIDTH, columns % WIDTH

    def chunk(index):
        if isinstance(index, int) and index == full:
            return Chunk(index, full * WIDTH, rest)
        return Chunk(index, index * WIDTH, WIDTH)

    return full, full + (1 if rest else 0), chunk


def gather_multiply(
    entry_count, gate_ref, up_ref, grad_ref, out_ref, factor_ref,
    held, grads, turned, gate_in, up_in, across_in, sums, total_out,
    middle_part, end_part,
    local_sem, gx_send, gx_recv, gz_recv, gz_out, gz_in, gy_send, gy_recv,
    gs_send, gs_recv, gf_send, gf_recv,
    z_recv, z_out, z_in, zo_send, ze_send, x_send, xn_send, x_recv,
    sq_send, sq_recv, fa_send, fa_recv,
):
    rep = lax.axis_index("rep")
    fsdp = lax.axis_index("fsdp")
    tp = lax.axis_index("tp")
    rows, columns = gate_ref.shape
    half = grads.shape[1]
    n_tp = 4
    quarter = half // n_tp
    full, count, chunk = chunking(columns)
    extras = (*EXTRA, count - 1)
    extra_columns = len(EXTRA) * WIDTH + chunk(count - 1).size
    other = 1 - fsdp
    side = rep // 2
    edge, near, far, far_edge = 3 * side, 1 + side, 2 - side, 3 - 3 * side
    is_edge = rep == edge
    inner = jnp.where(is_edge, near, far)
    sibling = tp + 1 - 2 * lax.rem(tp, 2)
    opposite = lax.rem(tp + 2, n_tp)
    past = lax.rem(sibling + 2, n_tp)

    def rows_of(r, s):
        return pl.ds(pl.multiple_of((r * 2 + s) * rows, rows), rows)

    def quarter_of(t):
        return pl.ds(pl.multiple_of(t * quarter, LANES), quarter)

    def remote(src, dst, send, recv, device):
        return pltpu.make_async_remote_copy(
            src_ref=src, dst_ref=dst, send_sem=send, recv_sem=recv,
            device_id=device, device_id_type=MESH,
        )

    loads = [
        pltpu.make_async_copy(
            grad_ref.at[:, pl.ds(pl.multiple_of(other * half + tp * quarter, LANES), quarter)],
            across_in, local_sem.at[0],
        ),
        pltpu.make_async_copy(
            grad_ref.at[:, pl.ds(pl.multiple_of(fsdp * half, LANES), half)],
            grads.at[rows_of(rep, fsdp), :], local_sem.at[1],
        ),
        pltpu.make_async_copy(gate_ref, gate_in, local_sem.at[2]),
        pltpu.make_async_copy(up_ref, up_in, local_sem.at[3]),
    ]
    for load in loads:
        load.start()

    barrier = pltpu.get_barrier_semaphore()
    for peer in ({"fsdp": other}, {"tp": sibling}, {"tp": opposite}):
        pl.semaphore_signal(barrier, inc=1, device_id=peer, device_id_type=MESH)
    pl.semaphore_signal(barrier, inc=1, device_id={"rep": inner}, device_id_type=MESH)

    @pl.when(jnp.logical_not(is_edge))
    def _():
        pl.semaphore_signal(barrier, inc=1, device_id={"rep": edge}, device_id_type=MESH)

    with jax.named_scope("barrier"):
        pl.semaphore_wait(barrier, 4 + jnp.where(is_edge, 0, 1))

    def grad_across():
        return remote(across_in, grads.at[rows_of(rep, fsdp), quarter_of(tp)], gx_send, gx_recv, {"fsdp": other})

    def grad_spot(r, s, t):
        return grads.at[rows_of(r, s), quarter_of(t)]

    def grad_hop(r, s, inward):
        spot = grad_spot(r, s, tp)
        to = inner if inward else edge
        return remote(spot, spot, (gz_in if inward else gz_out), gz_recv.at[r, s], {"rep": to})

    def grad_got(r, s):
        spot = grad_spot(r, s, tp)
        return remote(spot, spot, gz_in, gz_recv.at[r, s], {"rep": inner})

    def over_y(r, s, t):
        spot = grad_spot(r, s, t)
        return remote(spot, spot, gy_send, gy_recv.at[r, s], {"tp": opposite})

    def to_sibling(r, s, t):
        spot = grad_spot(r, s, t)
        return remote(spot, spot, gs_send, gs_recv.at[r], {"tp": sibling})

    def pass_sibling(r, s, t):
        spot = grad_spot(r, s, t)
        return remote(spot, spot, gf_send, gf_recv.at[r], {"tp": sibling})

    def hop(r, ch, inward, slot):
        spot = held.at[rows_of(r, fsdp), ch.cols]
        to = inner if inward else edge
        return remote(spot, spot, z_in if inward else z_out, z_recv.at[slot, ch.index], {"rep": to})

    def hop_got(slot, ch):
        spot = held.at[pl.ds(0, rows), ch.cols]
        return remote(spot, spot, z_in, z_recv.at[slot, ch.index], {"rep": inner})

    def hop_other(ch):
        spot = held.at[rows_of(edge, other), ch.cols]
        return remote(spot, spot, zo_send, x_recv.at[edge, ch.index], {"rep": inner})

    def cross(r, ch, send=None):
        spot = held.at[rows_of(r, fsdp), ch.cols]
        return remote(spot, spot, x_send if send is None else send, x_recv.at[r, ch.index], {"fsdp": other})

    def crossed(r, ch):
        spot = held.at[rows_of(r, other), ch.cols]
        return remote(spot, spot, x_send, x_recv.at[r, ch.index], {"fsdp": other})

    def hop_extra(ch):
        spot = held.at[rows_of(near, other), ch.cols]
        return remote(spot, spot, ze_send, x_recv.at[near, ch.index], {"rep": jnp.where(is_edge, near, edge)})

    def all_sent(blocks, width, send):
        spot = held.at[pl.ds(0, blocks * rows), pl.ds(0, width)]
        remote(spot, spot, send, gx_recv, {"fsdp": other}).wait_send()

    def among_extra(index):
        return functools.reduce(jnp.logical_or, [index == at for at in EXTRA])

    def when_extra(ch, act, otherwise):
        if isinstance(ch.index, int):
            act() if ch.index in extras else otherwise()
            return
        pl.when(among_extra(ch.index))(act)
        pl.when(jnp.logical_not(among_extra(ch.index)))(otherwise)

    def on_edge(act):
        pl.when(is_edge)(act)

    def on_middle(act):
        pl.when(jnp.logical_not(is_edge))(act)

    def chunks_from(low, high, act):
        if low < min(high, full):
            @pl.loop(low, min(high, full))
            def _(index):
                act(chunk(index))
        if full < count == high:
            act(chunk(full))

    loads[0].wait()
    grad_across().start()
    loads[1].wait()
    grad_hop(rep, fsdp, True).start()
    on_middle(lambda: grad_hop(rep, fsdp, False).start())

    with jax.named_scope("load"):
        loads[2].wait()
        loads[3].wait()

    @pl.loop(0, columns // LANES)
    def _(at):
        cols = pl.ds(pl.multiple_of(at * LANES, LANES), LANES)
        gate = gate_in[:, cols].astype(jnp.float32)
        held[rows_of(rep, fsdp), cols] = (
            jax.nn.silu(gate) * up_in[:, cols].astype(jnp.float32)
        ).astype(held.dtype)

    early = 2

    def own_inward(ch):
        hop(rep, ch, True, jnp.where(is_edge, 0, 1)).start()

    chunks_from(0, early, own_inward)
    on_middle(lambda: chunks_from(0, early, lambda ch: hop(rep, ch, False, 0).start()))

    def own_across(low, high):
        for index in range(low, min(high, count)):
            cross(rep, chunk(index)).start()

    own_across(0, 4)

    def share(r, s):
        over_y(r, s, tp).start()
        to_sibling(r, s, tp).start()

    def pass_on(r, s):
        over_y(r, s, opposite).wait_recv()
        pass_sibling(r, s, opposite).start()

    def settle(r, pairs):
        spots = grads.at[pl.ds(0, pairs * rows), pl.ds(0, quarter)]
        remote(spots, spots, gs_send, gs_recv.at[r], {"tp": sibling}).wait_recv()
        remote(spots, spots, gf_send, gf_recv.at[r], {"tp": sibling}).wait_recv()

    tile = 256

    def turn(r):
        spot = pl.ds(pl.multiple_of(r * 2 * rows, 2 * rows), 2 * rows)

        @pl.loop(0, half // tile)
        def _(m):
            part = pl.ds(pl.multiple_of(m * tile, tile), tile)
            turned[part, spot] = grads[spot, part].T

    def take_own():
        grad_across().wait_recv()
        grad_hop(rep, other, True).start()
        on_middle(lambda: grad_hop(rep, other, False).start())
        share(rep, other)

    def perform(plan, acts):
        for at, (name, *args) in enumerate(plan):
            with jax.named_scope(f"{name}{at}"):
                acts[name](*args)

    def grads_sent(blocks, send):
        all_sent(1, blocks * quarter, send)

    def shares_sent():
        grad_across().wait_send()
        for send in (gy_send, gs_send, gf_send):
            grads_sent(7, send)

    def clear():
        sums[fsdp * n_tp + tp] = jnp.zeros(sums.shape[1:], sums.dtype)

    def leave(product, spot, ch, squared):
        out_ref[spot, ch.cols] = product.astype(out_ref.dtype)
        if squared:
            squares = jnp.sum((product * product).reshape(TILE // 8, 8, ch.size), axis=0)
            total = squares[:, :LANES]
            for at in range(LANES, ch.size, LANES):
                total = total + squares[:, at:at + LANES]
            sums[fsdp * n_tp + tp] += total

    def tile_of(m):
        return pl.ds(pl.multiple_of(m * TILE, TILE), TILE)

    def multiply_tile(ch, m, squared):
        spot = tile_of(m)
        product = jnp.dot(turned[spot, :], held[:, ch.cols], preferred_element_type=jnp.float32)
        leave(product, spot, ch, squared)

    pair = 2 * rows
    ends = {"first": pl.multiple_of(edge * pair, pair), "late": pl.multiple_of(far_edge * pair, pair)}

    def part(spot, ch, start, size):
        tokens = pl.ds(start, size)
        return jnp.dot(turned[spot, tokens], held[tokens, ch.cols], preferred_element_type=jnp.float32)

    def kept(ch):
        return pl.ds((ch.index - (count - 3)) * WIDTH, ch.size)

    def begin(ch):
        @pl.loop(0, tiles)
        def _(m):
            spot = tile_of(m)
            middle_part[spot, kept(ch)] = part(spot, ch, pair, 2 * pair)

    def begin_end(ch):
        @pl.loop(0, tiles)
        def _(m):
            spot = tile_of(m)
            end_part[spot, kept(ch)] = part(spot, ch, ends["first"], pair)

    def complete(ch, squared):
        @pl.loop(0, tiles)
        def _(m):
            spot = tile_of(m)
            both = end_part[spot, kept(ch)] + part(spot, ch, ends["late"], pair)
            leave(middle_part[spot, kept(ch)] + both, spot, ch, squared)

    tiles = half // TILE

    def finish(ch, arrived, squared):
        with jax.named_scope("arrived_last"):
            arrived(ch)
        with jax.named_scope("multiply_last"):
            pl.loop(0, tiles)(lambda m: multiply_tile(ch, m, squared))

    def sweep(events, arrived_but_last, between, ended, lag, squared):
        def arrived(ch):
            arrived_but_last(ch)
            crossed(far_edge, ch).wait_recv()

        places = [at * tiles // len(events) for at in range(len(events))]

        def step(index):
            ch, lagging = chunk(index), chunk(index - lag)
            plan = [(place, event, ch) for place, event in zip(places, events)]
            plan.insert(sum(place == 0 for place in places), (0, arrived, lagging))

            @pl.loop(0, tiles)
            def _(m):
                for at, (place, event, subject) in enumerate(plan):
                    def run():
                        with jax.named_scope(f"event{at}"):
                            event(subject)
                    pl.when(m == place)(run)
                with jax.named_scope("multiply"):
                    multiply_tile(lagging, m, squared)

        last_three = [chunk(index) for index in range(count - 3, count)]
        far_pull, last_pull = events[1:]
        pl.loop(LAG, count - 3)(step)
        between()
        remaining = count - 3 - lag
        with jax.named_scope("far_last"):
            far_pull(last_three[0])
        chunks_from(remaining, remaining + 1, lambda ch: finish(ch, arrived, squared))
        with jax.named_scope("far_last"):
            for ch in last_three[1:]:
                far_pull(ch)
        with jax.named_scope("pull_last"):
            last_pull(last_three[0])
        chunks_from(remaining + 1, count - 3, lambda ch: finish(ch, arrived, squared))
        with jax.named_scope("pull_last"):
            for ch in last_three[1:]:
                last_pull(ch)
        ended()
        for ch in last_three:
            with jax.named_scope("begin"):
                arrived_but_last(ch)
                begin(ch)
                if squared:
                    begin_end(ch)
        for ch in last_three:
            with jax.named_scope("late"):
                crossed(far_edge, ch).wait_recv()
                complete(ch, squared)

    @on_edge
    def _():
        places = {"near": near, "far": far, "last": far_edge}
        sides = {"own": fsdp, "other": other}

        def take(name, s):
            grad_got(places[name], sides[s]).wait_recv()
            share(places[name], sides[s])

        def land(name, s, whole):
            r = rep if name == "rep" else places[name]
            pass_on(r, sides[s])
            if whole:
                settle(r, 1 if name == "rep" else 2)
                turn(r)

        def relay(*indices):
            for index in indices:
                if index + early < count:
                    own_inward(chunk(index + early))
                if index < count:
                    crossed(edge, chunk(index)).wait_recv()
                    hop_other(chunk(index)).start()

        def pull(slot, r):
            def event(ch):
                hop_got(slot, ch).wait_recv()
                cross(r, ch).start()
            return event

        def pull_near(ch):
            hop_got(0, ch).wait_recv()
            when_extra(ch, lambda: None, lambda: cross(near, ch, xn_send).start())

        pulls = [pull(1, far), pull(2, far_edge)]

        def near_at(*indices):
            for index in indices:
                pull_near(chunk(index))

        def near_ahead(ch):
            index = ch.index + FILL
            if isinstance(index, int):
                if index < count:
                    near_at(index)
                return
            pl.when(index < full)(lambda: near_at(index))
            if full < count:
                pl.when(index == full)(lambda: near_at(full))

        def early_events(*indices):
            for index in indices:
                if index >= early:
                    near_at(index + FILL)
                for event in pulls:
                    event(chunk(index))

        def arrived(ch):
            crossed(near, ch).wait_recv()
            crossed(far, ch).wait_recv()

        def compute(index):
            def whole(ch):
                arrived(ch)
                crossed(far_edge, ch).wait_recv()
            finish(chunk(index), whole, False)

        def batch(k):
            return range(k * count // 8, (k + 1) * count // 8)

        perform(
            [
                ("own",), ("across", 4, 9), ("take", "near", "own"), ("relay", *batch(0)),
                ("near", *range(early)), ("take", "near", "other"), ("across", 9, 12),
                ("land", "rep", "other", True), ("relay", *batch(1)),
                ("take", "far", "own"), ("across", 12, count), ("near", early), ("land", "near", "own", False),
                ("relay", *batch(2)), ("take", "far", "other"), ("near", early + 1),
                ("land", "near", "other", True), ("relay", *batch(3)), ("take", "last", "own"),
                ("near", early + 2), ("land", "far", "own", False), ("relay", *batch(4)),
                ("take", "last", "other"), ("land", "far", "other", True), ("relay", *batch(5)),
                ("early", 0), ("relay", *batch(6)), ("early", 1), ("land", "last", "own", False),
                ("relay", *batch(7)), ("early", 2), ("land", "last", "other", True),
                ("compute", 0), ("early", 3), ("compute", 1),
            ],
            {"own": take_own, "take": take, "land": land, "relay": relay, "early": early_events, "near": near_at,
             "compute": compute, "across": own_across},
        )

        def between():
            shares_sent()
            grads_sent(2, gz_in)
            all_sent(1, columns, z_in)
            all_sent(1, columns, zo_send)

        def near_and_part(ch):
            near_ahead(ch)
            for at in range(3):
                pl.when(ch.index == LAG + 2 + at)(lambda: begin_end(chunk(count - 3 + at)))

        sweep([near_and_part, *pulls], arrived, between, lambda: None, EDGE_LAG, False)
        all_sent(1, columns - extra_columns, xn_send)
        all_sent(3, columns, x_send)

    @on_middle
    def _():
        places = {"edge": edge, "far": far, "last": far_edge}
        sides = {"own": fsdp, "other": other}

        def take(name, s):
            r, s = places[name], sides[s]
            grad_got(r, s).wait_recv()
            grad_hop(r, s, name == "edge").start()
            share(r, s)

        def land(name, s, whole=True):
            r = rep if name == "rep" else places[name]
            pass_on(r, sides[s])
            if whole:
                settle(r, 1 if name == "rep" else 2)
                turn(r)

        def inward(*indices):
            for index in indices:
                ch = chunk(index)
                if not isinstance(index, int) or index >= early:
                    own_inward(ch)
                hop_got(0, ch).wait_recv()
                hop(edge, ch, True, 2).start()

        def fill(*indices):
            for index in indices:
                hop(rep, chunk(index), False, 0).start()

        def outer(ch):
            if isinstance(ch.index, int):
                if ch.index + FILL < count:
                    fill(ch.index + FILL)
            else:
                pl.when(ch.index + FILL < full)(lambda: fill(ch.index + FILL))
                if full < count:
                    pl.when(ch.index + FILL == full)(lambda: fill(full))
            follow(ch.index + AHEAD)
            if not isinstance(ch.index, int):
                pl.when(among_extra(ch.index))(lambda: send_extra(ch))

        def send_extra(ch):
            crossed(rep, ch).wait_recv()
            hop_extra(ch).start()

        def follow(index):
            if isinstance(index, int):
                if index < count:
                    inward(index)
                return
            pl.when(index < full)(lambda: inward(index))
            if full < count:
                pl.when(index == full)(lambda: inward(full))

        def pull(slot, r):
            def event(ch):
                hop_got(slot, ch).wait_recv()
                hop(r, ch, False, slot).start()
                cross(r, ch).start()
            return event

        pulls = [pull(1, far), pull(2, far_edge)]

        def early_events(*indices):
            for index in indices:
                if index >= early:
                    fill(index + FILL)
                for event in pulls:
                    event(chunk(index))

        perform(
            [
                ("own",), ("take", "far", "own"), ("across", 4, 9), ("fill", early),
                ("take", "edge", "own"), ("take", "edge", "other"), ("across", 9, 12),
                ("inward", *range(early)), ("take", "far", "other"),
                ("fill", early + 1), ("land", "rep", "other"), ("take", "last", "own"),
                ("across", 12, count),
                ("fill", early + 2), ("land", "far", "own", False),
                ("inward", *range(early, LAG)), ("take", "last", "other"), ("land", "edge", "own", False),
                ("early", 0, 1), ("inward", *range(LAG, LAG + 2)), ("land", "edge", "other"),
                ("land", "far", "other"), ("early", 2), ("inward", LAG + 2), ("land", "last", "own", False),
                ("early", 3), ("inward", LAG + 3), ("land", "last", "other"),
            ],
            {"own": take_own, "take": take, "land": land, "inward": inward, "early": early_events, "fill": fill,
             "across": own_across},
        )

        def arrived(ch):
            hop_other(ch).wait_recv()
            when_extra(ch, lambda: None, lambda: crossed(rep, ch).wait_recv())
            crossed(far, ch).wait_recv()

        clear()

        def ended():
            send_extra(chunk(count - 1))

        sweep([outer, *pulls], arrived, lambda: None, ended, LAG, True)

        mine = fsdp * n_tp + tp
        peers = [(a, k) for a in range(2) for k in range(n_tp) if a or k]

        def exchange(at):
            a, k = peers[at]
            to_side = other if a else fsdp
            to_tp = lax.rem(tp + k, n_tp)
            spot = sums.at[mine]
            return remote(spot, spot, sq_send, sq_recv, {"fsdp": to_side, "tp": to_tp})

        for at in range(len(peers)):
            exchange(at).start()
        with jax.named_scope("exchange"):
            seven = sums.at[pl.ds(0, len(peers))]
            remote(seven, seven, sq_send, sq_recv, {"fsdp": other}).wait_recv()
        square_total = jnp.sum(jnp.sum(sums[...], axis=0), keepdims=True)
        factor = 1.0 / jnp.sqrt(square_total / entry_count + 1e-06)
        total_out[...] = jnp.broadcast_to(factor, total_out.shape)
        remote(seven, seven, sq_send, sq_recv, {"fsdp": other}).wait_send()

    def tell():
        return remote(total_out, total_out, fa_send, fa_recv, {"rep": jnp.where(is_edge, near, edge)})

    on_middle(lambda: tell().start())
    with jax.named_scope("told"):
        on_edge(lambda: tell().wait_recv())
    factor_ref[...] = total_out[...]

    @on_middle
    def _():
        tell().wait_send()
        shares_sent()
        grads_sent(4, gz_in)
        grads_sent(6, gz_out)
        all_sent(2, columns, z_in)
        all_sent(3, columns, z_out)
        all_sent(3, columns, x_send)
        all_sent(1, extra_columns, ze_send)


def by_kernel(n_rep, n_tp, entry_count, gate_pre, up_pre, out_grad):
    rows, columns = gate_pre.shape
    tokens = rows * n_rep * 2
    half = out_grad.shape[1] // 2
    quarter = half // n_tp
    full, count, chunk = chunking(columns)
    kept = 2 * WIDTH + chunk(count - 1).size
    dma = pltpu.SemaphoreType.DMA
    block, whole = dma((n_rep, 2)), dma((n_rep,))
    return pl.pallas_call(
        functools.partial(gather_multiply, entry_count),
        out_shape=(
            pltpu.VMEM((half, columns), jnp.bfloat16),
            pltpu.VMEM((8, LANES), jnp.float32),
        ),
        in_specs=[pl.BlockSpec(memory_space=pl.ANY)] * 3,
        out_specs=(pl.BlockSpec(memory_space=pltpu.VMEM), pl.BlockSpec(memory_space=pltpu.VMEM)),
        scratch_shapes=[
            pltpu.VMEM((tokens, columns), jnp.bfloat16),
            pltpu.VMEM((tokens, half), jnp.bfloat16),
            pltpu.VMEM((half, tokens), jnp.bfloat16),
            pltpu.VMEM((rows, columns), jnp.bfloat16),
            pltpu.VMEM((rows, columns), jnp.bfloat16),
            pltpu.VMEM((rows, quarter), jnp.bfloat16),
            pltpu.VMEM((2 * n_tp, 8, LANES), jnp.float32),
            pltpu.VMEM((8, LANES), jnp.float32),
            pltpu.VMEM((half, kept), jnp.float32),
            pltpu.VMEM((half, kept), jnp.float32),
            dma((4,)), dma, dma, block, dma, dma, dma, block,
            dma, whole, dma, whole,
            dma((3, count)), dma, dma, dma, dma, dma, dma, dma((n_rep, count)),
            dma, dma, dma, dma,
        ],
        compiler_params=pltpu.CompilerParams(
            collective_id=0, has_side_effects=True, vmem_limit_bytes=VMEM_LIMIT * 4 // 5
        ),
    )(gate_pre, up_pre, out_grad)


def scale(summed, factors):
    half, columns = summed.shape
    rows = 128

    def body(summed_ref, factor_ref, out_ref, ready, sems):
        steps = half // rows
        depth = ready.shape[0]

        def leave(m):
            slot = lax.rem(m, depth)
            spot = pl.ds(pl.multiple_of(m * rows, rows), rows)
            return pltpu.make_async_copy(ready.at[slot], out_ref.at[spot, :], sems.at[slot])

        @pl.loop(0, steps)
        def _(m):
            slot = lax.rem(m, depth)
            spot = pl.ds(pl.multiple_of(m * rows, rows), rows)

            @pl.when(m >= depth)
            def _():
                leave(m - depth).wait()
            for at in range(0, columns, LANES):
                cols = pl.ds(at, LANES)
                scaled = summed_ref[spot, cols].astype(jnp.float32) * factor_ref[0:1, :]
                ready[slot, :, cols] = scaled.astype(ready.dtype)
            leave(m).start()

        @pl.loop(max(steps - depth, 0), steps)
        def _(m):
            leave(m).wait()

    return pl.pallas_call(
        body,
        out_shape=jax.ShapeDtypeStruct((half, columns), jnp.bfloat16),
        in_specs=[pl.BlockSpec(memory_space=pltpu.VMEM)] * 2,
        out_specs=pl.BlockSpec(memory_space=pl.ANY),
        scratch_shapes=[pltpu.VMEM((4, rows, columns), jnp.bfloat16), pltpu.SemaphoreType.DMA((4,))],
        compiler_params=pltpu.CompilerParams(vmem_limit_bytes=16 * 1024 * 1024),
    )(summed, factors)


def by_xla(gate_pre, up_pre, out_grad):
    hidden = (jax.nn.silu(gate_pre.astype(jnp.float32)) * up_pre.astype(jnp.float32)).astype(
        jnp.bfloat16
    )
    spread = lax.all_to_all(out_grad, "fsdp", split_axis=1, concat_axis=0, tiled=True)
    grad_rows = lax.all_gather(spread, "rep", axis=0, tiled=True)
    hidden_rows = lax.all_gather(hidden, ("rep", "fsdp"), axis=0, tiled=True)
    summed = lax.dot_general(
        grad_rows, hidden_rows, (((0,), (0,)), ((), ())), preferred_element_type=jnp.float32
    )
    return summed, jnp.sum(summed * summed)


def kernel_fits(n_rep, n_fsdp, n_tp, rows, columns, features):
    tokens, half = rows * n_rep * n_fsdp, features // n_fsdp
    held_bytes = 2 * (tokens * columns + 2 * tokens * half + half * columns + 2 * rows * columns)
    held_bytes += 24 * half * WIDTH
    aligned = rows % 128 == 0 and columns % LANES == 0 and half % (LANES * n_tp) == 0
    shaped = (n_rep, n_fsdp, n_tp) == (4, 2, 4) and columns >= max(12 * WIDTH, 7 * half // n_tp)
    return shaped and aligned and half % TILE == 0 and held_bytes < VMEM_LIMIT * 4 // 5


def solution(mesh):
    n_rep, n_fsdp, n_tp = (mesh.shape[axis] for axis in ("rep", "fsdp", "tp"))

    def on_device(gate_pre, up_pre, out_grad):
        half, columns = out_grad.shape[1] // n_fsdp, gate_pre.shape[1]
        entry_count = half * n_fsdp * columns * n_tp
        if kernel_fits(n_rep, n_fsdp, n_tp, *gate_pre.shape, out_grad.shape[1]):
            summed, factors = by_kernel(n_rep, n_tp, entry_count, gate_pre, up_pre, out_grad)
            return scale(summed, factors)
        summed, square_sum = by_xla(gate_pre, up_pre, out_grad)
        square_total = lax.psum(square_sum, ("fsdp", "tp"))
        factor = 1.0 / jnp.sqrt(square_total / entry_count + 1e-06)
        return (summed * factor).astype(jnp.bfloat16)

    return jax.shard_map(
        on_device,
        mesh=mesh,
        in_specs=(P(("rep", "fsdp"), "tp"), P(("rep", "fsdp"), "tp"), P(("rep", "fsdp"), None)),
        out_specs=P("fsdp", "tp"),
        check_vma=False,
    )
```
